32 devices in a mesh: row: 8 (over z, x), col: 4 (over y, core).
Axes of the slice: x: 2, y: 2, z: 4, core: 2. Of those that a mesh axis runs over, the one named last changes fastest.
Arguments:
- tensor: float32 [32, 1024, 1024], P(None, 'row', 'col'), may hold values from -6 to 6
- initial_first: float32 [1024, 256], P('row'), may hold values from -6 to 6
- initial_second: float32 [1024, 256], P('col'), may hold values from -6 to 6
Outputs:
- factor_first: float32 [1024, 256], P('row')
- factor_second: float32 [1024, 256], P('col')
- factor_frames: float32 [32, 256], replicated
- weights: float32 [256], replicated
The draws below stay inside these ranges and needn't reach their ends.
All inputs are finite; a program needn't handle non-finite values.
Results may differ from the reference program's by a relative error of at most 0.00024.
Values sent between devices are 32-bit elements; how exact they have to be, the bound alone decides.
A program may use at most 128 MiB of HBM per device.

```python
import math
import jax
import jax.numpy as jnp
from jax import lax

R = 256
K = 32
PASSES = 2
I = 1024
J = 1024


def block_scale(stream_key, shape, shards, least, high):
    factor_of = 1.0
    for position, parts in shards:
        draws = jax.random.uniform(jax.random.fold_in(jax.random.fold_in(stream_key, 6), position), (parts,), jnp.float32, least / len(shards), high / len(shards))
        factor_of = factor_of * jnp.repeat(jnp.exp(draws), shape[position] // parts).reshape((-1,) + (1,) * (len(shape) - 1 - position))
    return factor_of


def scatter_about(own_key, shape, scale, reach, split=(), dtype=jnp.bfloat16):
    array = jax.random.normal(own_key, shape, jnp.float32) * scale
    if len(split) > 0:
        array = block_scale(own_key, shape, split, -0.22, 0.18) * array
    return jnp.clip(array, min=-reach, max=reach).astype(dtype)


def setup_inputs(seed: int = 0) -> dict:
    seeds = jax.random.split(jax.random.key(seed), 4)
    return {
        "tensor": scatter_about(seeds[0], (K, I, J), 1.0, 6.0, ((1, 8), (2, 4)), jnp.float32),
        "initial_first": scatter_about(seeds[1], (I, R), 1.0, 6.0, ((0, 8),), jnp.float32),
        "initial_second": scatter_about(seeds[2], (J, R), 1.0, 6.0, ((0, 4),), jnp.float32),
    }


epsilon = 1e-06

def solve_gram(partials, hadamard):
    factor_lower = jnp.linalg.cholesky(hadamard)
    midway = lax.linalg.triangular_solve(factor_lower, partials, left_side=False, lower=True, transpose_a=True)
    return lax.linalg.triangular_solve(factor_lower, midway, left_side=False, lower=True, transpose_a=False)

def normalize(unscaled):
    scaling = jnp.sqrt(lax.optimization_barrier(jnp.mean(unscaled * unscaled, axis=0)) + epsilon)
    return (unscaled / scaling, scaling)

def gram_of(matrix):
    return jnp.dot(matrix.T, matrix, precision=lax.Precision.HIGHEST) / matrix.shape[0]

def reference(tensor, initial_first, initial_second):
    highest = lax.Precision.HIGHEST
    frames = tensor.shape[0]
    rows_first = tensor.shape[1]
    rows_second = tensor.shape[2]
    first_gram = gram_of(initial_first)
    second = initial_second
    second_gram = gram_of(initial_second)
    contracted = jnp.einsum('kij,ir->kjr', tensor, initial_first, precision=highest)
    for repeat in range(PASSES):
        frame_sums = jnp.einsum('kjr,jr->kr', contracted, second, precision=highest)
        frame_raw = solve_gram(frame_sums, first_gram * second_gram) / math.sqrt(rows_first * rows_second)
        factor_frames, unused = normalize(frame_raw)
        frame_gram = gram_of(factor_frames)
        second_sums = jnp.einsum('kjr,kr->jr', contracted, factor_frames, precision=highest)
        second_raw = solve_gram(second_sums, first_gram * frame_gram) / math.sqrt(rows_first * frames)
        second, unused = normalize(second_raw)
        second_gram = gram_of(second)
    second_contracted = jnp.einsum('kij,jr->kir', tensor, second, precision=highest)
    first_sums = jnp.einsum('kir,kr->ir', second_contracted, factor_frames, precision=highest)
    first_raw = solve_gram(first_sums, second_gram * frame_gram) / math.sqrt(rows_second * frames)
    factor_first, weights = normalize(first_raw)
    return (factor_first, second, factor_frames, weights)
```

```python
import functools
import math

import jax
import jax.numpy as jnp
from jax import lax
from jax.experimental import pallas as pl
from jax.experimental.pallas import tpu as pltpu
from jax.sharding import PartitionSpec as P

PASSES = 2
LANES = 128
PIVOTS = 16
MESH = pl.DeviceIdType.MESH
HIGHEST = lax.Precision.HIGHEST
HIGH = lax.Precision.HIGH

epsilon = 1e-06


def product(a, b, precision=HIGHEST):
    return jnp.dot(a, b, precision=precision, preferred_element_type=jnp.float32)


def cross(a, b, precision=HIGHEST):
    return lax.dot_general(
        a, b, (((0,), (0,)), ((), ())), precision=precision, preferred_element_type=jnp.float32
    )


def split(x):
    high = x.astype(jnp.bfloat16)
    rest = x - high.astype(jnp.float32)
    mid = rest.astype(jnp.bfloat16)
    return high, mid, (rest - mid.astype(jnp.float32)).astype(jnp.bfloat16)


def outer(left, right):
    h, m, l = split(left)
    hh, mm, ll = split(right)
    return lax.dot_general(
        jnp.concatenate([h, h, m, h, m, l], axis=0),
        jnp.concatenate([hh, mm, hh, ll, mm, hh], axis=0),
        (((0,), (0,)), ((), ())), preferred_element_type=jnp.float32,
    )


def invert(a, start, stop):
    size = a.shape[0]
    tiles = size // LANES
    row = lax.broadcasted_iota(jnp.int32, (PIVOTS, LANES), 0)
    lanes = [
        lax.broadcasted_iota(jnp.int32, (PIVOTS, LANES), 1) + q * LANES for q in range(tiles)
    ]
    wide = lax.broadcasted_iota(jnp.int32, (PIVOTS, size), 1)
    whole = lax.broadcasted_iota(jnp.int32, (size, size), 1)

    def step(g, carry):
        base = g * PIVOTS
        here = pl.ds(pl.multiple_of(base, PIVOTS), PIVOTS)
        rows = [a[here, q * LANES : (q + 1) * LANES] for q in range(tiles)]
        cols = []
        for t in range(PIVOTS):
            picked = sum(jnp.where(lanes[q] == base + t, rows[q], 0.0) for q in range(tiles))
            cols.append(
                jnp.broadcast_to(jnp.sum(picked, axis=1, keepdims=True), (PIVOTS, LANES))
            )
        work = []
        for q in range(tiles):
            place = lanes[q] - base
            inside = (place >= 0) & (place < PIVOTS)
            unit = jnp.where(place == row, 1.0, 0.0)
            work.append(jnp.where(inside, unit, rows[q]))
        for t in range(PIVOTS):
            pivot = 1.0 / jnp.broadcast_to(cols[t][t : t + 1, :], (PIVOTS, LANES))
            at = row == t

            def reduced(x):
                scaled = jnp.broadcast_to(x[t : t + 1, :], (PIVOTS, LANES)) * pivot
                return jnp.where(at, scaled, x - cols[t] * scaled)

            later = [reduced(cols[s]) for s in range(t + 1, PIVOTS)]
            work = [reduced(w) for w in work]
            cols[t + 1 :] = later
        solved = jnp.concatenate(work, axis=1)
        raw = a[here, :]
        inside = (wide >= base) & (wide < base + PIVOTS)
        left = jnp.where(inside, 0.0, jnp.where(wide < base, -raw, raw))
        kept = jnp.where((whole >= base) & (whole < base + PIVOTS), 0.0, a[...])
        a[...] = kept - outer(left, solved)
        a[here, :] = solved
        return carry

    lax.fori_loop(start, stop, step, 0)


def greet(sizes):
    barrier = pltpu.get_barrier_semaphore()
    for axis, n in sizes.items():
        me = lax.axis_index(axis)
        for d in range(1, n):
            pl.semaphore_signal(
                barrier, inc=1, device_id={axis: lax.rem(me + d, n)}, device_id_type=MESH
            )


def greeted(sizes):
    pl.semaphore_wait(pltpu.get_barrier_semaphore(), sum(n - 1 for n in sizes.values()))


def send(source, target, sems, at, device):
    copy = pltpu.make_async_remote_copy(
        src_ref=source, dst_ref=target, send_sem=sems.at[0, at], recv_sem=sems.at[1, at],
        device_id=device, device_id_type=MESH,
    )
    copy.start()
    return copy


def span(index, chunk):
    return pl.ds(pl.multiple_of(index * chunk, 8), chunk)


def scatter(axis, n, source, recv, sems, offset=0):
    me = lax.axis_index(axis)
    chunk = recv.shape[1]
    copies = []
    for d in range(1, n):
        peer = lax.rem(me + d, n)
        there = pl.ds(pl.multiple_of(offset + peer * chunk, 8), chunk)
        copies.append(send(source.at[there, :], recv.at[me], sems, d - 1, {axis: peer}))
    recv[me] = source[pl.ds(pl.multiple_of(offset + me * chunk, 8), chunk), :]
    return copies


def gather(axis, n, own, full, sems, offset=0):
    me = lax.axis_index(axis)
    chunk = own.shape[0]
    place = pl.ds(pl.multiple_of(offset + me * chunk, 8), chunk)
    full[place, :] = own
    return [
        send(full.at[place, :], full.at[place, :], sems, d - 1, {axis: lax.rem(me + d, n)})
        for d in range(1, n)
    ]


def finish(copies):
    for copy in copies:
        copy.wait()


def total(recv):
    result = recv[0]
    for s in range(1, recv.shape[0]):
        result = result + recv[s]
    return result


def total_blocks(full, n):
    chunk = full.shape[0] // n
    result = full[0:chunk, :]
    for s in range(1, n):
        result = result + full[s * chunk : (s + 1) * chunk, :]
    return result


class Twin:
    def __init__(self, col):
        self.count = col // 2
        me = lax.axis_index("col")
        self.core = lax.rem(me, 2)
        self.chip = me // 2
        self.partner = {"col": self.chip * 2 + 1 - self.core}
        self.others = [
            {"col": lax.rem(self.chip + d, self.count) * 2 + self.core}
            for d in range(1, self.count)
        ]


def halves_out(twin, gram, recv, sems):
    half = gram.shape[0] // 2
    return [send(gram.at[span(1 - twin.core, half), :], recv, sems, 0, twin.partner)]


def halves_across(twin, gram, recv, across, sems):
    half = gram.shape[0] // 2
    across[twin.chip] = gram[span(twin.core, half), :] + recv[...]
    here = across.at[twin.chip]
    return [send(here, here, sems, d, peer) for d, peer in enumerate(twin.others)]


def halves_back(twin, full, sems):
    half = full.shape[0] // 2
    mine = full.at[span(twin.core, half), :]
    return [send(mine, mine, sems, 0, twin.partner)]


def layout(sizes, frames, own_first, own_second, rank):
    row, col = sizes["row"], sizes["col"]
    square = (rank, rank)
    half = rank // 2
    chips = col // 2
    buffers = {
        "tens": (frames, own_first, own_second),
        "held": (frames, own_second, rank),
        "inv": square, "sums": (frames, rank),
        "gram_a": square, "recv_a": (row, half // row, rank), "full_a": square,
        "gram_b": square, "recv_b": (half, rank), "across_b": (chips, half, rank),
        "full_b": square,
        "terms_f": (own_first, rank), "recv_f": (col, own_first // col, rank),
        "full_f": (own_first, rank), "parts_w": (row * 8, rank),
    }
    axes = {
        "a": row, "a2": row, "a3": 2, "b": 2, "b2": chips, "b3": 2, "f": col, "f2": col,
        "w": row,
    }
    for p in range(PASSES):
        buffers.update({
            "parts_r%d" % p: (row * frames, rank), "parts_c%d" % p: (col * frames, rank),
            "raw_s%d" % p: (own_second, rank),
            "gram_g%d" % p: square, "recv_g%d" % p: (half, rank),
            "across_g%d" % p: (chips, half, rank), "full_g%d" % p: square,
        })
        axes.update({
            "r%d" % p: row, "c%d" % p: col, "g%d" % p: 2, "h%d" % p: chips, "i%d" % p: 2,
        })
        for q in range(rank // LANES):
            buffers.update({
                "terms_s%d%d" % (p, q): (own_second, LANES),
                "recv_s%d%d" % (p, q): (row, own_second // row, LANES),
                "full_s%d%d" % (p, q): (own_second, LANES),
            })
            axes.update({"s%d%d" % (p, q): row, "t%d%d" % (p, q): row})
    names = list(buffers) + ["sem_" + name for name in axes] + ["sem_load"]
    shapes = [pltpu.VMEM(shape, jnp.float32) for shape in buffers.values()]
    shapes += [pltpu.SemaphoreType.DMA((2, max(n - 1, 1))) for n in axes.values()]
    shapes += [pltpu.SemaphoreType.DMA((frames,))]
    return names, shapes


def kernel(sizes, names, tensor, first, second, first_out, second_out, frames_out, weights_out, *scratch):
    row, col = sizes["row"], sizes["col"]
    v = dict(zip(names, scratch))
    inv, sums, tens, held = v["inv"], v["sums"], v["tens"], v["held"]
    frames, own_first, own_second = tensor.shape
    rank = first.shape[1]
    half = rank // 2
    tiles = rank // LANES
    rows_first, rows_second = own_first * row, own_second * col
    steps = rank // PIVOTS
    twin = Twin(col)

    def load(k):
        return pltpu.make_async_copy(tensor.at[k], tens.at[k], v["sem_load"].at[k])

    def start_load(k, carry):
        load(k).start()
        return carry

    def contract(start, stop):
        group = math.gcd(stop - start, 4)

        def step(g, carry):
            ks = [start + g * group + u for u in range(group)]
            for k in ks:
                load(k).wait()
            parts = [cross(tens[k], first[...], HIGH) for k in ks]
            for k, part in zip(ks, parts):
                held[k] = part
                sums[pl.ds(k, 1), :] = jnp.sum(part * second[...], axis=0, keepdims=True)
            return carry

        lax.fori_loop(0, (stop - start) // group, step, 0)

    def frame_terms(raw, start, stop):
        def step(k, carry):
            sums[pl.ds(k, 1), :] = jnp.sum(held[k] * raw[...], axis=0, keepdims=True)
            return carry

        lax.fori_loop(start, stop, step, 0, unroll=4)

    def second_terms(out, q):
        block = math.gcd(own_second, 128)
        here = slice(q * LANES, (q + 1) * LANES)
        for c in range(0, own_second, block):
            def step(k, total):
                return total + held[k, c : c + block, here] * frames_out[pl.ds(k, 1), :][:, here]

            out[c : c + block, :] = lax.fori_loop(
                0, frames, step, jnp.zeros((block, LANES), jnp.float32), unroll=4
            )

    def first_terms(raw, start, stop):
        group = math.gcd(stop - start, 4)

        def step(g, carry):
            base = start + g * group
            stacked = tens[pl.ds(base, group)].reshape(group * own_first, own_second)
            part = product(stacked, raw[...], HIGH)
            v["terms_f"][...] += sum(
                part[u * own_first : (u + 1) * own_first, :] * frames_out[pl.ds(base + u, 1), :]
                for u in range(group)
            )
            return carry

        lax.fori_loop(0, (stop - start) // group, step, 0)

    def solve_frames(frame_sums):
        raw = product(frame_sums, inv[...]) * (1.0 / math.sqrt(rows_first * rows_second))
        normed = raw / jnp.sqrt(jnp.mean(raw * raw, axis=0, keepdims=True) + epsilon)
        frames_out[...] = normed
        return cross(normed, normed) / frames

    greet(sizes)
    lax.fori_loop(0, frames, start_load, 0)
    v["gram_a"][...] = cross(first[...], first[...])
    v["gram_b"][...] = cross(second[...], second[...])
    contract(0, frames // 4)
    greeted(sizes)
    offset = twin.core * half
    go_a = scatter("row", row, v["gram_a"], v["recv_a"], v["sem_a"], offset)
    go_b = halves_out(twin, v["gram_b"], v["recv_b"], v["sem_b"])
    contract(frames // 4, frames * 5 // 8)
    finish(go_b)
    go_b = halves_across(twin, v["gram_b"], v["recv_b"], v["across_b"], v["sem_b2"])
    finish(go_a)
    go_a = gather("row", row, total(v["recv_a"]), v["full_a"], v["sem_a2"], offset)
    contract(frames * 5 // 8, frames)
    go_r = gather("row", row, sums[...], v["parts_r0"], v["sem_r0"])
    finish(go_b)
    v["full_b"][span(twin.core, half), :] = total(v["across_b"])
    go_b = halves_back(twin, v["full_b"], v["sem_b3"])
    finish(go_a)
    go_a = halves_back(twin, v["full_a"], v["sem_a3"])
    finish(go_b)
    finish(go_a)
    first_gram = v["gram_a"]
    first_gram[...] = v["full_a"][...] * (1.0 / rows_first)
    second_gram = v["full_b"][...] * (1.0 / rows_second)
    wide = None
    for p in range(PASSES):
        here = str(p)
        split_at = steps // 8 if p == 0 else steps // 2
        inv[...] = first_gram[...] * second_gram
        invert(inv, 0, split_at)
        finish(go_r)
        go_c = gather(
            "col", col, total_blocks(v["parts_r" + here], row), v["parts_c" + here],
            v["sem_c" + here],
        )
        invert(inv, split_at, steps)
        finish(go_c)
        frame_sums = total_blocks(v["parts_c" + here], col)
        if wide is not None:
            frame_sums = frame_sums / wide
        frame_gram = solve_frames(frame_sums)
        parts = [here + str(q) for q in range(tiles)]
        go_s = []
        for q, part in enumerate(parts):
            second_terms(v["terms_s" + part], q)
            go_s.append(scatter(
                "row", row, v["terms_s" + part], v["recv_s" + part], v["sem_s" + part]
            ))
        inv[...] = first_gram[...] * frame_gram
        go_t = []
        at = 0
        for q, part in enumerate(parts):
            invert(inv, at, steps * (5 + 2 * q) // 8)
            at = steps * (5 + 2 * q) // 8
            finish(go_s[q])
            go_t.append(gather(
                "row", row, total(v["recv_s" + part]), v["full_s" + part], v["sem_t" + part]
            ))
        invert(inv, at, steps)
        for copies in go_t:
            finish(copies)
        raw = v["raw_s" + here]
        summed = jnp.concatenate([v["full_s" + part][...] for part in parts], axis=1)
        raw[...] = product(summed, inv[...]) * (1.0 / math.sqrt(rows_first * frames))
        gram_g, recv_g, across_g, full_g = (
            v[name + here] for name in ("gram_g", "recv_g", "across_g", "full_g")
        )
        gram_g[...] = cross(raw[...], raw[...])
        go_g = halves_out(twin, gram_g, recv_g, v["sem_g" + here])
        last = p + 1 == PASSES
        if last:
            v["terms_f"][...] = jnp.zeros((own_first, rank), jnp.float32)
            first_terms(raw, 0, frames // 4)
        else:
            later = str(p + 1)
            frame_terms(raw, 0, frames // 2)
        finish(go_g)
        go_g = halves_across(twin, gram_g, recv_g, across_g, v["sem_h" + here])
        if last:
            first_terms(raw, frames // 4, frames)
            go_f = scatter("col", col, v["terms_f"], v["recv_f"], v["sem_f"])
        else:
            frame_terms(raw, frames // 2, frames)
            go_r = gather("row", row, sums[...], v["parts_r" + later], v["sem_r" + later])
        finish(go_g)
        full_g[span(twin.core, half), :] = total(across_g)
        go_g = halves_back(twin, full_g, v["sem_i" + here])
        finish(go_g)
        gram = full_g[...] * (1.0 / rows_second)
        down = lax.broadcasted_iota(jnp.int32, (rank, rank), 0)
        across = lax.broadcasted_iota(jnp.int32, (rank, rank), 1)
        diagonal = jnp.where(down == across, gram, 0.0)
        wide = jnp.sqrt(jnp.sum(diagonal, axis=0, keepdims=True) + epsilon)
        tall = jnp.sqrt(jnp.sum(diagonal, axis=1, keepdims=True) + epsilon)
        second_gram = gram / wide / tall
    inv[...] = second_gram * frame_gram
    second_out[...] = raw[...] / wide
    invert(inv, 0, steps // 4)
    finish(go_f)
    go_f = gather("col", col, total(v["recv_f"]), v["full_f"], v["sem_f2"])
    invert(inv, steps // 4, steps)
    finish(go_f)
    raw = product(v["full_f"][...] / wide, inv[...]) * (1.0 / math.sqrt(rows_second * frames))
    squares = jnp.sum(raw * raw, axis=0, keepdims=True)
    go_w = gather("row", row, jnp.broadcast_to(squares, (8, rank)), v["parts_w"], v["sem_w"])
    first_out[...] = raw
    finish(go_w)
    weights = jnp.sqrt(total_blocks(v["parts_w"], row) * (1.0 / rows_first) + epsilon)
    weights_out[...] = weights
    first_out[...] = first_out[...] / weights[0:1, :]


def body(sizes, tensor, initial_first, initial_second):
    frames, own_first, own_second = tensor.shape
    rank = initial_first.shape[1]
    names, scratch = layout(sizes, frames, own_first, own_second, rank)
    vmem = pl.BlockSpec(memory_space=pltpu.VMEM)
    outs = ((own_first, rank), (own_second, rank), (frames, rank), (8, rank))
    factor_first, second, factor_frames, weights = pl.pallas_call(
        functools.partial(kernel, sizes, names),
        out_shape=[jax.ShapeDtypeStruct(shape, jnp.float32) for shape in outs],
        in_specs=[pl.BlockSpec(memory_space=pl.ANY), vmem, vmem],
        out_specs=[vmem] * len(outs),
        scratch_shapes=scratch,
        compiler_params=pltpu.CompilerParams(
            collective_id=0, has_side_effects=True, vmem_limit_bytes=48 * 1024 * 1024
        ),
        name="als",
    )(tensor, initial_first, initial_second)
    return (factor_first, second, factor_frames, weights[0])


def solution(mesh):
    sizes = {"row": mesh.shape["row"], "col": mesh.shape["col"]}
    placed = (P(None, "row", "col"), P("row", None), P("col", None))
    return jax.shard_map(
        functools.partial(body, sizes),
        mesh=mesh,
        in_specs=placed,
        out_specs=(P("row", None), P("col", None), P(), P()),
        check_vma=False,
    )
```

```python
import functools
import math

import jax
import jax.numpy as jnp
from jax import lax
from jax.experimental import pallas as pl
from jax.experimental.pallas import tpu as pltpu
from jax.sharding import PartitionSpec as P

PASSES = 2
LANES = 128
PIVOTS = 16
GROUP = 4
MESH = pl.DeviceIdType.MESH
HIGHEST = lax.Precision.HIGHEST
HIGH = lax.Precision.HIGH

epsilon = 1e-06


def product(a, b, precision=HIGHEST):
    return jnp.dot(a, b, precision=precision, preferred_element_type=jnp.float32)


def cross(a, b, precision=HIGHEST):
    return lax.dot_general(
        a, b, (((0,), (0,)), ((), ())), precision=precision, preferred_element_type=jnp.float32
    )


def split(x):
    high = x.astype(jnp.bfloat16)
    rest = x - high.astype(jnp.float32)
    mid = rest.astype(jnp.bfloat16)
    return high, mid, (rest - mid.astype(jnp.float32)).astype(jnp.bfloat16)


def outer(left, right):
    h, m, l = split(left)
    hh, mm, ll = split(right)
    return lax.dot_general(
        jnp.concatenate([h, h, m, h, m, l], axis=0),
        jnp.concatenate([hh, mm, hh, ll, mm, hh], axis=0),
        (((0,), (0,)), ((), ())), preferred_element_type=jnp.float32,
    )


def invert(a, start, stop):
    size = a.shape[0]
    tiles = size // LANES
    row = lax.broadcasted_iota(jnp.int32, (PIVOTS, LANES), 0)
    lanes = [
        lax.broadcasted_iota(jnp.int32, (PIVOTS, LANES), 1) + q * LANES for q in range(tiles)
    ]
    wide = lax.broadcasted_iota(jnp.int32, (PIVOTS, size), 1)
    whole = lax.broadcasted_iota(jnp.int32, (size, size), 1)

    def step(g, carry):
        base = g * PIVOTS
        here = pl.ds(pl.multiple_of(base, PIVOTS), PIVOTS)
        rows = [a[here, q * LANES : (q + 1) * LANES] for q in range(tiles)]
        cols = []
        for t in range(PIVOTS):
            picked = sum(jnp.where(lanes[q] == base + t, rows[q], 0.0) for q in range(tiles))
            cols.append(
                jnp.broadcast_to(jnp.sum(picked, axis=1, keepdims=True), (PIVOTS, LANES))
            )
        work = []
        for q in range(tiles):
            place = lanes[q] - base
            inside = (place >= 0) & (place < PIVOTS)
            unit = jnp.where(place == row, 1.0, 0.0)
            work.append(jnp.where(inside, unit, rows[q]))
        for t in range(PIVOTS):
            pivot = 1.0 / jnp.broadcast_to(cols[t][t : t + 1, :], (PIVOTS, LANES))
            at = row == t

            def reduced(x):
                scaled = jnp.broadcast_to(x[t : t + 1, :], (PIVOTS, LANES)) * pivot
                return jnp.where(at, scaled, x - cols[t] * scaled)

            later = [reduced(cols[s]) for s in range(t + 1, PIVOTS)]
            work = [reduced(w) for w in work]
            cols[t + 1 :] = later
        solved = jnp.concatenate(work, axis=1)
        raw = a[here, :]
        inside = (wide >= base) & (wide < base + PIVOTS)
        left = jnp.where(inside, 0.0, jnp.where(wide < base, -raw, raw))
        kept = jnp.where((whole >= base) & (whole < base + PIVOTS), 0.0, a[...])
        a[...] = kept - outer(left, solved)
        a[here, :] = solved
        return carry

    lax.fori_loop(start, stop, step, 0)


def greet(sizes):
    barrier = pltpu.get_barrier_semaphore()
    for axis, n in sizes.items():
        me = lax.axis_index(axis)
        for d in range(1, n):
            pl.semaphore_signal(
                barrier, inc=1, device_id={axis: lax.rem(me + d, n)}, device_id_type=MESH
            )


def greeted(sizes):
    pl.semaphore_wait(pltpu.get_barrier_semaphore(), sum(n - 1 for n in sizes.values()))


def send(source, target, sems, at, device):
    copy = pltpu.make_async_remote_copy(
        src_ref=source, dst_ref=target, send_sem=sems.at[0, at], recv_sem=sems.at[1, at],
        device_id=device, device_id_type=MESH,
    )
    copy.start()
    return copy


def span(index, chunk):
    return pl.ds(pl.multiple_of(index * chunk, 8), chunk)


def scatter(axis, n, source, recv, sems, offset=0):
    me = lax.axis_index(axis)
    chunk = recv.shape[1]
    copies = []
    for d in range(1, n):
        peer = lax.rem(me + d, n)
        there = pl.ds(pl.multiple_of(offset + peer * chunk, 8), chunk)
        copies.append(send(source.at[there, :], recv.at[me], sems, d - 1, {axis: peer}))
    recv[me] = source[pl.ds(pl.multiple_of(offset + me * chunk, 8), chunk), :]
    return copies


def gather(axis, n, own, full, sems, offset=0):
    me = lax.axis_index(axis)
    chunk = own.shape[0]
    place = pl.ds(pl.multiple_of(offset + me * chunk, 8), chunk)
    full[place, :] = own
    return [
        send(full.at[place, :], full.at[place, :], sems, d - 1, {axis: lax.rem(me + d, n)})
        for d in range(1, n)
    ]


def spread(axis, n, line, parts, sems):
    me = lax.axis_index(axis)
    here = parts.at[me, pl.ds(0, 1), :]
    parts[me, 0:1, :] = line
    return [send(here, here, sems, d - 1, {axis: lax.rem(me + d, n)}) for d in range(1, n)]


def finish(copies):
    for copy in copies:
        copy.wait()


def total(recv):
    result = recv[0]
    for s in range(1, recv.shape[0]):
        result = result + recv[s]
    return result


def total_blocks(full, n):
    chunk = full.shape[0] // n
    result = full[0:chunk, :]
    for s in range(1, n):
        result = result + full[s * chunk : (s + 1) * chunk, :]
    return result


class Twin:
    def __init__(self, col):
        self.count = col // 2
        me = lax.axis_index("col")
        self.core = lax.rem(me, 2)
        self.chip = me // 2
        self.partner = {"col": self.chip * 2 + 1 - self.core}
        self.others = [
            {"col": lax.rem(self.chip + d, self.count) * 2 + self.core}
            for d in range(1, self.count)
        ]


def halves_out(twin, gram, recv, sems):
    half = gram.shape[0] // 2
    return [send(gram.at[span(1 - twin.core, half), :], recv, sems, 0, twin.partner)]


def halves_across(twin, gram, recv, across, sems):
    half = gram.shape[0] // 2
    across[twin.chip] = gram[span(twin.core, half), :] + recv[...]
    here = across.at[twin.chip]
    return [send(here, here, sems, d, peer) for d, peer in enumerate(twin.others)]


def halves_back(twin, full, sems):
    half = full.shape[0] // 2
    mine = full.at[span(twin.core, half), :]
    return [send(mine, mine, sems, 0, twin.partner)]


def layout(sizes, frames, own_first, own_second, rank):
    row, col = sizes["row"], sizes["col"]
    square = (rank, rank)
    half = rank // 2
    chips = col // 2
    buffers = {
        "tens": (frames, own_first, own_second),
        "held": (frames, own_second, rank),
        "first": (own_first, rank), "second": (own_second, rank),
        "first_out": (own_first, rank), "second_out": (own_second, rank),
        "frames_out": (frames, rank), "weights_out": (8, rank),
        "inv": square, "sums": (frames, rank),
        "gram_a": square, "recv_a": (row, half // row, rank), "full_a": square,
        "gram_b": square, "recv_b": (half, rank), "across_b": (chips, half, rank),
        "full_b": square,
        "terms_f": (own_first, rank), "recv_f": (col, own_first // col, rank),
        "full_f": (own_first, rank), "parts_w": (row, 8, rank),
    }
    axes = {
        "a": row, "a2": row, "a3": 2, "b": 2, "b2": chips, "b3": 2, "f": col, "f2": col,
        "w": row,
    }
    for p in range(PASSES):
        buffers.update({
            "parts_r%d" % p: (row * frames, rank), "parts_c%d" % p: (col * frames, rank),
            "raw_s%d" % p: (own_second, rank),
            "gram_g%d" % p: square, "recv_g%d" % p: (half, rank),
            "across_g%d" % p: (chips, half, rank), "full_g%d" % p: square,
        })
        axes.update({
            "r%d" % p: row, "c%d" % p: col, "g%d" % p: 2, "h%d" % p: chips, "i%d" % p: 2,
        })
        for q in range(rank // LANES):
            buffers.update({
                "terms_s%d%d" % (p, q): (own_second, LANES),
                "recv_s%d%d" % (p, q): (row, own_second // row, LANES),
                "full_s%d%d" % (p, q): (own_second, LANES),
            })
            axes.update({"s%d%d" % (p, q): row, "t%d%d" % (p, q): row})
    names = list(buffers) + ["sem_" + name for name in axes] + ["sem_load", "sem_move"]
    shapes = [pltpu.VMEM(shape, jnp.float32) for shape in buffers.values()]
    shapes += [pltpu.SemaphoreType.DMA((2, max(n - 1, 1))) for n in axes.values()]
    shapes += [pltpu.SemaphoreType.DMA((frames // math.gcd(frames, GROUP),))]
    shapes += [pltpu.SemaphoreType.DMA((6,))]
    return names, shapes


def kernel(sizes, names, tensor, first_in, second_in, first_to, second_to, frames_to, weights_to, *scratch):
    row, col = sizes["row"], sizes["col"]
    v = dict(zip(names, scratch))
    inv, sums, tens, held = v["inv"], v["sums"], v["tens"], v["held"]
    first, second, frames_out, weights_out = v["first"], v["second"], v["frames_out"], v["weights_out"]
    first_out, second_out = v["first_out"], v["second_out"]
    frames, own_first, own_second = tensor.shape
    rank = first.shape[1]
    half = rank // 2
    tiles = rank // LANES
    rows_first, rows_second = own_first * row, own_second * col
    steps = rank // PIVOTS
    twin = Twin(col)

    group = math.gcd(frames, GROUP)
    loads = frames // group

    def load(g):
        block = pl.ds(g * group, group)
        return pltpu.make_async_copy(tensor.at[block], tens.at[block], v["sem_load"].at[g])

    def move(source, target, at):
        copy = pltpu.make_async_copy(source, target, v["sem_move"].at[at])
        copy.start()
        return copy

    def contract(start, stop):
        def step(g, carry):
            load(g).wait()
            ks = [g * group + u for u in range(group)]
            parts = [cross(tens[k], first[...], HIGH) for k in ks]
            for k, part in zip(ks, parts):
                held[k] = part
                sums[pl.ds(k, 1), :] = jnp.sum(part * second[...], axis=0, keepdims=True)
            return carry

        lax.fori_loop(start, stop, step, 0)

    def frame_terms(raw, start, stop):
        def step(k, carry):
            sums[pl.ds(k, 1), :] = jnp.sum(held[k] * raw[...], axis=0, keepdims=True)
            return carry

        lax.fori_loop(start, stop, step, 0, unroll=4)

    def second_terms(out, q):
        block = math.gcd(own_second, 128)
        here = slice(q * LANES, (q + 1) * LANES)
        for c in range(0, own_second, block):
            def step(k, total):
                return total + held[k, c : c + block, here] * frames_out[pl.ds(k, 1), :][:, here]

            out[c : c + block, :] = lax.fori_loop(
                0, frames, step, jnp.zeros((block, LANES), jnp.float32), unroll=4
            )

    def first_terms(raw, start, stop):
        group = math.gcd(stop - start, 4)

        def step(g, carry):
            base = start + g * group
            stacked = tens[pl.ds(base, group)].reshape(group * own_first, own_second)
            part = product(stacked, raw[...], HIGH)
            v["terms_f"][...] += sum(
                part[u * own_first : (u + 1) * own_first, :] * frames_out[pl.ds(base + u, 1), :]
                for u in range(group)
            )
            return carry

        lax.fori_loop(0, (stop - start) // group, step, 0)

    def solve_frames(frame_sums):
        raw = product(frame_sums, inv[...]) * (1.0 / math.sqrt(rows_first * rows_second))
        normed = raw / jnp.sqrt(jnp.mean(raw * raw, axis=0, keepdims=True) + epsilon)
        frames_out[...] = normed
        return cross(normed, normed) / frames

    greet(sizes)
    come = [move(first_in, first, 0), move(second_in, second, 1)]
    for g in range(loads):
        load(g).start()
    come[0].wait()
    v["gram_a"][...] = cross(first[...], first[...], HIGH)
    come[1].wait()
    v["gram_b"][...] = cross(second[...], second[...], HIGH)
    contract(0, loads // 4)
    greeted(sizes)
    offset = twin.core * half
    go_a = scatter("row", row, v["gram_a"], v["recv_a"], v["sem_a"], offset)
    go_b = halves_out(twin, v["gram_b"], v["recv_b"], v["sem_b"])
    contract(loads // 4, loads * 5 // 8)
    finish(go_b)
    go_b = halves_across(twin, v["gram_b"], v["recv_b"], v["across_b"], v["sem_b2"])
    finish(go_a)
    go_a = gather("row", row, total(v["recv_a"]), v["full_a"], v["sem_a2"], offset)
    contract(loads * 5 // 8, loads)
    go_r = gather("row", row, sums[...], v["parts_r0"], v["sem_r0"])
    finish(go_b)
    v["full_b"][span(twin.core, half), :] = total(v["across_b"])
    go_b = halves_back(twin, v["full_b"], v["sem_b3"])
    finish(go_a)
    go_a = halves_back(twin, v["full_a"], v["sem_a3"])
    finish(go_b)
    finish(go_a)
    first_gram = v["gram_a"]
    first_gram[...] = v["full_a"][...] * (1.0 / rows_first)
    second_gram = v["full_b"][...] * (1.0 / rows_second)
    wide = None
    for p in range(PASSES):
        here = str(p)
        split_at = 0 if p == 0 else steps // 2
        inv[...] = first_gram[...] * second_gram
        invert(inv, 0, split_at)
        finish(go_r)
        go_c = gather(
            "col", col, total_blocks(v["parts_r" + here], row), v["parts_c" + here],
            v["sem_c" + here],
        )
        invert(inv, split_at, steps)
        finish(go_c)
        frame_sums = total_blocks(v["parts_c" + here], col)
        if wide is not None:
            frame_sums = frame_sums / wide
        frame_gram = solve_frames(frame_sums)
        parts = [here + str(q) for q in range(tiles)]
        go_s = []
        for q, part in enumerate(parts):
            second_terms(v["terms_s" + part], q)
            go_s.append(scatter(
                "row", row, v["terms_s" + part], v["recv_s" + part], v["sem_s" + part]
            ))
        inv[...] = first_gram[...] * frame_gram
        go_t = []
        at = 0
        for q, part in enumerate(parts):
            invert(inv, at, steps * (5 + 2 * q) // 8)
            at = steps * (5 + 2 * q) // 8
            finish(go_s[q])
            go_t.append(gather(
                "row", row, total(v["recv_s" + part]), v["full_s" + part], v["sem_t" + part]
            ))
        invert(inv, at, steps)
        for copies in go_t:
            finish(copies)
        raw = v["raw_s" + here]
        summed = jnp.concatenate([v["full_s" + part][...] for part in parts], axis=1)
        raw[...] = product(summed, inv[...], HIGH) * (1.0 / math.sqrt(rows_first * frames))
        gram_g, recv_g, across_g, full_g = (
            v[name + here] for name in ("gram_g", "recv_g", "across_g", "full_g")
        )
        gram_g[...] = cross(raw[...], raw[...], HIGH)
        go_g = halves_out(twin, gram_g, recv_g, v["sem_g" + here])
        last = p + 1 == PASSES
        if last:
            v["terms_f"][...] = jnp.zeros((own_first, rank), jnp.float32)
            first_terms(raw, 0, frames // 4)
        else:
            later = str(p + 1)
            frame_terms(raw, 0, frames // 2)
        finish(go_g)
        go_g = halves_across(twin, gram_g, recv_g, across_g, v["sem_h" + here])
        if last:
            first_terms(raw, frames // 4, frames)
        else:
            frame_terms(raw, frames // 2, frames)
            go_r = gather("row", row, sums[...], v["parts_r" + later], v["sem_r" + later])
        finish(go_g)
        full_g[span(twin.core, half), :] = total(across_g)
        go_g = halves_back(twin, full_g, v["sem_i" + here])
        if last:
            go_f = scatter("col", col, v["terms_f"], v["recv_f"], v["sem_f"])
        finish(go_g)
        gram = full_g[...] * (1.0 / rows_second)
        down = lax.broadcasted_iota(jnp.int32, (rank, rank), 0)
        across = lax.broadcasted_iota(jnp.int32, (rank, rank), 1)
        diagonal = jnp.where(down == across, gram, 0.0)
        wide = jnp.sqrt(jnp.sum(diagonal, axis=0, keepdims=True) + epsilon)
        tall = jnp.sqrt(jnp.sum(diagonal, axis=1, keepdims=True) + epsilon)
        second_gram = gram / wide / tall
    inv[...] = second_gram * frame_gram
    second_out[...] = raw[...] / wide
    gone = [move(second_out, second_to, 2), move(frames_out, frames_to, 3)]
    invert(inv, 0, steps // 4)
    finish(go_f)
    go_f = gather("col", col, total(v["recv_f"]), v["full_f"], v["sem_f2"])
    invert(inv, steps // 4, steps)
    finish(go_f)
    raw = product(v["full_f"][...] / wide, inv[...]) * (1.0 / math.sqrt(rows_second * frames))
    squares = jnp.sum(raw * raw, axis=0, keepdims=True)
    go_w = spread("row", row, squares, v["parts_w"], v["sem_w"])
    first_out[...] = raw
    finish(go_w)
    weights = jnp.sqrt(total(v["parts_w"])[0:1, :] * (1.0 / rows_first) + epsilon)
    weights_out[...] = jnp.broadcast_to(weights, weights_out.shape)
    gone.append(move(weights_out, weights_to, 4))
    first_out[...] = first_out[...] / weights
    gone.append(move(first_out, first_to, 5))
    finish(gone)


def body(sizes, tensor, initial_first, initial_second):
    frames, own_first, own_second = tensor.shape
    rank = initial_first.shape[1]
    names, scratch = layout(sizes, frames, own_first, own_second, rank)
    anywhere = pl.BlockSpec(memory_space=pl.ANY)
    outs = ((own_first, rank), (own_second, rank), (frames, rank), (8, rank))
    factor_first, second, factor_frames, weights = pl.pallas_call(
        functools.partial(kernel, sizes, names),
        out_shape=[jax.ShapeDtypeStruct(shape, jnp.float32) for shape in outs],
        in_specs=[anywhere] * 3,
        out_specs=[anywhere] * len(outs),
        scratch_shapes=scratch,
        compiler_params=pltpu.CompilerParams(
            collective_id=0, has_side_effects=True, vmem_limit_bytes=67043328
        ),
        name="als",
    )(tensor, initial_first, initial_second)
    return (factor_first, second, factor_frames, weights[0])


def solution(mesh):
    sizes = {"row": mesh.shape["row"], "col": mesh.shape["col"]}
    placed = (P(None, "row", "col"), P("row", None), P("col", None))
    return jax.shard_map(
        functools.partial(body, sizes),
        mesh=mesh,
        in_specs=placed,
        out_specs=(P("row", None), P("col", None), P(), P()),
        check_vma=False,
    )
```

```python
import functools
import math

import jax
import jax.numpy as jnp
from jax import lax
from jax.experimental import pallas as pl
from jax.experimental.pallas import tpu as pltpu
from jax.sharding import PartitionSpec as P

PASSES = 2
LANES = 128
PIVOTS = 16
GROUP = 4
CUTS = 2
MESH = pl.DeviceIdType.MESH
HIGHEST = lax.Precision.HIGHEST
HIGH = lax.Precision.HIGH

epsilon = 1e-06


def product(a, b, precision=HIGHEST):
    return jnp.dot(a, b, precision=precision, preferred_element_type=jnp.float32)


def cross(a, b, precision=HIGHEST):
    return lax.dot_general(
        a, b, (((0,), (0,)), ((), ())), precision=precision, preferred_element_type=jnp.float32
    )


def split(x):
    high = x.astype(jnp.bfloat16)
    rest = x - high.astype(jnp.float32)
    mid = rest.astype(jnp.bfloat16)
    return high, mid, (rest - mid.astype(jnp.float32)).astype(jnp.bfloat16)


def outer(left, right):
    h, m, l = split(left)
    hh, mm, ll = split(right)
    return lax.dot_general(
        jnp.concatenate([h, h, m, h, m, l], axis=0),
        jnp.concatenate([hh, mm, hh, ll, mm, hh], axis=0),
        (((0,), (0,)), ((), ())), preferred_element_type=jnp.float32,
    )


def invert(a, start, stop):
    size = a.shape[0]
    tiles = size // LANES
    row = lax.broadcasted_iota(jnp.int32, (PIVOTS, LANES), 0)
    lanes = [
        lax.broadcasted_iota(jnp.int32, (PIVOTS, LANES), 1) + q * LANES for q in range(tiles)
    ]
    wide = lax.broadcasted_iota(jnp.int32, (PIVOTS, size), 1)
    whole = lax.broadcasted_iota(jnp.int32, (size, size), 1)

    def step(g, carry):
        base = g * PIVOTS
        here = pl.ds(pl.multiple_of(base, PIVOTS), PIVOTS)
        rows = [a[here, q * LANES : (q + 1) * LANES] for q in range(tiles)]
        cols = []
        for t in range(PIVOTS):
            picked = sum(jnp.where(lanes[q] == base + t, rows[q], 0.0) for q in range(tiles))
            cols.append(
                jnp.broadcast_to(jnp.sum(picked, axis=1, keepdims=True), (PIVOTS, LANES))
            )
        work = []
        for q in range(tiles):
            place = lanes[q] - base
            inside = (place >= 0) & (place < PIVOTS)
            unit = jnp.where(place == row, 1.0, 0.0)
            work.append(jnp.where(inside, unit, rows[q]))
        for t in range(PIVOTS):
            pivot = 1.0 / jnp.broadcast_to(cols[t][t : t + 1, :], (PIVOTS, LANES))
            at = row == t

            def reduced(x):
                scaled = jnp.broadcast_to(x[t : t + 1, :], (PIVOTS, LANES)) * pivot
                return jnp.where(at, scaled, x - cols[t] * scaled)

            later = [reduced(cols[s]) for s in range(t + 1, PIVOTS)]
            work = [reduced(w) for w in work]
            cols[t + 1 :] = later
        solved = jnp.concatenate(work, axis=1)
        raw = a[here, :]
        inside = (wide >= base) & (wide < base + PIVOTS)
        left = jnp.where(inside, 0.0, jnp.where(wide < base, -raw, raw))
        kept = jnp.where((whole >= base) & (whole < base + PIVOTS), 0.0, a[...])
        a[...] = kept - outer(left, solved)
        a[here, :] = solved
        return carry

    lax.fori_loop(start, stop, step, 0)


def greet(sizes):
    barrier = pltpu.get_barrier_semaphore()
    for axis, n in sizes.items():
        me = lax.axis_index(axis)
        for d in range(1, n):
            pl.semaphore_signal(
                barrier, inc=1, device_id={axis: lax.rem(me + d, n)}, device_id_type=MESH
            )


def greeted(sizes):
    pl.semaphore_wait(pltpu.get_barrier_semaphore(), sum(n - 1 for n in sizes.values()))


def send(source, target, sems, at, device):
    copy = pltpu.make_async_remote_copy(
        src_ref=source, dst_ref=target, send_sem=sems.at[0, at], recv_sem=sems.at[1, at],
        device_id=device, device_id_type=MESH,
    )
    copy.start()
    return copy


def span(index, chunk):
    return pl.ds(pl.multiple_of(index * chunk, 8), chunk)


def scatter(axis, n, source, recv, sems, offset=0):
    me = lax.axis_index(axis)
    chunk = recv.shape[1]
    copies = []
    for d in range(1, n):
        peer = lax.rem(me + d, n)
        there = pl.ds(pl.multiple_of(offset + peer * chunk, 8), chunk)
        copies.append(send(source.at[there, :], recv.at[me], sems, d - 1, {axis: peer}))
    recv[me] = source[pl.ds(pl.multiple_of(offset + me * chunk, 8), chunk), :]
    return copies


def gather(axis, n, own, full, sems, offset=0):
    me = lax.axis_index(axis)
    chunk = own.shape[0]
    place = pl.ds(pl.multiple_of(offset + me * chunk, 8), chunk)
    full[place, :] = own
    return [
        send(full.at[place, :], full.at[place, :], sems, d - 1, {axis: lax.rem(me + d, n)})
        for d in range(1, n)
    ]


def spread(axis, n, line, parts, sems):
    me = lax.axis_index(axis)
    here = parts.at[me, pl.ds(0, 1), :]
    parts[me, 0:1, :] = line
    return [send(here, here, sems, d - 1, {axis: lax.rem(me + d, n)}) for d in range(1, n)]


def scatter_piece(n, cut, source, recv, sems):
    me = lax.axis_index("row")
    chunk = recv.shape[1]
    small = chunk // CUTS
    inside = pl.ds(cut * small, small)
    copies = []
    for d in range(1, n):
        peer = lax.rem(me + d, n)
        there = pl.ds(pl.multiple_of(peer * chunk + cut * small, 8), small)
        copies.append(send(
            source.at[there, :], recv.at[me, inside, :], sems, cut * (n - 1) + d - 1,
            {"row": peer},
        ))
    recv[me, cut * small : (cut + 1) * small, :] = source[
        pl.ds(pl.multiple_of(me * chunk + cut * small, 8), small), :
    ]
    return copies


def gather_piece(n, cut, recv, full, sems):
    me = lax.axis_index("row")
    chunk = recv.shape[1]
    small = chunk // CUTS
    inside = slice(cut * small, (cut + 1) * small)
    place = pl.ds(pl.multiple_of(me * chunk + cut * small, 8), small)
    full[place, :] = total(recv[:, inside, :])
    return [
        send(
            full.at[place, :], full.at[place, :], sems, cut * (n - 1) + d - 1,
            {"row": lax.rem(me + d, n)},
        )
        for d in range(1, n)
    ]


def lots_out(sums, lots, recv, sems):
    n, few = lots.shape[:2]
    me = lax.axis_index("row")
    for d in range(n):
        lots[d] = sums[d * few : (d + 1) * few, :]
    recv[me] = lots[me]
    return [
        send(lots.at[peer], recv.at[me], sems, d, {"row": peer})
        for d, peer in enumerate(lax.rem(me + e, n) for e in range(1, n))
    ]


def lots_share(axis, n, own, full, sems):
    me = lax.axis_index(axis)
    full[me] = own
    return [
        send(full.at[me], full.at[me], sems, d - 1, {axis: lax.rem(me + d, n)})
        for d in range(1, n)
    ]


def finish(copies):
    for copy in copies:
        copy.wait()


def total(recv):
    result = recv[0]
    for s in range(1, recv.shape[0]):
        result = result + recv[s]
    return result


def total_blocks(full, n):
    chunk = full.shape[0] // n
    result = full[0:chunk, :]
    for s in range(1, n):
        result = result + full[s * chunk : (s + 1) * chunk, :]
    return result


class Twin:
    def __init__(self, col):
        self.count = col // 2
        me = lax.axis_index("col")
        self.core = lax.rem(me, 2)
        self.chip = me // 2
        self.partner = {"col": self.chip * 2 + 1 - self.core}
        self.others = [
            {"col": lax.rem(self.chip + d, self.count) * 2 + self.core}
            for d in range(1, self.count)
        ]


def halves_out(twin, gram, recv, sems):
    half = gram.shape[0] // 2
    return [send(gram.at[span(1 - twin.core, half), :], recv, sems, 0, twin.partner)]


def halves_across(twin, gram, recv, across, sems):
    half = gram.shape[0] // 2
    across[twin.chip] = gram[span(twin.core, half), :] + recv[...]
    here = across.at[twin.chip]
    return [send(here, here, sems, d, peer) for d, peer in enumerate(twin.others)]


def halves_back(twin, full, sems):
    half = full.shape[0] // 2
    mine = full.at[span(twin.core, half), :]
    return [send(mine, mine, sems, 0, twin.partner)]


def layout(sizes, frames, own_first, own_second, rank):
    row, col = sizes["row"], sizes["col"]
    square = (rank, rank)
    half = rank // 2
    chips = col // 2
    few = frames // row
    pieces = CUTS * (row - 1) + 1
    buffers = {
        "tens": (frames, own_first, own_second),
        "held": (frames, own_second, rank),
        "first": (own_first, rank), "second": (own_second, rank),
        "inv": square, "sums": (frames, rank),
        "gram_a": square, "recv_a": (row, half // row, rank), "full_a": square,
        "gram_b": square, "recv_b": (half, rank), "across_b": (chips, half, rank),
        "full_b": square,
        "terms_f": (own_first, rank), "recv_f": (col, own_first // col, rank),
        "full_f": (own_first, rank), "parts_w": (row, 8, rank),
    }
    axes = {
        "a": row, "a2": row, "a3": 2, "b": 2, "b2": chips, "b3": 2, "f": col, "f2": col,
        "w": row,
    }
    for p in range(PASSES):
        buffers.update({
            "lots_r%d" % p: (row, few, rank), "recv_r%d" % p: (row, few, rank),
            "parts_c%d" % p: (col, few, rank), "full_r%d" % p: (row, few, rank),
            "raw_s%d" % p: (own_second, rank),
            "gram_g%d" % p: square, "recv_g%d" % p: (half, rank),
            "across_g%d" % p: (chips, half, rank), "full_g%d" % p: square,
        })
        axes.update({
            "r%d" % p: row, "c%d" % p: col, "d%d" % p: row, "g%d" % p: 2, "h%d" % p: chips, "i%d" % p: 2,
        })
        for q in range(rank // LANES):
            buffers.update({
                "terms_s%d%d" % (p, q): (own_second, LANES),
                "recv_s%d%d" % (p, q): (row, own_second // row, LANES),
                "full_s%d%d" % (p, q): (own_second, LANES),
            })
            axes.update({"s%d%d" % (p, q): pieces, "t%d%d" % (p, q): pieces})
    names = list(buffers) + ["sem_" + name for name in axes] + ["sem_load", "sem_move"]
    shapes = [pltpu.VMEM(shape, jnp.float32) for shape in buffers.values()]
    shapes += [pltpu.SemaphoreType.DMA((2, max(n - 1, 1))) for n in axes.values()]
    shapes += [pltpu.SemaphoreType.DMA((frames // math.gcd(frames, GROUP),))]
    shapes += [pltpu.SemaphoreType.DMA((2,))]
    return names, shapes


def kernel(sizes, names, tensor, first_in, second_in, first_out, second_out, frames_out, weights_out, *scratch):
    row, col = sizes["row"], sizes["col"]
    v = dict(zip(names, scratch))
    inv, sums, tens, held = v["inv"], v["sums"], v["tens"], v["held"]
    first, second = v["first"], v["second"]
    frames, own_first, own_second = tensor.shape
    rank = first.shape[1]
    half = rank // 2
    tiles = rank // LANES
    rows_first, rows_second = own_first * row, own_second * col
    steps = rank // PIVOTS
    twin = Twin(col)

    group = math.gcd(frames, GROUP)
    loads = frames // group

    def load(g):
        block = pl.ds(g * group, group)
        return pltpu.make_async_copy(tensor.at[block], tens.at[block], v["sem_load"].at[g])

    def move(source, target, at):
        copy = pltpu.make_async_copy(source, target, v["sem_move"].at[at])
        copy.start()
        return copy

    def contract(start, stop):
        def step(g, carry):
            load(g).wait()
            ks = [g * group + u for u in range(group)]
            parts = [cross(tens[k], first[...], HIGH) for k in ks]
            for k, part in zip(ks, parts):
                held[k] = part
                sums[pl.ds(k, 1), :] = jnp.sum(part * second[...], axis=0, keepdims=True)
            return carry

        lax.fori_loop(start, stop, step, 0)

    def frame_terms(raw, start, stop):
        def step(k, carry):
            sums[pl.ds(k, 1), :] = jnp.sum(held[k] * raw[...], axis=0, keepdims=True)
            return carry

        lax.fori_loop(start, stop, step, 0, unroll=4)

    def second_terms(out, q):
        block = math.gcd(own_second, 128)
        here = slice(q * LANES, (q + 1) * LANES)
        for c in range(0, own_second, block):
            def step(k, total):
                return total + held[k, c : c + block, here] * frames_out[pl.ds(k, 1), :][:, here]

            out[c : c + block, :] = lax.fori_loop(
                0, frames, step, jnp.zeros((block, LANES), jnp.float32), unroll=4
            )

    def first_terms(raw, start, stop):
        group = math.gcd(stop - start, 4)

        def step(g, carry):
            base = start + g * group
            stacked = tens[pl.ds(base, group)].reshape(group * own_first, own_second)
            part = product(stacked, raw[...], HIGH)
            v["terms_f"][...] += sum(
                part[u * own_first : (u + 1) * own_first, :] * frames_out[pl.ds(base + u, 1), :]
                for u in range(group)
            )
            return carry

        lax.fori_loop(0, (stop - start) // group, step, 0)

    def frames_across(name):
        return lots_share(
            "col", col, total(v["recv_r" + name]), v["parts_c" + name], v["sem_c" + name]
        )

    def frames_back(name):
        return lots_share(
            "row", row, total(v["parts_c" + name]), v["full_r" + name], v["sem_d" + name]
        )

    def solve_frames(frame_sums):
        raw = product(frame_sums, inv[...]) * (1.0 / math.sqrt(rows_first * rows_second))
        normed = raw / jnp.sqrt(jnp.mean(raw * raw, axis=0, keepdims=True) + epsilon)
        frames_out[...] = normed
        return cross(normed, normed) / frames

    greet(sizes)
    come = [move(first_in, first, 0), move(second_in, second, 1)]
    for g in range(loads):
        load(g).start()
    come[0].wait()
    v["gram_a"][...] = cross(first[...], first[...], HIGH)
    come[1].wait()
    v["gram_b"][...] = cross(second[...], second[...], HIGH)
    contract(0, loads * 5 // 8)
    greeted(sizes)
    offset = twin.core * half
    go_a = scatter("row", row, v["gram_a"], v["recv_a"], v["sem_a"], offset)
    go_b = halves_out(twin, v["gram_b"], v["recv_b"], v["sem_b"])
    contract(loads * 5 // 8, loads)
    go_r = lots_out(sums, v["lots_r0"], v["recv_r0"], v["sem_r0"])
    finish(go_b)
    go_b = halves_across(twin, v["gram_b"], v["recv_b"], v["across_b"], v["sem_b2"])
    finish(go_a)
    go_a = gather("row", row, total(v["recv_a"]), v["full_a"], v["sem_a2"], offset)
    finish(go_r)
    go_c = frames_across("0")
    finish(go_b)
    v["full_b"][span(twin.core, half), :] = total(v["across_b"])
    go_b = halves_back(twin, v["full_b"], v["sem_b3"])
    finish(go_a)
    go_a = halves_back(twin, v["full_a"], v["sem_a3"])
    finish(go_c)
    go_d = frames_back("0")
    finish(go_b)
    finish(go_a)
    first_gram = v["gram_a"]
    first_gram[...] = v["full_a"][...] * (1.0 / rows_first)
    second_gram = v["full_b"][...] * (1.0 / rows_second)
    wide = None
    for p in range(PASSES):
        here = str(p)
        inv[...] = first_gram[...] * second_gram
        at = 0
        if p > 0:
            at = steps // 4
            invert(inv, 0, at)
            finish(go_c)
            go_d = frames_back(here)
        invert(inv, at, steps)
        finish(go_d)
        full_r = v["full_r" + here]
        frame_sums = jnp.concatenate([full_r[d] for d in range(row)], axis=0)
        if wide is not None:
            frame_sums = frame_sums / wide
        frame_gram = solve_frames(frame_sums)
        parts = [here + str(q) for q in range(tiles)]
        pieces = [(part, cut) for part in parts for cut in range(CUTS)]
        go_s = []
        for q, part in enumerate(parts):
            second_terms(v["terms_s" + part], q)
            for cut in range(CUTS):
                go_s.append(scatter_piece(
                    row, cut, v["terms_s" + part], v["recv_s" + part], v["sem_s" + part]
                ))
        inv[...] = first_gram[...] * frame_gram
        go_t = []
        at = 0
        for q, (part, cut) in enumerate(pieces):
            until = min(steps, steps * 5 // 8 + q * steps // (2 * len(pieces)))
            invert(inv, at, until)
            at = until
            finish(go_s[q])
            go_t.append(gather_piece(
                row, cut, v["recv_s" + part], v["full_s" + part], v["sem_t" + part]
            ))
        invert(inv, at, steps)
        for copies in go_t:
            finish(copies)
        raw = v["raw_s" + here]
        summed = jnp.concatenate([v["full_s" + part][...] for part in parts], axis=1)
        raw[...] = product(summed, inv[...], HIGH) * (1.0 / math.sqrt(rows_first * frames))
        gram_g, recv_g, across_g, full_g = (
            v[name + here] for name in ("gram_g", "recv_g", "across_g", "full_g")
        )
        gram_g[...] = cross(raw[...], raw[...], HIGH)
        go_g = halves_out(twin, gram_g, recv_g, v["sem_g" + here])
        last = p + 1 == PASSES
        if last:
            v["terms_f"][...] = jnp.zeros((own_first, rank), jnp.float32)
            first_terms(raw, 0, frames // 4)
        else:
            later = str(p + 1)
            frame_terms(raw, 0, frames // 2)
        finish(go_g)
        go_g = halves_across(twin, gram_g, recv_g, across_g, v["sem_h" + here])
        if last:
            first_terms(raw, frames // 4, frames)
        else:
            frame_terms(raw, frames // 2, frames)
            go_r = lots_out(sums, v["lots_r" + later], v["recv_r" + later], v["sem_r" + later])
        finish(go_g)
        if not last:
            finish(go_r)
            go_c = frames_across(later)
        full_g[span(twin.core, half), :] = total(across_g)
        go_g = halves_back(twin, full_g, v["sem_i" + here])
        if last:
            go_f = scatter("col", col, v["terms_f"], v["recv_f"], v["sem_f"])
        finish(go_g)
        gram = full_g[...] * (1.0 / rows_second)
        down = lax.broadcasted_iota(jnp.int32, (rank, rank), 0)
        across = lax.broadcasted_iota(jnp.int32, (rank, rank), 1)
        diagonal = jnp.where(down == across, gram, 0.0)
        wide = jnp.sqrt(jnp.sum(diagonal, axis=0, keepdims=True) + epsilon)
        tall = jnp.sqrt(jnp.sum(diagonal, axis=1, keepdims=True) + epsilon)
        second_gram = gram / wide / tall
    inv[...] = second_gram * frame_gram
    second_out[...] = raw[...] / wide
    invert(inv, 0, steps // 4)
    finish(go_f)
    go_f = gather("col", col, total(v["recv_f"]), v["full_f"], v["sem_f2"])
    invert(inv, steps // 4, steps)
    finish(go_f)
    raw = product(v["full_f"][...] / wide, inv[...]) * (1.0 / math.sqrt(rows_second * frames))
    squares = jnp.sum(raw * raw, axis=0, keepdims=True)
    go_w = spread("row", row, squares, v["parts_w"], v["sem_w"])
    first_out[...] = raw
    finish(go_w)
    weights = jnp.sqrt(total(v["parts_w"])[0:1, :] * (1.0 / rows_first) + epsilon)
    weights_out[...] = weights
    first_out[...] = first_out[...] / weights


def deliver(*refs):
    half = len(refs) // 2
    sems = refs[-1]
    copies = [
        pltpu.make_async_copy(source, target, sems.at[k])
        for k, (source, target) in enumerate(zip(refs[:half], refs[half : 2 * half]))
    ]
    for copy in copies:
        copy.start()
    for copy in copies:
        copy.wait()


def body(sizes, tensor, initial_first, initial_second):
    frames, own_first, own_second = tensor.shape
    rank = initial_first.shape[1]
    names, scratch = layout(sizes, frames, own_first, own_second, rank)
    far = pl.BlockSpec(memory_space=pltpu.HBM)
    near = pl.BlockSpec(memory_space=pltpu.VMEM)
    outs = ((own_first, rank), (own_second, rank), (frames, rank), (1, rank))
    shapes = [jax.ShapeDtypeStruct(shape, jnp.float32) for shape in outs]
    results = pl.pallas_call(
        functools.partial(kernel, sizes, names),
        out_shape=shapes,
        in_specs=[far] * 3,
        out_specs=[near] * len(outs),
        scratch_shapes=scratch,
        compiler_params=pltpu.CompilerParams(
            collective_id=0, has_side_effects=True, vmem_limit_bytes=48 * 1024 * 1024
        ),
        name="als",
    )(*[
        pltpu.with_memory_space_constraint(x, pltpu.HBM)
        for x in (tensor, initial_first, initial_second)
    ])
    results = pl.pallas_call(
        deliver,
        out_shape=shapes,
        in_specs=[near] * len(outs),
        out_specs=[far] * len(outs),
        scratch_shapes=[pltpu.SemaphoreType.DMA((len(outs),))],
        compiler_params=pltpu.CompilerParams(vmem_limit_bytes=1024 * 1024),
        name="deliver",
    )(*results)
    factor_first, second, factor_frames, weights = results
    return (factor_first, second, factor_frames, weights.reshape(rank))


def solution(mesh):
    sizes = {"row": mesh.shape["row"], "col": mesh.shape["col"]}
    placed = (P(None, "row", "col"), P("row", None), P("col", None))
    return jax.shard_map(
        functools.partial(body, sizes),
        mesh=mesh,
        in_specs=placed,
        out_specs=(P("row", None), P("col", None), P(), P()),
        check_vma=False,
    )
```

```python
import functools
import math

import jax
import jax.numpy as jnp
from jax import lax
from jax.experimental import pallas as pl
from jax.experimental.pallas import tpu as pltpu
from jax.sharding import PartitionSpec as P

PASSES = 2
LANES = 128
PIVOTS = 16
GROUP = 4
CUTS = 2
MESH = pl.DeviceIdType.MESH
HIGHEST = lax.Precision.HIGHEST
HIGH = lax.Precision.HIGH

epsilon = 1e-06


def product(a, b, precision=HIGHEST):
    return jnp.dot(a, b, precision=precision, preferred_element_type=jnp.float32)


def cross(a, b, precision=HIGHEST):
    return lax.dot_general(
        a, b, (((0,), (0,)), ((), ())), precision=precision, preferred_element_type=jnp.float32
    )


def split(x):
    high = x.astype(jnp.bfloat16)
    rest = x - high.astype(jnp.float32)
    mid = rest.astype(jnp.bfloat16)
    return high, mid, (rest - mid.astype(jnp.float32)).astype(jnp.bfloat16)


def stacked(solved):
    h, m, l = split(solved[...])
    return jnp.concatenate([h, m, h, l, m, h], axis=0)


def update(left, right):
    return jnp.dot(left, right, preferred_element_type=jnp.float32)


def begin(a, panel, solved, left):
    panel[...] = a[0:PIVOTS, :]
    solved[...] = jnp.zeros_like(solved)
    left[...] = jnp.zeros_like(left)


def flush(a, panel, solved, left):
    a[...] = a[...] - update(left[...], stacked(solved))
    a[a.shape[0] - PIVOTS :, :] = solved[...]


def invert(a, panel, solved, left, start, stop):
    size = a.shape[0]
    tiles = size // LANES
    each = LANES // PIVOTS
    row = lax.broadcasted_iota(jnp.int32, (PIVOTS, LANES), 0)
    lane = lax.broadcasted_iota(jnp.int32, (PIVOTS, LANES), 1)
    across = lax.broadcasted_iota(jnp.int32, (size, LANES), 1)
    parts = [slice(q * LANES, (q + 1) * LANES) for q in range(tiles)]

    def line(x, t):
        return jnp.broadcast_to(x[t : t + 1, :], (PIVOTS, LANES))

    def block(g):
        return pl.ds(pl.multiple_of(g * PIVOTS, PIVOTS), PIVOTS)

    def step(own, g, carry):
        at = g * PIVOTS - own * LANES
        place = lane - at
        inside = (place >= 0) & (place < PIVOTS)

        def columns(x):
            picked = [jnp.where(place == t, x, 0.0) for t in range(PIVOTS)]
            return [
                jnp.broadcast_to(jnp.sum(y, axis=1, keepdims=True), (PIVOTS, LANES))
                for y in picked
            ]

        rows = [panel[:, part] for part in parts]
        cols = columns(rows[own])
        right = stacked(solved)
        ahead = block(jnp.minimum(g + 1, size // PIVOTS - 1))
        stale = a[ahead, :] - update(left[ahead, :], right)
        stale = [stale[:, part] for part in parts]
        scales = columns(stale[own])
        stale[own] = jnp.where(inside, 0.0, stale[own])
        whole = update(left[...], right)
        behind = block(jnp.maximum(g - 1, 0))
        for q, part in enumerate(parts):
            kept, done = a[:, part] - whole[:, part], solved[:, part]
            if q == own:
                kept = jnp.where((across >= at) & (across < at + PIVOTS), 0.0, kept)
                done = jnp.where(inside, 0.0, done)
            a[:, part] = kept
            a[behind, part] = done
        beside = jnp.where(inside, 0.0, jnp.where(place < 0, -rows[own], rows[own]))
        h, m, l = split(
            jnp.concatenate([-x for x in rows[:own]] + [beside] + rows[own + 1 :], axis=1)
        )
        left[...] = jnp.concatenate([h, h, m, h, m, l], axis=0).T
        work = list(rows)
        work[own] = jnp.where(inside, jnp.where(place == row, 1.0, 0.0), rows[own])
        for t in range(PIVOTS):
            pivot = 1.0 / line(cols[t], t)
            factor = (cols[t] - jnp.where(row == t, 1.0, 0.0)) * pivot
            cols[t + 1 :] = [x - factor * line(x, t) for x in cols[t + 1 :]]
            work = [x - factor * line(x, t) for x in work]
        for q, part in enumerate(parts):
            fresh = stale[q]
            for t in range(PIVOTS):
                fresh = fresh - scales[t] * line(work[q], t)
            panel[:, part] = fresh
            solved[:, part] = work[q]
        return carry

    for q in range(tiles):
        low, high = max(start, q * each), min(stop, (q + 1) * each)
        if low < high:
            lax.fori_loop(low, high, functools.partial(step, q), 0)


def greet(sizes):
    barrier = pltpu.get_barrier_semaphore()
    for axis, n in sizes.items():
        me = lax.axis_index(axis)
        for d in range(1, n):
            pl.semaphore_signal(
                barrier, inc=1, device_id={axis: lax.rem(me + d, n)}, device_id_type=MESH
            )


def greeted(sizes):
    pl.semaphore_wait(pltpu.get_barrier_semaphore(), sum(n - 1 for n in sizes.values()))


def send(source, target, sems, at, device):
    copy = pltpu.make_async_remote_copy(
        src_ref=source, dst_ref=target, send_sem=sems.at[0, at], recv_sem=sems.at[1, at],
        device_id=device, device_id_type=MESH,
    )
    copy.start()
    return copy


def span(index, chunk):
    return pl.ds(pl.multiple_of(index * chunk, 8), chunk)


def scatter(axis, n, source, recv, sems, offset=0):
    me = lax.axis_index(axis)
    chunk = recv.shape[1]
    copies = []
    for d in range(1, n):
        peer = lax.rem(me + d, n)
        there = pl.ds(pl.multiple_of(offset + peer * chunk, 8), chunk)
        copies.append(send(source.at[there, :], recv.at[me], sems, d - 1, {axis: peer}))
    recv[me] = source[pl.ds(pl.multiple_of(offset + me * chunk, 8), chunk), :]
    return copies


def gather(axis, n, own, full, sems, offset=0):
    me = lax.axis_index(axis)
    chunk = own.shape[0]
    place = pl.ds(pl.multiple_of(offset + me * chunk, 8), chunk)
    full[place, :] = own
    return [
        send(full.at[place, :], full.at[place, :], sems, d - 1, {axis: lax.rem(me + d, n)})
        for d in range(1, n)
    ]


def spread(axis, n, line, parts, sems):
    me = lax.axis_index(axis)
    here = parts.at[me, pl.ds(0, 1), :]
    parts[me, 0:1, :] = line
    return [send(here, here, sems, d - 1, {axis: lax.rem(me + d, n)}) for d in range(1, n)]


def scatter_piece(n, cut, source, recv, sems):
    me = lax.axis_index("row")
    chunk = recv.shape[1]
    small = chunk // CUTS
    inside = pl.ds(cut * small, small)
    copies = []
    for d in range(1, n):
        peer = lax.rem(me + d, n)
        there = pl.ds(pl.multiple_of(peer * chunk + cut * small, 8), small)
        copies.append(send(
            source.at[there, :], recv.at[me, inside, :], sems, cut * (n - 1) + d - 1,
            {"row": peer},
        ))
    recv[me, cut * small : (cut + 1) * small, :] = source[
        pl.ds(pl.multiple_of(me * chunk + cut * small, 8), small), :
    ]
    return copies


def gather_piece(n, cut, recv, full, sems):
    me = lax.axis_index("row")
    chunk = recv.shape[1]
    small = chunk // CUTS
    inside = slice(cut * small, (cut + 1) * small)
    place = pl.ds(pl.multiple_of(me * chunk + cut * small, 8), small)
    full[place, :] = total(recv[:, inside, :])
    return [
        send(
            full.at[place, :], full.at[place, :], sems, cut * (n - 1) + d - 1,
            {"row": lax.rem(me + d, n)},
        )
        for d in range(1, n)
    ]


def lots_out(sums, lots, recv, sems):
    n, few = lots.shape[:2]
    me = lax.axis_index("row")
    for d in range(n):
        lots[d] = sums[d * few : (d + 1) * few, :]
    recv[me] = lots[me]
    return [
        send(lots.at[peer], recv.at[me], sems, d, {"row": peer})
        for d, peer in enumerate(lax.rem(me + e, n) for e in range(1, n))
    ]


def lots_share(axis, n, own, full, sems):
    me = lax.axis_index(axis)
    full[me] = own
    return [
        send(full.at[me], full.at[me], sems, d - 1, {axis: lax.rem(me + d, n)})
        for d in range(1, n)
    ]


def finish(copies):
    for copy in copies:
        copy.wait()


def total(recv):
    result = recv[0]
    for s in range(1, recv.shape[0]):
        result = result + recv[s]
    return result


def total_blocks(full, n):
    chunk = full.shape[0] // n
    result = full[0:chunk, :]
    for s in range(1, n):
        result = result + full[s * chunk : (s + 1) * chunk, :]
    return result


class Twin:
    def __init__(self, col):
        self.count = col // 2
        me = lax.axis_index("col")
        self.core = lax.rem(me, 2)
        self.chip = me // 2
        self.partner = {"col": self.chip * 2 + 1 - self.core}
        self.others = [
            {"col": lax.rem(self.chip + d, self.count) * 2 + self.core}
            for d in range(1, self.count)
        ]


def halves_out(twin, gram, recv, sems):
    half = gram.shape[0] // 2
    return [send(gram.at[span(1 - twin.core, half), :], recv, sems, 0, twin.partner)]


def halves_across(twin, gram, recv, across, sems):
    half = gram.shape[0] // 2
    across[twin.chip] = gram[span(twin.core, half), :] + recv[...]
    here = across.at[twin.chip]
    return [send(here, here, sems, d, peer) for d, peer in enumerate(twin.others)]


def halves_back(twin, full, sems):
    half = full.shape[0] // 2
    mine = full.at[span(twin.core, half), :]
    return [send(mine, mine, sems, 0, twin.partner)]


def layout(sizes, frames, own_first, own_second, rank):
    row, col = sizes["row"], sizes["col"]
    square = (rank, rank)
    half = rank // 2
    chips = col // 2
    few = frames // row
    pieces = CUTS * (row - 1) + 1
    buffers = {
        "tens": (frames, own_first, own_second),
        "held": (frames, own_second, rank),
        "first": (own_first, rank), "second": (own_second, rank),
        "inv": square, "panel": (PIVOTS, rank), "solved": (PIVOTS, rank),
        "sums": (frames, rank),
        "gram_a": square, "recv_a": (row, half // row, rank), "full_a": square,
        "gram_b": square, "recv_b": (half, rank), "across_b": (chips, half, rank),
        "full_b": square,
        "terms_f": (own_first, rank), "recv_f": (col, own_first // col, rank),
        "full_f": (own_first, rank), "parts_w": (row, 8, rank),
    }
    axes = {
        "a": row, "a2": row, "a3": 2, "b": 2, "b2": chips, "b3": 2, "f": col, "f2": col,
        "w": row,
    }
    for p in range(PASSES):
        buffers.update({
            "lots_r%d" % p: (row, few, rank), "recv_r%d" % p: (row, few, rank),
            "parts_c%d" % p: (col, few, rank), "full_r%d" % p: (row, few, rank),
            "raw_s%d" % p: (own_second, rank),
            "gram_g%d" % p: square, "recv_g%d" % p: (half, rank),
            "across_g%d" % p: (chips, half, rank), "full_g%d" % p: square,
        })
        axes.update({
            "r%d" % p: row, "c%d" % p: col, "d%d" % p: row, "g%d" % p: 2, "h%d" % p: chips, "i%d" % p: 2,
        })
        for q in range(rank // LANES):
            buffers.update({
                "terms_s%d%d" % (p, q): (own_second, LANES),
                "recv_s%d%d" % (p, q): (row, own_second // row, LANES),
                "full_s%d%d" % (p, q): (own_second, LANES),
            })
            axes.update({"s%d%d" % (p, q): pieces, "t%d%d" % (p, q): pieces})
    names = list(buffers) + ["sem_" + name for name in axes] + ["sem_load", "sem_move"]
    shapes = [pltpu.VMEM(shape, jnp.float32) for shape in buffers.values()]
    names.insert(len(shapes), "across_left")
    shapes.append(pltpu.VMEM((rank, 6 * PIVOTS), jnp.bfloat16))
    shapes += [pltpu.SemaphoreType.DMA((2, max(n - 1, 1))) for n in axes.values()]
    shapes += [pltpu.SemaphoreType.DMA((frames // math.gcd(frames, GROUP),))]
    shapes += [pltpu.SemaphoreType.DMA((2,))]
    return names, shapes


def kernel(sizes, names, tensor, first_in, second_in, first_out, second_out, frames_out, weights_out, *scratch):
    row, col = sizes["row"], sizes["col"]
    v = dict(zip(names, scratch))
    inv, sums, tens, held = v["inv"], v["sums"], v["tens"], v["held"]
    first, second = v["first"], v["second"]
    frames, own_first, own_second = tensor.shape
    rank = first.shape[1]
    half = rank // 2
    tiles = rank // LANES
    rows_first, rows_second = own_first * row, own_second * col
    steps = rank // PIVOTS
    twin = Twin(col)

    group = math.gcd(frames, GROUP)
    loads = frames // group

    def load(g):
        block = pl.ds(g * group, group)
        return pltpu.make_async_copy(tensor.at[block], tens.at[block], v["sem_load"].at[g])

    def move(source, target, at):
        copy = pltpu.make_async_copy(source, target, v["sem_move"].at[at])
        copy.start()
        return copy

    def contract(start, stop):
        def step(g, carry):
            load(g).wait()
            ks = [g * group + u for u in range(group)]
            parts = [cross(tens[k], first[...], HIGH) for k in ks]
            for k, part in zip(ks, parts):
                held[k] = part
                sums[pl.ds(k, 1), :] = jnp.sum(part * second[...], axis=0, keepdims=True)
            return carry

        lax.fori_loop(start, stop, step, 0)

    def frame_terms(raw, start, stop):
        def step(k, carry):
            sums[pl.ds(k, 1), :] = jnp.sum(held[k] * raw[...], axis=0, keepdims=True)
            return carry

        lax.fori_loop(start, stop, step, 0, unroll=4)

    def second_terms(out, q):
        block = math.gcd(own_second, 128)
        here = slice(q * LANES, (q + 1) * LANES)
        for c in range(0, own_second, block):
            def step(k, total):
                return total + held[k, c : c + block, here] * frames_out[pl.ds(k, 1), :][:, here]

            out[c : c + block, :] = lax.fori_loop(
                0, frames, step, jnp.zeros((block, LANES), jnp.float32), unroll=4
            )

    def first_terms(raw, start, stop):
        group = math.gcd(stop - start, 4)

        def step(g, carry):
            base = start + g * group
            stacked = tens[pl.ds(base, group)].reshape(group * own_first, own_second)
            part = product(stacked, raw[...], HIGH)
            v["terms_f"][...] += sum(
                part[u * own_first : (u + 1) * own_first, :] * frames_out[pl.ds(base + u, 1), :]
                for u in range(group)
            )
            return carry

        lax.fori_loop(0, (stop - start) // group, step, 0)

    def frames_across(name):
        return lots_share(
            "col", col, total(v["recv_r" + name]), v["parts_c" + name], v["sem_c" + name]
        )

    def frames_back(name):
        return lots_share(
            "row", row, total(v["parts_c" + name]), v["full_r" + name], v["sem_d" + name]
        )

    def solve_frames(frame_sums, scale):
        raw = product(frame_sums * scale, inv[...]) * scale
        raw = raw * (1.0 / math.sqrt(rows_first * rows_second))
        normed = raw / jnp.sqrt(jnp.mean(raw * raw, axis=0, keepdims=True) + epsilon)
        frames_out[...] = normed
        return cross(normed, normed) / frames

    state = (inv, v["panel"], v["solved"], v["across_left"])

    def unit(gram):
        down = lax.broadcasted_iota(jnp.int32, (rank, rank), 0)
        across = lax.broadcasted_iota(jnp.int32, (rank, rank), 1)
        diagonal = jnp.where(down == across, gram, 0.0)
        wide = 1.0 / jnp.sqrt(jnp.sum(diagonal, axis=0, keepdims=True))
        tall = 1.0 / jnp.sqrt(jnp.sum(diagonal, axis=1, keepdims=True))
        return gram * wide * tall, wide

    greet(sizes)
    come = [move(first_in, first, 0), move(second_in, second, 1)]
    for g in range(loads):
        load(g).start()
    come[0].wait()
    v["gram_a"][...] = cross(first[...], first[...], HIGH)
    greeted(sizes)
    offset = twin.core * half
    go_a = scatter("row", row, v["gram_a"], v["recv_a"], v["sem_a"], offset)
    come[1].wait()
    v["gram_b"][...] = cross(second[...], second[...], HIGH)
    go_b = halves_out(twin, v["gram_b"], v["recv_b"], v["sem_b"])
    contract(0, loads // 2)
    finish(go_b)
    go_b = halves_across(twin, v["gram_b"], v["recv_b"], v["across_b"], v["sem_b2"])
    contract(loads // 2, loads)
    go_r = lots_out(sums, v["lots_r0"], v["recv_r0"], v["sem_r0"])
    finish(go_a)
    go_a = gather("row", row, total(v["recv_a"]), v["full_a"], v["sem_a2"], offset)
    finish(go_b)
    v["full_b"][span(twin.core, half), :] = total(v["across_b"])
    go_b = halves_back(twin, v["full_b"], v["sem_b3"])
    finish(go_r)
    go_c = frames_across("0")
    finish(go_b)
    second_gram, second_scale = unit(v["full_b"][...] * (1.0 / rows_second))
    finish(go_a)
    go_a = halves_back(twin, v["full_a"], v["sem_a3"])
    finish(go_a)
    first_gram = v["gram_a"]
    first_gram[...], first_scale = unit(v["full_a"][...] * (1.0 / rows_first))
    wide = None
    for p in range(PASSES):
        here = str(p)
        inv[...] = first_gram[...] * second_gram
        begin(*state)
        invert(*state, 0, steps // 8)
        finish(go_c)
        go_d = frames_back(here)
        invert(*state, steps // 8, steps)
        flush(*state)
        finish(go_d)
        full_r = v["full_r" + here]
        frame_sums = jnp.concatenate([full_r[d] for d in range(row)], axis=0)
        if wide is None:
            frame_scale = first_scale * second_scale
        else:
            frame_sums = frame_sums / wide
            frame_scale = first_scale
        frame_gram = solve_frames(frame_sums, frame_scale)
        parts = [here + str(q) for q in range(tiles)]
        pieces = [(part, cut) for part in parts for cut in range(CUTS)]
        go_s = []
        for q, part in enumerate(parts):
            second_terms(v["terms_s" + part], q)
            for cut in range(CUTS):
                go_s.append(scatter_piece(
                    row, cut, v["terms_s" + part], v["recv_s" + part], v["sem_s" + part]
                ))
        inv[...] = first_gram[...] * frame_gram
        go_t = []
        at = 0
        begin(*state)
        for q, (part, cut) in enumerate(pieces):
            until = steps * 7 // 8 if q == 0 else steps
            if at < until:
                invert(*state, at, until)
                at = until
            finish(go_s[q])
            go_t.append(gather_piece(
                row, cut, v["recv_s" + part], v["full_s" + part], v["sem_t" + part]
            ))
        flush(*state)
        for copies in go_t:
            finish(copies)
        raw = v["raw_s" + here]
        summed = jnp.concatenate([v["full_s" + part][...] for part in parts], axis=1)
        raw[...] = product(summed * first_scale, inv[...], HIGH) * (
            first_scale * (1.0 / math.sqrt(rows_first * frames))
        )
        gram_g, recv_g, across_g, full_g = (
            v[name + here] for name in ("gram_g", "recv_g", "across_g", "full_g")
        )
        gram_g[...] = cross(raw[...], raw[...], HIGH)
        go_g = halves_out(twin, gram_g, recv_g, v["sem_g" + here])
        last = p + 1 == PASSES
        if last:
            v["terms_f"][...] = jnp.zeros((own_first, rank), jnp.float32)
            first_terms(raw, 0, frames // 4)
        else:
            later = str(p + 1)
            frame_terms(raw, 0, frames)
            go_r = lots_out(sums, v["lots_r" + later], v["recv_r" + later], v["sem_r" + later])
        finish(go_g)
        go_g = halves_across(twin, gram_g, recv_g, across_g, v["sem_h" + here])
        if last:
            first_terms(raw, frames // 4, frames)
        else:
            finish(go_r)
            go_c = frames_across(later)
        finish(go_g)
        full_g[span(twin.core, half), :] = total(across_g)
        go_g = halves_back(twin, full_g, v["sem_i" + here])
        if last:
            go_f = scatter("col", col, v["terms_f"], v["recv_f"], v["sem_f"])
        finish(go_g)
        gram = full_g[...] * (1.0 / rows_second)
        down = lax.broadcasted_iota(jnp.int32, (rank, rank), 0)
        across = lax.broadcasted_iota(jnp.int32, (rank, rank), 1)
        diagonal = jnp.where(down == across, gram, 0.0)
        wide = jnp.sqrt(jnp.sum(diagonal, axis=0, keepdims=True) + epsilon)
        tall = jnp.sqrt(jnp.sum(diagonal, axis=1, keepdims=True) + epsilon)
        second_gram = gram / wide / tall
    inv[...] = second_gram * frame_gram
    second_out[...] = raw[...] / wide
    begin(*state)
    invert(*state, 0, steps // 2)
    finish(go_f)
    go_f = gather("col", col, total(v["recv_f"]), v["full_f"], v["sem_f2"])
    invert(*state, steps // 2, steps)
    flush(*state)
    finish(go_f)
    raw = product(v["full_f"][...] / wide, inv[...]) * (1.0 / math.sqrt(rows_second * frames))
    squares = jnp.sum(raw * raw, axis=0, keepdims=True)
    go_w = spread("row", row, squares, v["parts_w"], v["sem_w"])
    first_out[...] = raw
    finish(go_w)
    weights = jnp.sqrt(total(v["parts_w"])[0:1, :] * (1.0 / rows_first) + epsilon)
    weights_out[...] = weights
    first_out[...] = first_out[...] / weights


def deliver(*refs):
    half = len(refs) // 2
    sems = refs[-1]
    copies = [
        pltpu.make_async_copy(source, target, sems.at[k])
        for k, (source, target) in enumerate(zip(refs[:half], refs[half : 2 * half]))
    ]
    for copy in copies:
        copy.start()
    for copy in copies:
        copy.wait()


def body(sizes, tensor, initial_first, initial_second):
    frames, own_first, own_second = tensor.shape
    rank = initial_first.shape[1]
    names, scratch = layout(sizes, frames, own_first, own_second, rank)
    far = pl.BlockSpec(memory_space=pltpu.HBM)
    near = pl.BlockSpec(memory_space=pltpu.VMEM)
    outs = ((own_first, rank), (own_second, rank), (frames, rank), (1, rank))
    shapes = [jax.ShapeDtypeStruct(shape, jnp.float32) for shape in outs]
    results = pl.pallas_call(
        functools.partial(kernel, sizes, names),
        out_shape=shapes,
        in_specs=[far] * 3,
        out_specs=[near] * len(outs),
        scratch_shapes=scratch,
        compiler_params=pltpu.CompilerParams(
            collective_id=0, has_side_effects=True, vmem_limit_bytes=48 * 1024 * 1024
        ),
        name="als",
    )(*[
        pltpu.with_memory_space_constraint(x, pltpu.HBM)
        for x in (tensor, initial_first, initial_second)
    ])
    results = pl.pallas_call(
        deliver,
        out_shape=shapes,
        in_specs=[near] * len(outs),
        out_specs=[far] * len(outs),
        scratch_shapes=[pltpu.SemaphoreType.DMA((len(outs),))],
        compiler_params=pltpu.CompilerParams(vmem_limit_bytes=1024 * 1024),
        name="deliver",
    )(*results)
    factor_first, second, factor_frames, weights = results
    return (factor_first, second, factor_frames, weights.reshape(rank))


def solution(mesh):
    sizes = {"row": mesh.shape["row"], "col": mesh.shape["col"]}
    placed = (P(None, "row", "col"), P("row", None), P("col", None))
    return jax.shard_map(
        functools.partial(body, sizes),
        mesh=mesh,
        in_specs=placed,
        out_specs=(P("row", None), P("col", None), P(), P()),
        check_vma=False,
    )
```

```python
import functools
import math

import jax
import jax.numpy as jnp
from jax import lax
from jax.experimental import pallas as pl
from jax.experimental.pallas import tpu as pltpu
from jax.sharding import PartitionSpec as P

PASSES = 2
LANES = 128
PIVOTS = 16
GROUP = 4
CUTS = 2
MESH = pl.DeviceIdType.MESH
HIGHEST = lax.Precision.HIGHEST
HIGH = lax.Precision.HIGH

epsilon = 1e-06


def product(a, b, precision=HIGHEST):
    return jnp.dot(a, b, precision=precision, preferred_element_type=jnp.float32)


def cross(a, b, precision=HIGHEST):
    return lax.dot_general(
        a, b, (((0,), (0,)), ((), ())), precision=precision, preferred_element_type=jnp.float32
    )


def split(x):
    high = x.astype(jnp.bfloat16)
    rest = x - high.astype(jnp.float32)
    mid = rest.astype(jnp.bfloat16)
    return high, mid, (rest - mid.astype(jnp.float32)).astype(jnp.bfloat16)


def stacked(solved):
    h, m, l = split(solved[...])
    return jnp.concatenate([h, m, h, l, m, h], axis=0)


def update(left, right):
    return jnp.dot(left, right, preferred_element_type=jnp.float32)


def begin(a, panel, solved, left):
    panel[...] = a[0:PIVOTS, :]
    solved[...] = jnp.zeros_like(solved)
    left[...] = jnp.zeros_like(left)


def flush(a, panel, solved, left):
    a[...] = a[...] - update(left[...], stacked(solved))
    a[a.shape[0] - PIVOTS :, :] = solved[...]


def invert(a, panel, solved, left, start, stop):
    size = a.shape[0]
    tiles = size // LANES
    each = LANES // PIVOTS
    row = lax.broadcasted_iota(jnp.int32, (PIVOTS, LANES), 0)
    lane = lax.broadcasted_iota(jnp.int32, (PIVOTS, LANES), 1)
    across = lax.broadcasted_iota(jnp.int32, (size, LANES), 1)
    parts = [slice(q * LANES, (q + 1) * LANES) for q in range(tiles)]

    def line(x, t):
        return jnp.broadcast_to(x[t : t + 1, :], (PIVOTS, LANES))

    def block(g):
        return pl.ds(pl.multiple_of(g * PIVOTS, PIVOTS), PIVOTS)

    def step(own, g, carry):
        at = g * PIVOTS - own * LANES
        place = lane - at
        inside = (place >= 0) & (place < PIVOTS)

        def columns(x):
            picked = [jnp.where(place == t, x, 0.0) for t in range(PIVOTS)]
            return [
                jnp.broadcast_to(jnp.sum(y, axis=1, keepdims=True), (PIVOTS, LANES))
                for y in picked
            ]

        rows = [panel[:, part] for part in parts]
        cols = columns(rows[own])
        right = stacked(solved)
        ahead = block(jnp.minimum(g + 1, size // PIVOTS - 1))
        stale = a[ahead, :] - update(left[ahead, :], right)
        stale = [stale[:, part] for part in parts]
        scales = columns(stale[own])
        stale[own] = jnp.where(inside, 0.0, stale[own])
        whole = update(left[...], right)
        behind = block(jnp.maximum(g - 1, 0))
        for q, part in enumerate(parts):
            kept, done = a[:, part] - whole[:, part], solved[:, part]
            if q == own:
                kept = jnp.where((across >= at) & (across < at + PIVOTS), 0.0, kept)
                done = jnp.where(inside, 0.0, done)
            a[:, part] = kept
            a[behind, part] = done
        beside = jnp.where(inside, 0.0, jnp.where(place < 0, -rows[own], rows[own]))
        h, m, l = split(
            jnp.concatenate([-x for x in rows[:own]] + [beside] + rows[own + 1 :], axis=1)
        )
        left[...] = jnp.concatenate([h, h, m, h, m, l], axis=0).T
        work = list(rows)
        work[own] = jnp.where(inside, jnp.where(place == row, 1.0, 0.0), rows[own])
        for t in range(PIVOTS):
            pivot = 1.0 / line(cols[t], t)
            factor = (cols[t] - jnp.where(row == t, 1.0, 0.0)) * pivot
            cols[t + 1 :] = [x - factor * line(x, t) for x in cols[t + 1 :]]
            work = [x - factor * line(x, t) for x in work]
        for q, part in enumerate(parts):
            fresh = stale[q]
            for t in range(PIVOTS):
                fresh = fresh - scales[t] * line(work[q], t)
            panel[:, part] = fresh
            solved[:, part] = work[q]
        return carry

    for q in range(tiles):
        low, high = max(start, q * each), min(stop, (q + 1) * each)
        if low < high:
            lax.fori_loop(low, high, functools.partial(step, q), 0)


def greet(sizes):
    barrier = pltpu.get_barrier_semaphore()
    for axis, n in sizes.items():
        me = lax.axis_index(axis)
        for d in range(1, n):
            pl.semaphore_signal(
                barrier, inc=1, device_id={axis: lax.rem(me + d, n)}, device_id_type=MESH
            )


def greeted(sizes):
    pl.semaphore_wait(pltpu.get_barrier_semaphore(), sum(n - 1 for n in sizes.values()))


def send(source, target, sems, device):
    pltpu.make_async_remote_copy(
        src_ref=source, dst_ref=target, send_sem=sems.at[0], recv_sem=sems.at[1],
        device_id=device, device_id_type=MESH,
    ).start()


def finish(exchange):
    view, sems = exchange
    if view is not None:
        for k in range(2):
            pltpu.make_async_copy(view, view, sems.at[k]).wait()


def span(index, chunk):
    return pl.ds(pl.multiple_of(index * chunk, 8), chunk)


def others(axis, n):
    me = lax.axis_index(axis)
    return [lax.rem(me + d, n) for d in range(1, n)]


def scatter(axis, n, source, recv, sems, offset=0):
    me = lax.axis_index(axis)
    chunk = recv.shape[1]

    def of(peer):
        return pl.ds(pl.multiple_of(offset + peer * chunk, 8), chunk)

    for peer in others(axis, n):
        send(source.at[of(peer), :], recv.at[me], sems, {axis: peer})
    recv[me] = source[of(me), :]
    return recv.at[pl.ds(0, n - 1)], sems


def gather(axis, n, own, full, sems, offset=0):
    me = lax.axis_index(axis)
    chunk = own.shape[0]
    place = pl.ds(pl.multiple_of(offset + me * chunk, 8), chunk)
    full[place, :] = own
    for peer in others(axis, n):
        send(full.at[place, :], full.at[place, :], sems, {axis: peer})
    return full.at[pl.ds(0, (n - 1) * chunk), :], sems


def spread(axis, n, line, parts, sems):
    me = lax.axis_index(axis)
    one = pl.ds(0, 1)
    parts[me, 0:1, :] = line
    for peer in others(axis, n):
        send(parts.at[me, one, :], parts.at[me, one, :], sems, {axis: peer})
    return parts.at[pl.ds(0, n - 1), one, :], sems


def scatter_piece(n, cut, source, recv, sems):
    me = lax.axis_index("row")
    chunk = recv.shape[1]
    small = chunk // CUTS
    inside = pl.ds(cut * small, small)

    def of(peer):
        return pl.ds(pl.multiple_of(peer * chunk + cut * small, 8), small)

    for peer in others("row", n):
        send(source.at[of(peer), :], recv.at[me, inside, :], sems.at[cut], {"row": peer})
    recv[me, cut * small : (cut + 1) * small, :] = source[of(me), :]
    return recv.at[pl.ds(0, n - 1), inside, :], sems.at[cut]


def gather_piece(n, cut, recv, full, sems):
    me = lax.axis_index("row")
    chunk = recv.shape[1]
    small = chunk // CUTS
    inside = slice(cut * small, (cut + 1) * small)
    place = pl.ds(pl.multiple_of(me * chunk + cut * small, 8), small)
    full[place, :] = total(recv[:, inside, :])
    for peer in others("row", n):
        send(full.at[place, :], full.at[place, :], sems.at[cut], {"row": peer})
    return full.at[pl.ds(0, (n - 1) * small), :], sems.at[cut]


def lots_out(sums, lots, recv, sems):
    n, few = lots.shape[:2]
    me = lax.axis_index("row")
    for d in range(n):
        lots[d] = sums[d * few : (d + 1) * few, :]
    recv[me] = lots[me]
    for peer in others("row", n):
        send(lots.at[peer], recv.at[me], sems, {"row": peer})
    return recv.at[pl.ds(0, n - 1)], sems


def lots_share(axis, n, own, full, sems):
    me = lax.axis_index(axis)
    full[me] = own
    for peer in others(axis, n):
        send(full.at[me], full.at[me], sems, {axis: peer})
    return full.at[pl.ds(0, n - 1)], sems


def total(recv):
    result = recv[0]
    for s in range(1, recv.shape[0]):
        result = result + recv[s]
    return result


def total_blocks(full, n):
    chunk = full.shape[0] // n
    result = full[0:chunk, :]
    for s in range(1, n):
        result = result + full[s * chunk : (s + 1) * chunk, :]
    return result


class Twin:
    def __init__(self, col):
        self.count = col // 2
        me = lax.axis_index("col")
        self.core = lax.rem(me, 2)
        self.chip = me // 2
        self.partner = {"col": self.chip * 2 + 1 - self.core}
        self.others = [
            {"col": lax.rem(self.chip + d, self.count) * 2 + self.core}
            for d in range(1, self.count)
        ]


def halves_out(twin, gram, recv, sems):
    half = gram.shape[0] // 2
    send(gram.at[span(1 - twin.core, half), :], recv, sems, twin.partner)
    return recv, sems


def halves_across(twin, gram, recv, across, sems):
    half = gram.shape[0] // 2
    across[twin.chip] = gram[span(twin.core, half), :] + recv[...]
    here = across.at[twin.chip]
    for peer in twin.others:
        send(here, here, sems, peer)
    view = across.at[pl.ds(0, twin.count - 1)] if twin.count > 1 else None
    return view, sems


def halves_back(twin, full, sems):
    half = full.shape[0] // 2
    mine = full.at[span(twin.core, half), :]
    send(mine, mine, sems, twin.partner)
    return mine, sems


def layout(sizes, frames, own_first, own_second, rank):
    row, col = sizes["row"], sizes["col"]
    square = (rank, rank)
    half = rank // 2
    chips = col // 2
    few = frames // row
    buffers = {
        "tens": (frames, own_first, own_second),
        "held": (frames, own_second, rank),
        "first": (own_first, rank), "second": (own_second, rank),
        "inv": square, "panel": (PIVOTS, rank), "solved": (PIVOTS, rank),
        "sums": (frames, rank),
        "gram_a": square, "recv_a": (row, half // row, rank), "full_a": square,
        "gram_b": square, "recv_b": (half, rank), "across_b": (chips, half, rank),
        "full_b": square,
        "terms_f": (own_first, rank), "recv_f": (col, own_first // col, rank),
        "full_f": (own_first, rank), "parts_w": (row, 8, rank),
    }
    pairs = ["a", "a2", "a3", "b", "b2", "b3", "f", "f2", "w"]
    cuts = []
    for p in range(PASSES):
        buffers.update({
            "lots_r%d" % p: (row, few, rank), "recv_r%d" % p: (row, few, rank),
            "parts_c%d" % p: (col, few, rank), "full_r%d" % p: (row, few, rank),
            "raw_s%d" % p: (own_second, rank),
            "gram_g%d" % p: square, "recv_g%d" % p: (half, rank),
            "across_g%d" % p: (chips, half, rank), "full_g%d" % p: square,
        })
        pairs += [name + str(p) for name in "rcdghi"]
        for q in range(rank // LANES):
            buffers.update({
                "terms_s%d%d" % (p, q): (own_second, LANES),
                "recv_s%d%d" % (p, q): (row, own_second // row, LANES),
                "full_s%d%d" % (p, q): (own_second, LANES),
            })
            cuts += ["s%d%d" % (p, q), "t%d%d" % (p, q)]
    names = list(buffers) + ["sem_" + name for name in pairs + cuts] + ["sem_load", "sem_move"]
    shapes = [pltpu.VMEM(shape, jnp.float32) for shape in buffers.values()]
    names.insert(len(shapes), "across_left")
    shapes.append(pltpu.VMEM((rank, 6 * PIVOTS), jnp.bfloat16))
    shapes += [pltpu.SemaphoreType.DMA((2,)) for name in pairs]
    shapes += [pltpu.SemaphoreType.DMA((CUTS, 2)) for name in cuts]
    shapes += [pltpu.SemaphoreType.DMA((frames // math.gcd(frames, GROUP),))]
    shapes += [pltpu.SemaphoreType.DMA((2,))]
    return names, shapes


def kernel(sizes, names, tensor, first_in, second_in, first_out, second_out, frames_out, weights_out, *scratch):
    row, col = sizes["row"], sizes["col"]
    v = dict(zip(names, scratch))
    inv, sums, tens, held = v["inv"], v["sums"], v["tens"], v["held"]
    first, second = v["first"], v["second"]
    frames, own_first, own_second = tensor.shape
    rank = first.shape[1]
    half = rank // 2
    tiles = rank // LANES
    rows_first, rows_second = own_first * row, own_second * col
    steps = rank // PIVOTS
    twin = Twin(col)

    group = math.gcd(frames, GROUP)
    loads = frames // group

    def load(g):
        block = pl.ds(g * group, group)
        return pltpu.make_async_copy(tensor.at[block], tens.at[block], v["sem_load"].at[g])

    def move(source, target, at):
        copy = pltpu.make_async_copy(source, target, v["sem_move"].at[at])
        copy.start()
        return copy

    def contract(start, stop):
        def step(g, carry):
            load(g).wait()
            ks = [g * group + u for u in range(group)]
            parts = [cross(tens[k], first[...], HIGH) for k in ks]
            for k, part in zip(ks, parts):
                held[k] = part
                sums[pl.ds(k, 1), :] = jnp.sum(part * second[...], axis=0, keepdims=True)
            return carry

        lax.fori_loop(start, stop, step, 0)

    def frame_terms(raw, start, stop):
        def step(k, carry):
            sums[pl.ds(k, 1), :] = jnp.sum(held[k] * raw[...], axis=0, keepdims=True)
            return carry

        lax.fori_loop(start, stop, step, 0, unroll=4)

    def second_terms(out, q):
        block = math.gcd(own_second, 128)
        here = slice(q * LANES, (q + 1) * LANES)
        for c in range(0, own_second, block):
            def step(k, total):
                return total + held[k, c : c + block, here] * frames_out[pl.ds(k, 1), :][:, here]

            out[c : c + block, :] = lax.fori_loop(
                0, frames, step, jnp.zeros((block, LANES), jnp.float32), unroll=4
            )

    def first_terms(raw, start, stop):
        group = math.gcd(stop - start, 4)

        def step(g, carry):
            base = start + g * group
            stacked = tens[pl.ds(base, group)].reshape(group * own_first, own_second)
            part = product(stacked, raw[...], HIGH)
            v["terms_f"][...] += sum(
                part[u * own_first : (u + 1) * own_first, :] * frames_out[pl.ds(base + u, 1), :]
                for u in range(group)
            )
            return carry

        lax.fori_loop(0, (stop - start) // group, step, 0)

    def frames_across(name):
        return lots_share(
            "col", col, total(v["recv_r" + name]), v["parts_c" + name], v["sem_c" + name]
        )

    def frames_back(name):
        return lots_share(
            "row", row, total(v["parts_c" + name]), v["full_r" + name], v["sem_d" + name]
        )

    def solve_frames(frame_sums, scale):
        raw = product(frame_sums * scale, inv[...]) * scale
        raw = raw * (1.0 / math.sqrt(rows_first * rows_second))
        normed = raw / jnp.sqrt(jnp.mean(raw * raw, axis=0, keepdims=True) + epsilon)
        frames_out[...] = normed
        return cross(normed, normed) / frames

    state = (inv, v["panel"], v["solved"], v["across_left"])

    def unit(gram):
        down = lax.broadcasted_iota(jnp.int32, (rank, rank), 0)
        across = lax.broadcasted_iota(jnp.int32, (rank, rank), 1)
        diagonal = jnp.where(down == across, gram, 0.0)
        wide = 1.0 / jnp.sqrt(jnp.sum(diagonal, axis=0, keepdims=True))
        tall = 1.0 / jnp.sqrt(jnp.sum(diagonal, axis=1, keepdims=True))
        return gram * wide * tall, wide

    come = [move(first_in, first, 0)]
    greet(sizes)
    come.append(move(second_in, second, 1))
    come[0].wait()
    for g in range(loads):
        load(g).start()
    v["gram_a"][...] = cross(first[...], first[...], HIGH)
    greeted(sizes)
    offset = twin.core * half
    go_a = scatter("row", row, v["gram_a"], v["recv_a"], v["sem_a"], offset)
    come[1].wait()
    v["gram_b"][...] = cross(second[...], second[...], HIGH)
    go_b = halves_out(twin, v["gram_b"], v["recv_b"], v["sem_b"])
    contract(0, loads // 2)
    finish(go_b)
    go_b = halves_across(twin, v["gram_b"], v["recv_b"], v["across_b"], v["sem_b2"])
    contract(loads // 2, loads)
    go_r = lots_out(sums, v["lots_r0"], v["recv_r0"], v["sem_r0"])
    finish(go_a)
    go_a = gather("row", row, total(v["recv_a"]), v["full_a"], v["sem_a2"], offset)
    finish(go_b)
    v["full_b"][span(twin.core, half), :] = total(v["across_b"])
    go_b = halves_back(twin, v["full_b"], v["sem_b3"])
    finish(go_r)
    go_c = frames_across("0")
    finish(go_b)
    second_gram, second_scale = unit(v["full_b"][...] * (1.0 / rows_second))
    finish(go_a)
    go_a = halves_back(twin, v["full_a"], v["sem_a3"])
    finish(go_a)
    first_gram = v["gram_a"]
    first_gram[...], first_scale = unit(v["full_a"][...] * (1.0 / rows_first))
    wide = None
    for p in range(PASSES):
        here = str(p)
        inv[...] = first_gram[...] * second_gram
        begin(*state)
        invert(*state, 0, steps // 8)
        finish(go_c)
        go_d = frames_back(here)
        invert(*state, steps // 8, steps)
        flush(*state)
        finish(go_d)
        full_r = v["full_r" + here]
        frame_sums = jnp.concatenate([full_r[d] for d in range(row)], axis=0)
        if wide is None:
            frame_scale = first_scale * second_scale
        else:
            frame_sums = frame_sums / wide
            frame_scale = first_scale
        frame_gram = solve_frames(frame_sums, frame_scale)
        parts = [here + str(q) for q in range(tiles)]
        pieces = [(part, cut) for part in parts for cut in range(CUTS)]
        go_s = []
        for q, part in enumerate(parts):
            second_terms(v["terms_s" + part], q)
            for cut in range(CUTS):
                go_s.append(scatter_piece(
                    row, cut, v["terms_s" + part], v["recv_s" + part], v["sem_s" + part]
                ))
        inv[...] = first_gram[...] * frame_gram
        go_t = []
        at = 0
        begin(*state)
        for q, (part, cut) in enumerate(pieces):
            until = steps * 7 // 8 if q == 0 else steps
            if at < until:
                invert(*state, at, until)
                at = until
            finish(go_s[q])
            go_t.append(gather_piece(
                row, cut, v["recv_s" + part], v["full_s" + part], v["sem_t" + part]
            ))
        flush(*state)
        for go in go_t:
            finish(go)
        raw = v["raw_s" + here]
        summed = jnp.concatenate([v["full_s" + part][...] for part in parts], axis=1)
        raw[...] = product(summed * first_scale, inv[...], HIGH) * (
            first_scale * (1.0 / math.sqrt(rows_first * frames))
        )
        gram_g, recv_g, across_g, full_g = (
            v[name + here] for name in ("gram_g", "recv_g", "across_g", "full_g")
        )
        gram_g[...] = cross(raw[...], raw[...], HIGH)
        go_g = halves_out(twin, gram_g, recv_g, v["sem_g" + here])
        last = p + 1 == PASSES
        if last:
            v["terms_f"][...] = jnp.zeros((own_first, rank), jnp.float32)
            first_terms(raw, 0, frames // 4)
        else:
            later = str(p + 1)
            frame_terms(raw, 0, frames)
            go_r = lots_out(sums, v["lots_r" + later], v["recv_r" + later], v["sem_r" + later])
        finish(go_g)
        go_g = halves_across(twin, gram_g, recv_g, across_g, v["sem_h" + here])
        if last:
            first_terms(raw, frames // 4, frames)
            go_f = scatter("col", col, v["terms_f"], v["recv_f"], v["sem_f"])
        else:
            finish(go_r)
            go_c = frames_across(later)
        finish(go_g)
        full_g[span(twin.core, half), :] = total(across_g)
        go_g = halves_back(twin, full_g, v["sem_i" + here])
        finish(go_g)
        gram = full_g[...] * (1.0 / rows_second)
        down = lax.broadcasted_iota(jnp.int32, (rank, rank), 0)
        across = lax.broadcasted_iota(jnp.int32, (rank, rank), 1)
        diagonal = jnp.where(down == across, gram, 0.0)
        wide = jnp.sqrt(jnp.sum(diagonal, axis=0, keepdims=True) + epsilon)
        tall = jnp.sqrt(jnp.sum(diagonal, axis=1, keepdims=True) + epsilon)
        second_gram = gram / wide / tall
    inv[...] = second_gram * frame_gram
    second_out[...] = raw[...] / wide
    begin(*state)
    invert(*state, 0, steps // 2)
    finish(go_f)
    go_f = gather("col", col, total(v["recv_f"]), v["full_f"], v["sem_f2"])
    invert(*state, steps // 2, steps)
    flush(*state)
    finish(go_f)
    raw = product(v["full_f"][...] / wide, inv[...]) * (1.0 / math.sqrt(rows_second * frames))
    squares = jnp.sum(raw * raw, axis=0, keepdims=True)
    go_w = spread("row", row, squares, v["parts_w"], v["sem_w"])
    first_out[...] = raw
    finish(go_w)
    weights = jnp.sqrt(total(v["parts_w"])[0:1, :] * (1.0 / rows_first) + epsilon)
    weights_out[...] = weights
    first_out[...] = first_out[...] / weights


def deliver(*refs):
    half = len(refs) // 2
    sems = refs[-1]
    copies = [
        pltpu.make_async_copy(source, target, sems.at[k])
        for k, (source, target) in enumerate(zip(refs[:half], refs[half : 2 * half]))
    ]
    for copy in copies:
        copy.start()
    for copy in copies:
        copy.wait()


def body(sizes, tensor, initial_first, initial_second):
    frames, own_first, own_second = tensor.shape
    rank = initial_first.shape[1]
    names, scratch = layout(sizes, frames, own_first, own_second, rank)
    far = pl.BlockSpec(memory_space=pltpu.HBM)
    near = pl.BlockSpec(memory_space=pltpu.VMEM)
    outs = ((own_first, rank), (own_second, rank), (frames, rank), (1, rank))
    shapes = [jax.ShapeDtypeStruct(shape, jnp.float32) for shape in outs]
    results = pl.pallas_call(
        functools.partial(kernel, sizes, names),
        out_shape=shapes,
        in_specs=[far] * 3,
        out_specs=[near] * len(outs),
        scratch_shapes=scratch,
        compiler_params=pltpu.CompilerParams(
            collective_id=0, has_side_effects=True, vmem_limit_bytes=48 * 1024 * 1024
        ),
        name="als",
    )(*[
        pltpu.with_memory_space_constraint(x, pltpu.HBM)
        for x in (tensor, initial_first, initial_second)
    ])
    results = pl.pallas_call(
        deliver,
        out_shape=shapes,
        in_specs=[near] * len(outs),
        out_specs=[far] * len(outs),
        scratch_shapes=[pltpu.SemaphoreType.DMA((len(outs),))],
        compiler_params=pltpu.CompilerParams(vmem_limit_bytes=1024 * 1024),
        name="deliver",
    )(*results)
    factor_first, second, factor_frames, weights = results
    return (factor_first, second, factor_frames, weights.reshape(rank))


def solution(mesh):
    sizes = {"row": mesh.shape["row"], "col": mesh.shape["col"]}
    placed = (P(None, "row", "col"), P("row", None), P("col", None))
    return jax.shard_map(
        functools.partial(body, sizes),
        mesh=mesh,
        in_specs=placed,
        out_specs=(P("row", None), P("col", None), P(), P()),
        check_vma=False,
    )
```

```python
import functools
import math

import jax
import jax.numpy as jnp
from jax import lax
from jax.experimental import pallas as pl
from jax.experimental.pallas import tpu as pltpu
from jax.sharding import PartitionSpec as P

PASSES = 2
LANES = 128
PIVOTS = 16
GROUP = 8
CUTS = 2
MESH = pl.DeviceIdType.MESH
HIGHEST = lax.Precision.HIGHEST
HIGH = lax.Precision.HIGH

epsilon = 1e-06


def product(a, b, precision=HIGHEST):
    return jnp.dot(a, b, precision=precision, preferred_element_type=jnp.float32)


def cross(a, b, precision=HIGHEST):
    return lax.dot_general(
        a, b, (((0,), (0,)), ((), ())), precision=precision, preferred_element_type=jnp.float32
    )


def split(x):
    high = x.astype(jnp.bfloat16)
    rest = x - high.astype(jnp.float32)
    mid = rest.astype(jnp.bfloat16)
    return high, mid, (rest - mid.astype(jnp.float32)).astype(jnp.bfloat16)


def stacked(solved):
    h, m, l = split(solved[...])
    return jnp.concatenate([h, m, h, l, m, h], axis=0)


def update(left, right):
    return jnp.dot(left, right, preferred_element_type=jnp.float32)


def begin(a, panel, solved, left):
    panel[...] = a[0:PIVOTS, :]
    solved[...] = jnp.zeros_like(solved)
    left[...] = jnp.zeros_like(left)


def flush(a, panel, solved, left):
    a[...] = a[...] - update(left[...], stacked(solved))
    a[a.shape[0] - PIVOTS :, :] = solved[...]


def invert(a, panel, solved, left, start, stop):
    size = a.shape[0]
    tiles = size // LANES
    each = LANES // PIVOTS
    row = lax.broadcasted_iota(jnp.int32, (PIVOTS, LANES), 0)
    lane = lax.broadcasted_iota(jnp.int32, (PIVOTS, LANES), 1)
    across = lax.broadcasted_iota(jnp.int32, (size, LANES), 1)
    parts = [slice(q * LANES, (q + 1) * LANES) for q in range(tiles)]

    def line(x, t):
        return jnp.broadcast_to(x[t : t + 1, :], (PIVOTS, LANES))

    def block(g):
        return pl.ds(pl.multiple_of(g * PIVOTS, PIVOTS), PIVOTS)

    def step(own, g, carry):
        at = g * PIVOTS - own * LANES
        place = lane - at
        inside = (place >= 0) & (place < PIVOTS)

        def columns(x):
            picked = [jnp.where(place == t, x, 0.0) for t in range(PIVOTS)]
            return [
                jnp.broadcast_to(jnp.sum(y, axis=1, keepdims=True), (PIVOTS, LANES))
                for y in picked
            ]

        rows = [panel[:, part] for part in parts]
        cols = columns(rows[own])
        right = stacked(solved)
        ahead = block(jnp.minimum(g + 1, size // PIVOTS - 1))
        stale = a[ahead, :] - update(left[ahead, :], right)
        stale = [stale[:, part] for part in parts]
        scales = columns(stale[own])
        stale[own] = jnp.where(inside, 0.0, stale[own])
        whole = update(left[...], right)
        behind = block(jnp.maximum(g - 1, 0))
        for q, part in enumerate(parts):
            kept, done = a[:, part] - whole[:, part], solved[:, part]
            if q == own:
                kept = jnp.where((across >= at) & (across < at + PIVOTS), 0.0, kept)
                done = jnp.where(inside, 0.0, done)
            a[:, part] = kept
            a[behind, part] = done
        beside = jnp.where(inside, 0.0, jnp.where(place < 0, -rows[own], rows[own]))
        h, m, l = split(
            jnp.concatenate([-x for x in rows[:own]] + [beside] + rows[own + 1 :], axis=1)
        )
        left[...] = jnp.concatenate([h, h, m, h, m, l], axis=0).T
        work = list(rows)
        work[own] = jnp.where(inside, jnp.where(place == row, 1.0, 0.0), rows[own])
        for t in range(PIVOTS):
            pivot = 1.0 / line(cols[t], t)
            factor = (cols[t] - jnp.where(row == t, 1.0, 0.0)) * pivot
            cols[t + 1 :] = [x - factor * line(x, t) for x in cols[t + 1 :]]
            work = [x - factor * line(x, t) for x in work]
        for q, part in enumerate(parts):
            fresh = stale[q]
            for t in range(PIVOTS):
                fresh = fresh - scales[t] * line(work[q], t)
            panel[:, part] = fresh
            solved[:, part] = work[q]
        return carry

    for q in range(tiles):
        low, high = max(start, q * each), min(stop, (q + 1) * each)
        if low < high:
            lax.fori_loop(low, high, functools.partial(step, q), 0)


def greet(sizes):
    barrier = pltpu.get_barrier_semaphore()
    for axis, n in sizes.items():
        me = lax.axis_index(axis)
        for d in range(1, n):
            pl.semaphore_signal(
                barrier, inc=1, device_id={axis: lax.rem(me + d, n)}, device_id_type=MESH
            )


def greeted(sizes):
    pl.semaphore_wait(pltpu.get_barrier_semaphore(), sum(n - 1 for n in sizes.values()))


def send(source, target, sems, device):
    pltpu.make_async_remote_copy(
        src_ref=source, dst_ref=target, send_sem=sems.at[0], recv_sem=sems.at[1],
        device_id=device, device_id_type=MESH,
    ).start()


def finish(exchange):
    view, sems = exchange
    if view is not None:
        for k in range(2):
            pltpu.make_async_copy(view, view, sems.at[k]).wait()


def span(index, chunk):
    return pl.ds(pl.multiple_of(index * chunk, 8), chunk)


def others(axis, n):
    me = lax.axis_index(axis)
    if n & (n - 1):
        return [lax.rem(me + d, n) for d in range(1, n)]
    peers = []
    for e in range(n - 1, 0, -1):
        peer = me
        for bit in (1 << k for k in range(n.bit_length() - 1)):
            if e & bit:
                peer = peer + bit - 2 * bit * lax.rem(me // bit, 2)
        peers.append(peer)
    return peers


def cuts_of(own_second, row):
    return max(1, min(CUTS, own_second // row // 8))


def scatter(axis, n, source, recv, sems, offset=0):
    me = lax.axis_index(axis)
    chunk = recv.shape[1]

    def of(peer):
        return pl.ds(pl.multiple_of(offset + peer * chunk, 8), chunk)

    for peer in others(axis, n):
        send(source.at[of(peer), :], recv.at[me], sems, {axis: peer})
    recv[me] = source[of(me), :]
    return recv.at[pl.ds(0, n - 1)], sems


def gather(axis, n, own, full, sems, offset=0):
    me = lax.axis_index(axis)
    chunk = own.shape[0]
    place = pl.ds(pl.multiple_of(offset + me * chunk, 8), chunk)
    full[place, :] = own
    for peer in others(axis, n):
        send(full.at[place, :], full.at[place, :], sems, {axis: peer})
    return full.at[pl.ds(0, (n - 1) * chunk), :], sems


def spread(axis, n, line, parts, sems):
    me = lax.axis_index(axis)
    one = pl.ds(0, 1)
    parts[me, 0:1, :] = line
    for peer in others(axis, n):
        send(parts.at[me, one, :], parts.at[me, one, :], sems, {axis: peer})
    return parts.at[pl.ds(0, n - 1), one, :], sems


def lots_out(sums, lots, recv, sems):
    n, few = lots.shape[:2]
    me = lax.axis_index("row")
    for d in range(n):
        lots[d] = sums[d * few : (d + 1) * few, :]
    recv[me] = lots[me]
    for peer in others("row", n):
        send(lots.at[peer], recv.at[me], sems, {"row": peer})
    return recv.at[pl.ds(0, n - 1)], sems


def lots_share(axis, n, own, full, sems):
    me = lax.axis_index(axis)
    full[me] = own
    for peer in others(axis, n):
        send(full.at[me], full.at[me], sems, {axis: peer})
    return full.at[pl.ds(0, n - 1)], sems


def total(recv):
    result = recv[0]
    for s in range(1, recv.shape[0]):
        result = result + recv[s]
    return result


def total_blocks(full, n):
    chunk = full.shape[0] // n
    result = full[0:chunk, :]
    for s in range(1, n):
        result = result + full[s * chunk : (s + 1) * chunk, :]
    return result


class Twin:
    def __init__(self, col):
        self.count = col // 2
        me = lax.axis_index("col")
        self.core = lax.rem(me, 2)
        self.chip = me // 2
        self.partner = {"col": self.chip * 2 + 1 - self.core}
        self.others = [
            {"col": lax.rem(self.chip + d, self.count) * 2 + self.core}
            for d in range(1, self.count)
        ]


def halves_out(twin, gram, recv, sems):
    half = gram.shape[0] // 2
    send(gram.at[span(1 - twin.core, half), :], recv, sems, twin.partner)
    return recv, sems


def halves_across(twin, gram, recv, across, sems):
    half = gram.shape[0] // 2
    across[twin.chip] = gram[span(twin.core, half), :] + recv[...]
    here = across.at[twin.chip]
    for peer in twin.others:
        send(here, here, sems, peer)
    view = across.at[pl.ds(0, twin.count - 1)] if twin.count > 1 else None
    return view, sems


def halves_back(twin, full, sems):
    half = full.shape[0] // 2
    mine = full.at[span(twin.core, half), :]
    send(mine, mine, sems, twin.partner)
    return mine, sems


def layout(sizes, frames, own_first, own_second, rank):
    row, col = sizes["row"], sizes["col"]
    square = (rank, rank)
    half = rank // 2
    chips = col // 2
    few = frames // row
    count = cuts_of(own_second, row)
    buffers = {
        "tens": (frames, own_first, own_second),
        "held": (frames, own_second, rank),
        "first": (own_first, rank), "second": (own_second, rank),
        "inv": square, "panel": (PIVOTS, rank), "solved": (PIVOTS, rank),
        "sums": (frames, rank),
        "gram_a": square, "recv_a": (row, half // row, rank), "full_a": square,
        "gram_b": square, "recv_b": (half, rank), "across_b": (chips, half, rank),
        "full_b": square,
        "terms_f": (own_first, rank), "recv_f": (col, own_first // col, rank),
        "full_f": (own_first, rank), "parts_w": (row, 8, rank),
    }
    pairs = ["a", "a2", "a3", "b", "b2", "b3", "f", "f2", "w"] + list("rdgi")
    pairs += [name + str(p) for p in range(PASSES) for name in "ch"]
    cuts = ["s", "t"]
    for p in range(PASSES):
        buffers.update({
            "lots_r%d" % p: (row, few, rank), "recv_r%d" % p: (row, few, rank),
            "parts_c%d" % p: (col, few, rank), "full_r%d" % p: (row, few, rank),
            "raw_s%d" % p: (own_second, rank),
            "gram_g%d" % p: square, "recv_g%d" % p: (half, rank),
            "across_g%d" % p: (chips, half, rank), "full_g%d" % p: square,
        })
        for q in range(count):
            buffers.update({
                "terms_s%d%d" % (p, q): (own_second // count, rank),
                "recv_s%d%d" % (p, q): (row, own_second // count // row, rank),
                "full_s%d%d" % (p, q): (own_second // count, rank),
            })
    names = list(buffers) + ["sem_" + name for name in pairs + cuts] + ["sem_load", "sem_move"]
    shapes = [pltpu.VMEM(shape, jnp.float32) for shape in buffers.values()]
    names.insert(len(shapes), "across_left")
    shapes.append(pltpu.VMEM((rank, 6 * PIVOTS), jnp.bfloat16))
    shapes += [pltpu.SemaphoreType.DMA((2,)) for name in pairs]
    shapes += [pltpu.SemaphoreType.DMA((count, 2)) for name in cuts]
    shapes += [pltpu.SemaphoreType.DMA((frames // math.gcd(frames, GROUP),))]
    shapes += [pltpu.SemaphoreType.DMA((2,))]
    return names, shapes


def kernel(sizes, names, tensor, first_in, second_in, first_out, second_out, frames_out, weights_out, *scratch):
    row, col = sizes["row"], sizes["col"]
    v = dict(zip(names, scratch))
    inv, sums, tens, held = v["inv"], v["sums"], v["tens"], v["held"]
    first, second = v["first"], v["second"]
    frames, own_first, own_second = tensor.shape
    rank = first.shape[1]
    half = rank // 2
    count = cuts_of(own_second, row)
    rows_first, rows_second = own_first * row, own_second * col
    steps = rank // PIVOTS
    twin = Twin(col)

    group = math.gcd(frames, GROUP)
    loads = frames // group

    def load(g):
        block = pl.ds(g * group, group)
        return pltpu.make_async_copy(tensor.at[block], tens.at[block], v["sem_load"].at[g])

    def move(source, target, at):
        copy = pltpu.make_async_copy(source, target, v["sem_move"].at[at])
        copy.start()
        return copy

    def contract(start, stop):
        def step(g, carry):
            load(g).wait()
            ks = [g * group + u for u in range(group)]
            parts = [cross(tens[k], first[...], HIGH) for k in ks]
            for k, part in zip(ks, parts):
                held[k] = part
                sums[pl.ds(k, 1), :] = jnp.sum(part * second[...], axis=0, keepdims=True)
            return carry

        lax.fori_loop(start, stop, step, 0)

    def frame_terms(raw, start, stop):
        def step(k, carry):
            sums[pl.ds(k, 1), :] = jnp.sum(held[k] * raw[...], axis=0, keepdims=True)
            return carry

        lax.fori_loop(start, stop, step, 0, unroll=4)

    def lines(q):
        small = own_second // row // count
        starts = [d * small * count + q * small for d in range(row)]
        return [slice(start, start + small) for start in starts]

    def second_terms(out, q):
        small = own_second // row // count
        zero = tuple(jnp.zeros((small, rank), jnp.float32) for _ in range(row))

        def step(k, totals):
            weight = frames_out[pl.ds(k, 1), :]
            return tuple(total + held[k, at, :] * weight for total, at in zip(totals, lines(q)))

        for d, total in enumerate(lax.fori_loop(0, frames, step, zero, unroll=4)):
            out[d * small : (d + 1) * small, :] = total

    def first_terms(raw, start, stop):
        group = math.gcd(stop - start, 4)

        def step(g, carry):
            base = start + g * group
            stacked = tens[pl.ds(base, group)].reshape(group * own_first, own_second)
            part = product(stacked, raw[...], HIGH)
            v["terms_f"][...] += sum(
                part[u * own_first : (u + 1) * own_first, :] * frames_out[pl.ds(base + u, 1), :]
                for u in range(group)
            )
            return carry

        lax.fori_loop(0, (stop - start) // group, step, 0)

    def frames_across(name):
        return lots_share(
            "col", col, total(v["recv_r" + name]), v["parts_c" + name], v["sem_c" + name]
        )

    def frames_back(name):
        return lots_share(
            "row", row, total(v["parts_c" + name]), v["full_r" + name], v["sem_d"]
        )

    def solve_frames(frame_sums, scale):
        raw = product(frame_sums * scale, inv[...], HIGH) * scale
        raw = raw * (1.0 / math.sqrt(rows_first * rows_second))
        normed = raw / jnp.sqrt(jnp.mean(raw * raw, axis=0, keepdims=True) + epsilon)
        frames_out[...] = normed
        return cross(normed, normed, HIGH) * (1.0 / frames)

    state = (inv, v["panel"], v["solved"], v["across_left"])

    def unit(gram):
        down = lax.broadcasted_iota(jnp.int32, (rank, rank), 0)
        across = lax.broadcasted_iota(jnp.int32, (rank, rank), 1)
        diagonal = jnp.where(down == across, gram, 0.0)
        wide = 1.0 / jnp.sqrt(jnp.sum(diagonal, axis=0, keepdims=True))
        tall = 1.0 / jnp.sqrt(jnp.sum(diagonal, axis=1, keepdims=True))
        return gram * wide * tall, wide

    come = [move(first_in, first, 0)]
    greet(sizes)
    come.append(move(second_in, second, 1))
    come[0].wait()
    for g in range(loads):
        load(g).start()
    v["gram_a"][...] = cross(first[...], first[...], HIGH)
    greeted(sizes)
    offset = twin.core * half
    go_a = scatter("row", row, v["gram_a"], v["recv_a"], v["sem_a"], offset)
    come[1].wait()
    v["gram_b"][...] = cross(second[...], second[...], HIGH)
    go_b = halves_out(twin, v["gram_b"], v["recv_b"], v["sem_b"])
    contract(0, loads // 2)
    finish(go_b)
    go_b = halves_across(twin, v["gram_b"], v["recv_b"], v["across_b"], v["sem_b2"])
    contract(loads // 2, loads)
    go_r = lots_out(sums, v["lots_r0"], v["recv_r0"], v["sem_r"])
    finish(go_a)
    go_a = gather("row", row, total(v["recv_a"]), v["full_a"], v["sem_a2"], offset)
    finish(go_b)
    v["full_b"][span(twin.core, half), :] = total(v["across_b"])
    go_b = halves_back(twin, v["full_b"], v["sem_b3"])
    finish(go_r)
    go_c = frames_across("0")
    finish(go_b)
    second_gram, second_scale = unit(v["full_b"][...] * (1.0 / rows_second))
    finish(go_a)
    go_a = halves_back(twin, v["full_a"], v["sem_a3"])
    finish(go_a)
    first_gram = v["gram_a"]
    first_gram[...], first_scale = unit(v["full_a"][...] * (1.0 / rows_first))
    wide = None
    for p in range(PASSES):
        here = str(p)
        inv[...] = first_gram[...] * second_gram
        begin(*state)
        invert(*state, 0, steps // 8)
        finish(go_c)
        go_d = frames_back(here)
        invert(*state, steps // 8, steps)
        flush(*state)
        finish(go_d)
        full_r = v["full_r" + here]
        frame_sums = jnp.concatenate([full_r[d] for d in range(row)], axis=0)
        if wide is None:
            frame_scale = first_scale * second_scale
        else:
            frame_sums = frame_sums / wide
            frame_scale = first_scale
        frame_gram = solve_frames(frame_sums, frame_scale)
        parts = [here + str(q) for q in range(count)]
        go_s = []
        for q, part in enumerate(parts):
            second_terms(v["terms_s" + part], q)
            go_s.append(scatter(
                "row", row, v["terms_s" + part], v["recv_s" + part], v["sem_s"].at[q]
            ))
        inv[...] = first_gram[...] * frame_gram
        go_t = []
        at = 0
        begin(*state)
        for q, part in enumerate(parts):
            until = steps if q + 1 == count else min(steps, steps * (6 + q) // 8)
            if at < until:
                invert(*state, at, until)
                at = until
            finish(go_s[q])
            go_t.append(gather(
                "row", row, total(v["recv_s" + part]), v["full_s" + part], v["sem_t"].at[q]
            ))
        flush(*state)
        raw = v["raw_s" + here]
        gram_g, recv_g, across_g, full_g = (
            v[name + here] for name in ("gram_g", "recv_g", "across_g", "full_g")
        )
        for q, part in enumerate(parts):
            finish(go_t[q])
            some = product(v["full_s" + part][...] * first_scale, inv[...], HIGH) * (
                first_scale * (1.0 / math.sqrt(rows_first * frames))
            )
            small = some.shape[0] // row
            for d, place in enumerate(lines(q)):
                raw[place, :] = some[d * small : (d + 1) * small, :]
            terms = cross(some, some, HIGH)
            gram_g[...] = terms if q == 0 else gram_g[...] + terms
        go_g = halves_out(twin, gram_g, recv_g, v["sem_g"])
        last = p + 1 == PASSES
        if last:
            v["terms_f"][...] = jnp.zeros((own_first, rank), jnp.float32)
            first_terms(raw, 0, frames // 4)
        else:
            later = str(p + 1)
            frame_terms(raw, 0, frames)
            go_r = lots_out(sums, v["lots_r" + later], v["recv_r" + later], v["sem_r"])
        finish(go_g)
        go_g = halves_across(twin, gram_g, recv_g, across_g, v["sem_h" + here])
        if last:
            first_terms(raw, frames // 4, frames)
            go_f = scatter("col", col, v["terms_f"], v["recv_f"], v["sem_f"])
        else:
            finish(go_r)
            go_c = frames_across(later)
        finish(go_g)
        full_g[span(twin.core, half), :] = total(across_g)
        go_g = halves_back(twin, full_g, v["sem_i"])
        finish(go_g)
        gram = full_g[...] * (1.0 / rows_second)
        down = lax.broadcasted_iota(jnp.int32, (rank, rank), 0)
        across = lax.broadcasted_iota(jnp.int32, (rank, rank), 1)
        diagonal = jnp.where(down == across, gram, 0.0)
        wide = jnp.sqrt(jnp.sum(diagonal, axis=0, keepdims=True) + epsilon)
        tall = jnp.sqrt(jnp.sum(diagonal, axis=1, keepdims=True) + epsilon)
        second_gram = gram / wide / tall
    inv[...] = second_gram * frame_gram
    second_out[...] = raw[...] / wide
    begin(*state)
    invert(*state, 0, steps // 8)
    finish(go_f)
    go_f = gather("col", col, total(v["recv_f"]), v["full_f"], v["sem_f2"])
    invert(*state, steps // 8, steps)
    flush(*state)
    finish(go_f)
    raw = product(v["full_f"][...] / wide, inv[...], HIGH) * (1.0 / math.sqrt(rows_second * frames))
    squares = jnp.sum(raw * raw, axis=0, keepdims=True)
    go_w = spread("row", row, squares, v["parts_w"], v["sem_w"])
    first_out[...] = raw
    finish(go_w)
    weights = jnp.sqrt(total(v["parts_w"])[0:1, :] * (1.0 / rows_first) + epsilon)
    weights_out[...] = weights
    first_out[...] = first_out[...] / weights


def deliver(*refs):
    half = len(refs) // 2
    sems = refs[-1]
    copies = [
        pltpu.make_async_copy(source, target, sems.at[k])
        for k, (source, target) in enumerate(zip(refs[:half], refs[half : 2 * half]))
    ]
    for copy in copies:
        copy.start()
    for copy in copies:
        copy.wait()


def body(sizes, tensor, initial_first, initial_second):
    frames, own_first, own_second = tensor.shape
    rank = initial_first.shape[1]
    names, scratch = layout(sizes, frames, own_first, own_second, rank)
    far = pl.BlockSpec(memory_space=pltpu.HBM)
    near = pl.BlockSpec(memory_space=pltpu.VMEM)
    outs = ((own_first, rank), (own_second, rank), (frames, rank), (1, rank))
    shapes = [jax.ShapeDtypeStruct(shape, jnp.float32) for shape in outs]
    results = pl.pallas_call(
        functools.partial(kernel, sizes, names),
        out_shape=shapes,
        in_specs=[far] * 3,
        out_specs=[near] * len(outs),
        scratch_shapes=scratch,
        compiler_params=pltpu.CompilerParams(
            collective_id=0, has_side_effects=True, vmem_limit_bytes=48 * 1024 * 1024
        ),
        name="als",
    )(*[
        pltpu.with_memory_space_constraint(x, pltpu.HBM)
        for x in (tensor, initial_first, initial_second)
    ])
    results = pl.pallas_call(
        deliver,
        out_shape=shapes,
        in_specs=[near] * len(outs),
        out_specs=[far] * len(outs),
        scratch_shapes=[pltpu.SemaphoreType.DMA((len(outs),))],
        compiler_params=pltpu.CompilerParams(vmem_limit_bytes=1024 * 1024),
        name="deliver",
    )(*results)
    factor_first, second, factor_frames, weights = results
    return (factor_first, second, factor_frames, weights.reshape(rank))


def solution(mesh):
    sizes = {"row": mesh.shape["row"], "col": mesh.shape["col"]}
    placed = (P(None, "row", "col"), P("row", None), P("col", None))
    return jax.shard_map(
        functools.partial(body, sizes),
        mesh=mesh,
        in_specs=placed,
        out_specs=(P("row", None), P("col", None), P(), P()),
        check_vma=False,
    )
```

```python
import functools
import math

import jax
import jax.numpy as jnp
from jax import lax
from jax.experimental import pallas as pl
from jax.experimental.pallas import tpu as pltpu
from jax.sharding import PartitionSpec as P

PASSES = 2
LANES = 128
PIVOTS = 16
GROUP = 8
CUTS = 4
MESH = pl.DeviceIdType.MESH
HIGHEST = lax.Precision.HIGHEST
HIGH = lax.Precision.HIGH

epsilon = 1e-06


def product(a, b, precision=HIGHEST):
    return jnp.dot(a, b, precision=precision, preferred_element_type=jnp.float32)


def cross(a, b, precision=HIGHEST):
    return lax.dot_general(
        a, b, (((0,), (0,)), ((), ())), precision=precision, preferred_element_type=jnp.float32
    )


def split(x):
    high = x.astype(jnp.bfloat16)
    rest = x - high.astype(jnp.float32)
    mid = rest.astype(jnp.bfloat16)
    return high, mid, (rest - mid.astype(jnp.float32)).astype(jnp.bfloat16)


def stacked(solved):
    h, m, l = split(solved[...])
    return jnp.concatenate([h, m, h, l, m, h], axis=0)


def update(left, right):
    return jnp.dot(left, right, preferred_element_type=jnp.float32)


def begin(a, panel, solved, left):
    panel[...] = a[0:PIVOTS, :]
    solved[...] = jnp.zeros_like(solved)
    left[...] = jnp.zeros_like(left)


def flush(a, panel, solved, left):
    a[...] = a[...] - update(left[...], stacked(solved))
    a[a.shape[0] - PIVOTS :, :] = solved[...]


def invert(a, panel, solved, left, start, stop):
    size = a.shape[0]
    tiles = size // LANES
    each = LANES // PIVOTS
    row = lax.broadcasted_iota(jnp.int32, (PIVOTS, LANES), 0)
    lane = lax.broadcasted_iota(jnp.int32, (PIVOTS, LANES), 1)
    across = lax.broadcasted_iota(jnp.int32, (size, LANES), 1)
    parts = [slice(q * LANES, (q + 1) * LANES) for q in range(tiles)]

    def line(x, t):
        return jnp.broadcast_to(x[t : t + 1, :], (PIVOTS, LANES))

    def block(g):
        return pl.ds(pl.multiple_of(g * PIVOTS, PIVOTS), PIVOTS)

    def step(own, g, carry):
        at = g * PIVOTS - own * LANES
        place = lane - at
        inside = (place >= 0) & (place < PIVOTS)

        def columns(x):
            picked = [jnp.where(place == t, x, 0.0) for t in range(PIVOTS)]
            return [
                jnp.broadcast_to(jnp.sum(y, axis=1, keepdims=True), (PIVOTS, LANES))
                for y in picked
            ]

        rows = [panel[:, part] for part in parts]
        cols = columns(rows[own])
        right = stacked(solved)
        ahead = block(jnp.minimum(g + 1, size // PIVOTS - 1))
        stale = a[ahead, :] - update(left[ahead, :], right)
        stale = [stale[:, part] for part in parts]
        scales = columns(stale[own])
        stale[own] = jnp.where(inside, 0.0, stale[own])
        whole = update(left[...], right)
        behind = block(jnp.maximum(g - 1, 0))
        for q, part in enumerate(parts):
            kept, done = a[:, part] - whole[:, part], solved[:, part]
            if q == own:
                kept = jnp.where((across >= at) & (across < at + PIVOTS), 0.0, kept)
                done = jnp.where(inside, 0.0, done)
            a[:, part] = kept
            a[behind, part] = done
        beside = jnp.where(inside, 0.0, jnp.where(place < 0, -rows[own], rows[own]))
        h, m, l = split(
            jnp.concatenate([-x for x in rows[:own]] + [beside] + rows[own + 1 :], axis=1)
        )
        left[...] = jnp.concatenate([h, h, m, h, m, l], axis=0).T
        work = list(rows)
        work[own] = jnp.where(inside, jnp.where(place == row, 1.0, 0.0), rows[own])
        for t in range(PIVOTS):
            pivot = 1.0 / line(cols[t], t)
            factor = (cols[t] - jnp.where(row == t, 1.0, 0.0)) * pivot
            cols[t + 1 :] = [x - factor * line(x, t) for x in cols[t + 1 :]]
            work = [x - factor * line(x, t) for x in work]
        for q, part in enumerate(parts):
            fresh = stale[q]
            for t in range(PIVOTS):
                fresh = fresh - scales[t] * line(work[q], t)
            panel[:, part] = fresh
            solved[:, part] = work[q]
        return carry

    for q in range(tiles):
        low, high = max(start, q * each), min(stop, (q + 1) * each)
        if low < high:
            lax.fori_loop(low, high, functools.partial(step, q), 0)


def greet(sizes):
    barrier = pltpu.get_barrier_semaphore()
    for axis, n in sizes.items():
        me = lax.axis_index(axis)
        for d in range(1, n):
            pl.semaphore_signal(
                barrier, inc=1, device_id={axis: lax.rem(me + d, n)}, device_id_type=MESH
            )


def greeted(sizes):
    pl.semaphore_wait(pltpu.get_barrier_semaphore(), sum(n - 1 for n in sizes.values()))


def send(source, target, sems, device):
    pltpu.make_async_remote_copy(
        src_ref=source, dst_ref=target, send_sem=sems.at[0], recv_sem=sems.at[1],
        device_id=device, device_id_type=MESH,
    ).start()


def finish(exchange):
    view, sems = exchange
    if view is not None:
        for k in range(2):
            pltpu.make_async_copy(view, view, sems.at[k]).wait()


def span(index, chunk):
    return pl.ds(pl.multiple_of(index * chunk, 8), chunk)


def others(axis, n):
    me = lax.axis_index(axis)
    if n & (n - 1):
        return [lax.rem(me + d, n) for d in range(1, n)]
    peers = []
    for e in range(n - 1, 0, -1):
        peer = me
        for bit in (1 << k for k in range(n.bit_length() - 1)):
            if e & bit:
                peer = peer + bit - 2 * bit * lax.rem(me // bit, 2)
        peers.append(peer)
    return peers


def cuts_of(own_second, row):
    return max(1, min(CUTS, own_second // row // 8))


def scatter(axis, n, source, recv, sems, offset=0):
    me = lax.axis_index(axis)
    chunk = recv.shape[1]

    def of(peer):
        return pl.ds(pl.multiple_of(offset + peer * chunk, 8), chunk)

    for peer in others(axis, n):
        send(source.at[of(peer), :], recv.at[me], sems, {axis: peer})
    recv[me] = source[of(me), :]
    return recv.at[pl.ds(0, n - 1)], sems


def gather(axis, n, own, full, sems, offset=0):
    me = lax.axis_index(axis)
    chunk = own.shape[0]
    place = pl.ds(pl.multiple_of(offset + me * chunk, 8), chunk)
    full[place, :] = own
    for peer in others(axis, n):
        send(full.at[place, :], full.at[place, :], sems, {axis: peer})
    return full.at[pl.ds(0, (n - 1) * chunk), :], sems


def spread(axis, n, line, parts, sems):
    me = lax.axis_index(axis)
    one = pl.ds(0, 1)
    parts[me, 0:1, :] = line
    for peer in others(axis, n):
        send(parts.at[me, one, :], parts.at[me, one, :], sems, {axis: peer})
    return parts.at[pl.ds(0, n - 1), one, :], sems


def lots_out(sums, lots, recv, sems):
    n, few = lots.shape[:2]
    me = lax.axis_index("row")
    for d in range(n):
        lots[d] = sums[d * few : (d + 1) * few, :]
    recv[me] = lots[me]
    for peer in others("row", n):
        send(lots.at[peer], recv.at[me], sems, {"row": peer})
    return recv.at[pl.ds(0, n - 1)], sems


def lots_share(axis, n, own, full, sems):
    me = lax.axis_index(axis)
    full[me] = own
    for peer in others(axis, n):
        send(full.at[me], full.at[me], sems, {axis: peer})
    return full.at[pl.ds(0, n - 1)], sems


def total(recv):
    result = recv[0]
    for s in range(1, recv.shape[0]):
        result = result + recv[s]
    return result


def total_blocks(full, n):
    chunk = full.shape[0] // n
    result = full[0:chunk, :]
    for s in range(1, n):
        result = result + full[s * chunk : (s + 1) * chunk, :]
    return result


class Twin:
    def __init__(self, col):
        self.count = col // 2
        me = lax.axis_index("col")
        self.core = lax.rem(me, 2)
        self.chip = me // 2
        self.partner = {"col": self.chip * 2 + 1 - self.core}
        self.others = [
            {"col": lax.rem(self.chip + d, self.count) * 2 + self.core}
            for d in range(1, self.count)
        ]


def halves_out(twin, gram, recv, sems):
    half = gram.shape[0] // 2
    send(gram.at[span(1 - twin.core, half), :], recv, sems, twin.partner)
    return recv, sems


def halves_across(twin, gram, recv, across, sems):
    half = gram.shape[0] // 2
    across[twin.chip] = gram[span(twin.core, half), :] + recv[...]
    here = across.at[twin.chip]
    for peer in twin.others:
        send(here, here, sems, peer)
    view = across.at[pl.ds(0, twin.count - 1)] if twin.count > 1 else None
    return view, sems


def halves_back(twin, full, sems):
    half = full.shape[0] // 2
    mine = full.at[span(twin.core, half), :]
    send(mine, mine, sems, twin.partner)
    return mine, sems


def layout(sizes, frames, own_first, own_second, rank):
    row, col = sizes["row"], sizes["col"]
    square = (rank, rank)
    half = rank // 2
    chips = col // 2
    few = frames // row
    count = cuts_of(own_second, row)
    buffers = {
        "tens": (frames, own_first, own_second),
        "held": (frames, own_second, rank),
        "first": (own_first, rank), "second": (own_second, rank),
        "inv": square, "panel": (PIVOTS, rank), "solved": (PIVOTS, rank),
        "sums": (frames, rank),
        "gram_a": square, "recv_a": (row, half // row, rank), "full_a": square,
        "gram_b": square, "recv_b": (half, rank), "across_b": (chips, half, rank),
        "full_b": square,
        "terms_f": (own_first, rank), "recv_f": (col, own_first // col, rank),
        "full_f": (own_first, rank), "parts_w": (row, 8, rank),
    }
    pairs = ["a", "a2", "a3", "b", "b2", "b3", "f", "f2", "w"] + list("rdgi")
    pairs += [name + str(p) for p in range(PASSES) for name in "ch"]
    cuts = ["s", "t"]
    for p in range(PASSES):
        buffers.update({
            "lots_r%d" % p: (row, few, rank), "recv_r%d" % p: (row, few, rank),
            "parts_c%d" % p: (col, few, rank), "full_r%d" % p: (row, few, rank),
            "raw_s%d" % p: (own_second, rank),
            "gram_g%d" % p: square, "recv_g%d" % p: (half, rank),
            "across_g%d" % p: (chips, half, rank), "full_g%d" % p: square,
        })
        for q in range(count):
            buffers.update({
                "terms_s%d%d" % (p, q): (own_second // count, rank),
                "recv_s%d%d" % (p, q): (row, own_second // count // row, rank),
                "full_s%d%d" % (p, q): (own_second // count, rank),
            })
    names = list(buffers) + ["sem_" + name for name in pairs + cuts] + ["sem_load", "sem_move"]
    shapes = [pltpu.VMEM(shape, jnp.float32) for shape in buffers.values()]
    names.insert(len(shapes), "across_left")
    shapes.append(pltpu.VMEM((rank, 6 * PIVOTS), jnp.bfloat16))
    shapes += [pltpu.SemaphoreType.DMA((2,)) for name in pairs]
    shapes += [pltpu.SemaphoreType.DMA((count, 2)) for name in cuts]
    shapes += [pltpu.SemaphoreType.DMA((frames // math.gcd(frames, GROUP),))]
    shapes += [pltpu.SemaphoreType.DMA((2,))]
    return names, shapes


def kernel(sizes, names, tensor, first_in, second_in, first_out, second_out, frames_out, weights_out, *scratch):
    row, col = sizes["row"], sizes["col"]
    v = dict(zip(names, scratch))
    inv, sums, tens, held = v["inv"], v["sums"], v["tens"], v["held"]
    first, second = v["first"], v["second"]
    frames, own_first, own_second = tensor.shape
    rank = first.shape[1]
    half = rank // 2
    count = cuts_of(own_second, row)
    rows_first, rows_second = own_first * row, own_second * col
    steps = rank // PIVOTS
    twin = Twin(col)

    group = math.gcd(frames, GROUP)
    loads = frames // group

    def load(g):
        block = pl.ds(g * group, group)
        return pltpu.make_async_copy(tensor.at[block], tens.at[block], v["sem_load"].at[g])

    def move(source, target, at):
        copy = pltpu.make_async_copy(source, target, v["sem_move"].at[at])
        copy.start()
        return copy

    def contract(start, stop):
        def step(g, carry):
            load(g).wait()
            ks = [g * group + u for u in range(group)]
            parts = [cross(tens[k], first[...], HIGH) for k in ks]
            for k, part in zip(ks, parts):
                held[k] = part
                sums[pl.ds(k, 1), :] = jnp.sum(part * second[...], axis=0, keepdims=True)
            return carry

        lax.fori_loop(start, stop, step, 0)

    def frame_terms(raw, start, stop):
        def step(k, carry):
            sums[pl.ds(k, 1), :] = jnp.sum(held[k] * raw[...], axis=0, keepdims=True)
            return carry

        lax.fori_loop(start, stop, step, 0, unroll=4)

    def lines(q):
        small = own_second // row // count
        starts = [d * small * count + q * small for d in range(row)]
        return [slice(start, start + small) for start in starts]

    def second_terms(out, q):
        small = own_second // row // count
        zero = tuple(jnp.zeros((small, rank), jnp.float32) for _ in range(row))

        def step(k, totals):
            weight = frames_out[pl.ds(k, 1), :]
            return tuple(total + held[k, at, :] * weight for total, at in zip(totals, lines(q)))

        for d, total in enumerate(lax.fori_loop(0, frames, step, zero, unroll=4)):
            out[d * small : (d + 1) * small, :] = total

    def first_terms(raw, start, stop):
        group = math.gcd(stop - start, 4)

        def step(g, carry):
            base = start + g * group
            stacked = tens[pl.ds(base, group)].reshape(group * own_first, own_second)
            part = product(stacked, raw[...], HIGH)
            v["terms_f"][...] += sum(
                part[u * own_first : (u + 1) * own_first, :] * frames_out[pl.ds(base + u, 1), :]
                for u in range(group)
            )
            return carry

        lax.fori_loop(0, (stop - start) // group, step, 0)

    def frames_across(name):
        return lots_share(
            "col", col, total(v["recv_r" + name]), v["parts_c" + name], v["sem_c" + name]
        )

    def frames_back(name):
        return lots_share(
            "row", row, total(v["parts_c" + name]), v["full_r" + name], v["sem_d"]
        )

    def solve_frames(frame_sums, scale):
        raw = product(frame_sums * scale, inv[...], HIGH) * scale
        raw = raw * (1.0 / math.sqrt(rows_first * rows_second))
        normed = raw / jnp.sqrt(jnp.mean(raw * raw, axis=0, keepdims=True) + epsilon)
        frames_out[...] = normed

    state = (inv, v["panel"], v["solved"], v["across_left"])

    def unit(gram):
        down = lax.broadcasted_iota(jnp.int32, (rank, rank), 0)
        across = lax.broadcasted_iota(jnp.int32, (rank, rank), 1)
        diagonal = jnp.where(down == across, gram, 0.0)
        wide = 1.0 / jnp.sqrt(jnp.sum(diagonal, axis=0, keepdims=True))
        tall = 1.0 / jnp.sqrt(jnp.sum(diagonal, axis=1, keepdims=True))
        return gram * wide * tall, wide

    come = [move(first_in, first, 0)]
    greet(sizes)
    come.append(move(second_in, second, 1))
    come[0].wait()
    for g in range(loads):
        load(g).start()
    v["gram_a"][...] = cross(first[...], first[...], HIGH)
    greeted(sizes)
    offset = twin.core * half
    go_a = scatter("row", row, v["gram_a"], v["recv_a"], v["sem_a"], offset)
    come[1].wait()
    v["gram_b"][...] = cross(second[...], second[...], HIGH)
    go_b = halves_out(twin, v["gram_b"], v["recv_b"], v["sem_b"])
    contract(0, loads // 2)
    finish(go_b)
    go_b = halves_across(twin, v["gram_b"], v["recv_b"], v["across_b"], v["sem_b2"])
    contract(loads // 2, loads)
    go_r = lots_out(sums, v["lots_r0"], v["recv_r0"], v["sem_r"])
    finish(go_a)
    go_a = gather("row", row, total(v["recv_a"]), v["full_a"], v["sem_a2"], offset)
    finish(go_b)
    v["full_b"][span(twin.core, half), :] = total(v["across_b"])
    go_b = halves_back(twin, v["full_b"], v["sem_b3"])
    finish(go_r)
    go_c = frames_across("0")
    finish(go_b)
    second_gram, second_scale = unit(v["full_b"][...] * (1.0 / rows_second))
    finish(go_a)
    go_a = halves_back(twin, v["full_a"], v["sem_a3"])
    finish(go_a)
    first_gram = v["gram_a"]
    first_gram[...], first_scale = unit(v["full_a"][...] * (1.0 / rows_first))
    wide = None
    for p in range(PASSES):
        here = str(p)
        inv[...] = first_gram[...] * second_gram
        begin(*state)
        invert(*state, 0, steps // 8)
        finish(go_c)
        go_d = frames_back(here)
        invert(*state, steps // 8, steps)
        flush(*state)
        finish(go_d)
        full_r = v["full_r" + here]
        frame_sums = jnp.concatenate([full_r[d] for d in range(row)], axis=0)
        if wide is None:
            frame_scale = first_scale * second_scale
        else:
            frame_sums = frame_sums / wide
            frame_scale = first_scale
        solve_frames(frame_sums, frame_scale)
        parts = [here + str(q) for q in range(count)]
        go_s = []
        for q, part in enumerate(parts):
            second_terms(v["terms_s" + part], q)
            go_s.append(scatter(
                "row", row, v["terms_s" + part], v["recv_s" + part], v["sem_s"].at[q]
            ))
        frame_gram = cross(frames_out[...], frames_out[...], HIGH) * (1.0 / frames)
        inv[...] = first_gram[...] * frame_gram
        go_t = []
        at = 0
        begin(*state)
        for q, part in enumerate(parts):
            until = steps if q + 1 == count else min(steps, steps * (7 + q) // 8)
            if at < until:
                invert(*state, at, until)
                at = until
            finish(go_s[q])
            go_t.append(gather(
                "row", row, total(v["recv_s" + part]), v["full_s" + part], v["sem_t"].at[q]
            ))
        flush(*state)
        raw = v["raw_s" + here]
        gram_g, recv_g, across_g, full_g = (
            v[name + here] for name in ("gram_g", "recv_g", "across_g", "full_g")
        )
        for q, part in enumerate(parts):
            finish(go_t[q])
            some = product(v["full_s" + part][...] * first_scale, inv[...], HIGH) * (
                first_scale * (1.0 / math.sqrt(rows_first * frames))
            )
            small = some.shape[0] // row
            for d, place in enumerate(lines(q)):
                raw[place, :] = some[d * small : (d + 1) * small, :]
            terms = cross(some, some, HIGH)
            gram_g[...] = terms if q == 0 else gram_g[...] + terms
        go_g = halves_out(twin, gram_g, recv_g, v["sem_g"])
        last = p + 1 == PASSES
        if last:
            v["terms_f"][...] = jnp.zeros((own_first, rank), jnp.float32)
            first_terms(raw, 0, frames // 4)
        else:
            later = str(p + 1)
            frame_terms(raw, 0, frames)
            go_r = lots_out(sums, v["lots_r" + later], v["recv_r" + later], v["sem_r"])
        finish(go_g)
        go_g = halves_across(twin, gram_g, recv_g, across_g, v["sem_h" + here])
        if last:
            first_terms(raw, frames // 4, frames)
            go_f = scatter("col", col, v["terms_f"], v["recv_f"], v["sem_f"])
        else:
            finish(go_r)
            go_c = frames_across(later)
        finish(go_g)
        full_g[span(twin.core, half), :] = total(across_g)
        go_g = halves_back(twin, full_g, v["sem_i"])
        finish(go_g)
        gram = full_g[...] * (1.0 / rows_second)
        down = lax.broadcasted_iota(jnp.int32, (rank, rank), 0)
        across = lax.broadcasted_iota(jnp.int32, (rank, rank), 1)
        diagonal = jnp.where(down == across, gram, 0.0)
        wide = jnp.sqrt(jnp.sum(diagonal, axis=0, keepdims=True) + epsilon)
        tall = jnp.sqrt(jnp.sum(diagonal, axis=1, keepdims=True) + epsilon)
        second_gram = gram / wide / tall
    inv[...] = second_gram * frame_gram
    begin(*state)
    invert(*state, 0, steps // 8)
    finish(go_f)
    go_f = gather("col", col, total(v["recv_f"]), v["full_f"], v["sem_f2"])
    invert(*state, steps // 8, steps)
    flush(*state)
    finish(go_f)
    second_raw, raw = raw, product(v["full_f"][...] / wide, inv[...], HIGH) * (1.0 / math.sqrt(rows_second * frames))
    squares = jnp.sum(raw * raw, axis=0, keepdims=True)
    go_w = spread("row", row, squares, v["parts_w"], v["sem_w"])
    first_out[...] = raw
    second_out[...] = second_raw[...] / wide
    finish(go_w)
    weights = jnp.sqrt(total(v["parts_w"])[0:1, :] * (1.0 / rows_first) + epsilon)
    weights_out[...] = weights
    first_out[...] = first_out[...] / weights


def deliver(*refs):
    half = len(refs) // 2
    sems = refs[-1]
    copies = [
        pltpu.make_async_copy(source, target, sems.at[k])
        for k, (source, target) in enumerate(zip(refs[:half], refs[half : 2 * half]))
    ]
    for copy in copies:
        copy.start()
    for copy in copies:
        copy.wait()


def body(sizes, tensor, initial_first, initial_second):
    frames, own_first, own_second = tensor.shape
    rank = initial_first.shape[1]
    names, scratch = layout(sizes, frames, own_first, own_second, rank)
    far = pl.BlockSpec(memory_space=pltpu.HBM)
    near = pl.BlockSpec(memory_space=pltpu.VMEM)
    outs = ((own_first, rank), (own_second, rank), (frames, rank), (1, rank))
    shapes = [jax.ShapeDtypeStruct(shape, jnp.float32) for shape in outs]
    results = pl.pallas_call(
        functools.partial(kernel, sizes, names),
        out_shape=shapes,
        in_specs=[far] * 3,
        out_specs=[near] * len(outs),
        scratch_shapes=scratch,
        compiler_params=pltpu.CompilerParams(
            collective_id=0, has_side_effects=True, vmem_limit_bytes=48 * 1024 * 1024
        ),
        name="als",
    )(*[
        pltpu.with_memory_space_constraint(x, pltpu.HBM)
        for x in (tensor, initial_first, initial_second)
    ])
    results = pl.pallas_call(
        deliver,
        out_shape=shapes,
        in_specs=[near] * len(outs),
        out_specs=[far] * len(outs),
        scratch_shapes=[pltpu.SemaphoreType.DMA((len(outs),))],
        compiler_params=pltpu.CompilerParams(vmem_limit_bytes=1024 * 1024),
        name="deliver",
    )(*results)
    factor_first, second, factor_frames, weights = results
    return (factor_first, second, factor_frames, weights.reshape(rank))


def solution(mesh):
    sizes = {"row": mesh.shape["row"], "col": mesh.shape["col"]}
    placed = (P(None, "row", "col"), P("row", None), P("col", None))
    return jax.shard_map(
        functools.partial(body, sizes),
        mesh=mesh,
        in_specs=placed,
        out_specs=(P("row", None), P("col", None), P(), P()),
        check_vma=False,
    )
```

```python
import functools
import math

import jax
import jax.numpy as jnp
from jax import lax
from jax.experimental import pallas as pl
from jax.experimental.pallas import tpu as pltpu
from jax.sharding import PartitionSpec as P

PASSES = 2
LANES = 128
PIVOTS = 16
GROUP = 16
CUTS = 4
MESH = pl.DeviceIdType.MESH
HIGHEST = lax.Precision.HIGHEST
HIGH = lax.Precision.HIGH

epsilon = 1e-06


def product(a, b, precision=HIGHEST):
    return jnp.dot(a, b, precision=precision, preferred_element_type=jnp.float32)


def cross(a, b, precision=HIGHEST):
    return lax.dot_general(
        a, b, (((0,), (0,)), ((), ())), precision=precision, preferred_element_type=jnp.float32
    )


def split(x):
    high = x.astype(jnp.bfloat16)
    rest = x - high.astype(jnp.float32)
    mid = rest.astype(jnp.bfloat16)
    return high, mid, (rest - mid.astype(jnp.float32)).astype(jnp.bfloat16)


def stacked(solved):
    h, m, l = split(solved[...])
    return jnp.concatenate([h, m, h, l, m, h], axis=0)


def update(left, right):
    return jnp.dot(left, right, preferred_element_type=jnp.float32)


def begin(a, panel, solved, left):
    panel[...] = a[0:PIVOTS, :]
    solved[...] = jnp.zeros_like(solved)
    left[...] = jnp.zeros_like(left)


def flush(a, panel, solved, left):
    a[...] = a[...] - update(left[...], stacked(solved))
    a[a.shape[0] - PIVOTS :, :] = solved[...]


def invert(a, panel, solved, left, start, stop):
    size = a.shape[0]
    tiles = size // LANES
    each = LANES // PIVOTS
    row = lax.broadcasted_iota(jnp.int32, (PIVOTS, LANES), 0)
    lane = lax.broadcasted_iota(jnp.int32, (PIVOTS, LANES), 1)
    across = lax.broadcasted_iota(jnp.int32, (size, LANES), 1)
    parts = [slice(q * LANES, (q + 1) * LANES) for q in range(tiles)]

    def line(x, t):
        return jnp.broadcast_to(x[t : t + 1, :], (PIVOTS, LANES))

    def block(g):
        return pl.ds(pl.multiple_of(g * PIVOTS, PIVOTS), PIVOTS)

    def step(own, g, carry):
        at = g * PIVOTS - own * LANES
        place = lane - at
        inside = (place >= 0) & (place < PIVOTS)

        def columns(x):
            picked = [jnp.where(place == t, x, 0.0) for t in range(PIVOTS)]
            return [
                jnp.broadcast_to(jnp.sum(y, axis=1, keepdims=True), (PIVOTS, LANES))
                for y in picked
            ]

        rows = [panel[:, part] for part in parts]
        cols = columns(rows[own])
        right = stacked(solved)
        ahead = block(jnp.minimum(g + 1, size // PIVOTS - 1))
        stale = a[ahead, :] - update(left[ahead, :], right)
        stale = [stale[:, part] for part in parts]
        scales = columns(stale[own])
        stale[own] = jnp.where(inside, 0.0, stale[own])
        whole = update(left[...], right)
        behind = block(jnp.maximum(g - 1, 0))
        for q, part in enumerate(parts):
            kept, done = a[:, part] - whole[:, part], solved[:, part]
            if q == own:
                kept = jnp.where((across >= at) & (across < at + PIVOTS), 0.0, kept)
                done = jnp.where(inside, 0.0, done)
            a[:, part] = kept
            a[behind, part] = done
        beside = jnp.where(inside, 0.0, jnp.where(place < 0, -rows[own], rows[own]))
        h, m, l = split(
            jnp.concatenate([-x for x in rows[:own]] + [beside] + rows[own + 1 :], axis=1)
        )
        left[...] = jnp.concatenate([h, h, m, h, m, l], axis=0).T
        work = list(rows)
        work[own] = jnp.where(inside, jnp.where(place == row, 1.0, 0.0), rows[own])
        for t in range(PIVOTS):
            pivot = 1.0 / line(cols[t], t)
            factor = (cols[t] - jnp.where(row == t, 1.0, 0.0)) * pivot
            cols[t + 1 :] = [x - factor * line(x, t) for x in cols[t + 1 :]]
            work = [x - factor * line(x, t) for x in work]
        for q, part in enumerate(parts):
            fresh = stale[q]
            for t in range(PIVOTS):
                fresh = fresh - scales[t] * line(work[q], t)
            panel[:, part] = fresh
            solved[:, part] = work[q]
        return carry

    for q in range(tiles):
        low, high = max(start, q * each), min(stop, (q + 1) * each)
        if low < high:
            lax.fori_loop(low, high, functools.partial(step, q), 0)


def greet(sizes):
    barrier = pltpu.get_barrier_semaphore()
    for axis, n in sizes.items():
        me = lax.axis_index(axis)
        for d in range(1, n):
            pl.semaphore_signal(
                barrier, inc=1, device_id={axis: lax.rem(me + d, n)}, device_id_type=MESH
            )


def greeted(sizes):
    pl.semaphore_wait(pltpu.get_barrier_semaphore(), sum(n - 1 for n in sizes.values()))


def send(source, target, sems, device):
    pltpu.make_async_remote_copy(
        src_ref=source, dst_ref=target, send_sem=sems.at[0], recv_sem=sems.at[1],
        device_id=device, device_id_type=MESH,
    ).start()


def finish(exchange):
    view, sems = exchange
    if view is not None:
        for k in range(2):
            pltpu.make_async_copy(view, view, sems.at[k]).wait()


def span(index, chunk):
    return pl.ds(pl.multiple_of(index * chunk, 8), chunk)


def others(axis, n):
    me = lax.axis_index(axis)
    if n & (n - 1):
        return [lax.rem(me + d, n) for d in range(1, n)]
    peers = []
    for e in range(n - 1, 0, -1):
        peer = me
        for bit in (1 << k for k in range(n.bit_length() - 1)):
            if e & bit:
                peer = peer + bit - 2 * bit * lax.rem(me // bit, 2)
        peers.append(peer)
    return peers


def cuts_of(own_second, row):
    return max(1, min(CUTS, own_second // row // 8))


def scatter(axis, n, source, recv, sems, offset=0):
    me = lax.axis_index(axis)
    chunk = recv.shape[1]

    def of(peer):
        return pl.ds(pl.multiple_of(offset + peer * chunk, 8), chunk)

    for peer in others(axis, n):
        send(source.at[of(peer), :], recv.at[me], sems, {axis: peer})
    recv[me] = source[of(me), :]
    return recv.at[pl.ds(0, n - 1)], sems


def gather(axis, n, own, full, sems, offset=0):
    me = lax.axis_index(axis)
    chunk = own.shape[0]
    place = pl.ds(pl.multiple_of(offset + me * chunk, 8), chunk)
    full[place, :] = own
    for peer in others(axis, n):
        send(full.at[place, :], full.at[place, :], sems, {axis: peer})
    return full.at[pl.ds(0, (n - 1) * chunk), :], sems


def spread(axis, n, line, parts, sems):
    me = lax.axis_index(axis)
    one = pl.ds(0, 1)
    parts[me, 0:1, :] = line
    for peer in others(axis, n):
        send(parts.at[me, one, :], parts.at[me, one, :], sems, {axis: peer})
    return parts.at[pl.ds(0, n - 1), one, :], sems


def lots_out(sums, lots, recv, sems):
    n, few = lots.shape[:2]
    me = lax.axis_index("row")
    for d in range(n):
        lots[d] = sums[d * few : (d + 1) * few, :]
    recv[me] = lots[me]
    for peer in others("row", n):
        send(lots.at[peer], recv.at[me], sems, {"row": peer})
    return recv.at[pl.ds(0, n - 1)], sems


def lots_share(axis, n, own, full, sems):
    me = lax.axis_index(axis)
    full[me] = own
    for peer in others(axis, n):
        send(full.at[me], full.at[me], sems, {axis: peer})
    return full.at[pl.ds(0, n - 1)], sems


def total(recv):
    result = recv[0]
    for s in range(1, recv.shape[0]):
        result = result + recv[s]
    return result


def total_blocks(full, n):
    chunk = full.shape[0] // n
    result = full[0:chunk, :]
    for s in range(1, n):
        result = result + full[s * chunk : (s + 1) * chunk, :]
    return result


class Twin:
    def __init__(self, col):
        self.count = col // 2
        me = lax.axis_index("col")
        self.core = lax.rem(me, 2)
        self.chip = me // 2
        self.partner = {"col": self.chip * 2 + 1 - self.core}
        self.others = [
            {"col": lax.rem(self.chip + d, self.count) * 2 + self.core}
            for d in range(1, self.count)
        ]


def halves_out(twin, gram, recv, sems):
    half = gram.shape[0] // 2
    send(gram.at[span(1 - twin.core, half), :], recv, sems, twin.partner)
    return recv, sems


def halves_across(twin, gram, recv, across, sems):
    half = gram.shape[0] // 2
    across[twin.chip] = gram[span(twin.core, half), :] + recv[...]
    here = across.at[twin.chip]
    for peer in twin.others:
        send(here, here, sems, peer)
    view = across.at[pl.ds(0, twin.count - 1)] if twin.count > 1 else None
    return view, sems


def halves_back(twin, full, sems):
    half = full.shape[0] // 2
    mine = full.at[span(twin.core, half), :]
    send(mine, mine, sems, twin.partner)
    return mine, sems


def layout(sizes, frames, own_first, own_second, rank):
    row, col = sizes["row"], sizes["col"]
    square = (rank, rank)
    half = rank // 2
    chips = col // 2
    few = frames // row
    count = cuts_of(own_second, row)
    buffers = {
        "tens": (frames, own_first, own_second),
        "held": (frames, own_second, rank),
        "first": (own_first, rank), "second": (own_second, rank),
        "inv": square, "panel": (PIVOTS, rank), "solved": (PIVOTS, rank),
        "sums": (frames, rank),
        "gram_a": square, "recv_a": (row, half // row, rank), "full_a": square,
        "gram_b": square, "recv_b": (half, rank), "across_b": (chips, half, rank),
        "full_b": square,
        "terms_f": (own_first, rank), "recv_f": (col, own_first // col, rank),
        "full_f": (own_first, rank), "parts_w": (row, 8, rank),
    }
    pairs = ["a", "a2", "a3", "b", "b2", "b3", "f", "f2", "w"] + list("rdgi")
    pairs += [name + str(p) for p in range(PASSES) for name in "ch"]
    cuts = ["s", "t"]
    for p in range(PASSES):
        buffers.update({
            "lots_r%d" % p: (row, few, rank), "recv_r%d" % p: (row, few, rank),
            "parts_c%d" % p: (col, few, rank), "full_r%d" % p: (row, few, rank),
            "raw_s%d" % p: (own_second, rank),
            "gram_g%d" % p: square, "recv_g%d" % p: (half, rank),
            "across_g%d" % p: (chips, half, rank), "full_g%d" % p: square,
        })
        for q in range(count):
            buffers.update({
                "terms_s%d%d" % (p, q): (own_second // count, rank),
                "recv_s%d%d" % (p, q): (row, own_second // count // row, rank),
                "full_s%d%d" % (p, q): (own_second // count, rank),
            })
    names = list(buffers) + ["sem_" + name for name in pairs + cuts] + ["sem_load", "sem_move"]
    shapes = [pltpu.VMEM(shape, jnp.float32) for shape in buffers.values()]
    names.insert(len(shapes), "across_left")
    shapes.append(pltpu.VMEM((rank, 6 * PIVOTS), jnp.bfloat16))
    shapes += [pltpu.SemaphoreType.DMA((2,)) for name in pairs]
    shapes += [pltpu.SemaphoreType.DMA((count, 2)) for name in cuts]
    shapes += [pltpu.SemaphoreType.DMA((frames // math.gcd(frames, GROUP),))]
    shapes += [pltpu.SemaphoreType.DMA((2,))]
    return names, shapes


def kernel(sizes, names, tensor, first_in, second_in, first_out, second_out, frames_out, weights_out, *scratch):
    row, col = sizes["row"], sizes["col"]
    v = dict(zip(names, scratch))
    inv, sums, tens, held = v["inv"], v["sums"], v["tens"], v["held"]
    first, second = v["first"], v["second"]
    frames, own_first, own_second = tensor.shape
    rank = first.shape[1]
    half = rank // 2
    count = cuts_of(own_second, row)
    rows_first, rows_second = own_first * row, own_second * col
    steps = rank // PIVOTS
    twin = Twin(col)

    group = math.gcd(frames, GROUP)
    loads = frames // group

    def load(g):
        block = pl.ds(g * group, group)
        return pltpu.make_async_copy(tensor.at[block], tens.at[block], v["sem_load"].at[g])

    def move(source, target, at):
        copy = pltpu.make_async_copy(source, target, v["sem_move"].at[at])
        copy.start()
        return copy

    def contract(start, stop):
        def step(g, carry):
            load(g).wait()
            ks = [g * group + u for u in range(group)]
            parts = [cross(tens[k], first[...], HIGH) for k in ks]
            for k, part in zip(ks, parts):
                held[k] = part
                sums[pl.ds(k, 1), :] = jnp.sum(part * second[...], axis=0, keepdims=True)
            return carry

        lax.fori_loop(start, stop, step, 0)

    def frame_terms(raw, start, stop):
        def step(k, carry):
            sums[pl.ds(k, 1), :] = jnp.sum(held[k] * raw[...], axis=0, keepdims=True)
            return carry

        lax.fori_loop(start, stop, step, 0, unroll=4)

    def lines(q):
        small = own_second // row // count
        starts = [d * small * count + q * small for d in range(row)]
        return [slice(start, start + small) for start in starts]

    def second_terms(out, q):
        small = own_second // row // count
        zero = tuple(jnp.zeros((small, rank), jnp.float32) for _ in range(row))

        def step(k, totals):
            weight = frames_out[pl.ds(k, 1), :]
            return tuple(total + held[k, at, :] * weight for total, at in zip(totals, lines(q)))

        for d, total in enumerate(lax.fori_loop(0, frames, step, zero, unroll=4)):
            out[d * small : (d + 1) * small, :] = total

    def first_terms(raw, start, stop):
        group = math.gcd(stop - start, 4)

        def step(g, carry):
            base = start + g * group
            stacked = tens[pl.ds(base, group)].reshape(group * own_first, own_second)
            part = product(stacked, raw[...], HIGH)
            v["terms_f"][...] += sum(
                part[u * own_first : (u + 1) * own_first, :] * frames_out[pl.ds(base + u, 1), :]
                for u in range(group)
            )
            return carry

        lax.fori_loop(0, (stop - start) // group, step, 0)

    def frames_across(name):
        return lots_share(
            "col", col, total(v["recv_r" + name]), v["parts_c" + name], v["sem_c" + name]
        )

    def frames_back(name):
        return lots_share(
            "row", row, total(v["parts_c" + name]), v["full_r" + name], v["sem_d"]
        )

    def solve_frames(frame_sums, scale):
        raw = product(frame_sums * scale, inv[...], HIGH) * scale
        raw = raw * (1.0 / math.sqrt(rows_first * rows_second))
        normed = raw / jnp.sqrt(jnp.mean(raw * raw, axis=0, keepdims=True) + epsilon)
        frames_out[...] = normed

    state = (inv, v["panel"], v["solved"], v["across_left"])

    def unit(gram):
        down = lax.broadcasted_iota(jnp.int32, (rank, rank), 0)
        across = lax.broadcasted_iota(jnp.int32, (rank, rank), 1)
        diagonal = jnp.where(down == across, gram, 0.0)
        wide = 1.0 / jnp.sqrt(jnp.sum(diagonal, axis=0, keepdims=True))
        tall = 1.0 / jnp.sqrt(jnp.sum(diagonal, axis=1, keepdims=True))
        return gram * wide * tall, wide

    come = [move(first_in, first, 0)]
    greet(sizes)
    come.append(move(second_in, second, 1))
    come[0].wait()
    for g in range(loads):
        load(g).start()
    v["gram_a"][...] = cross(first[...], first[...], HIGH)
    greeted(sizes)
    offset = twin.core * half
    go_a = scatter("row", row, v["gram_a"], v["recv_a"], v["sem_a"], offset)
    come[1].wait()
    v["gram_b"][...] = cross(second[...], second[...], HIGH)
    go_b = halves_out(twin, v["gram_b"], v["recv_b"], v["sem_b"])
    contract(0, loads // 2)
    finish(go_b)
    go_b = halves_across(twin, v["gram_b"], v["recv_b"], v["across_b"], v["sem_b2"])
    contract(loads // 2, loads)
    go_r = lots_out(sums, v["lots_r0"], v["recv_r0"], v["sem_r"])
    finish(go_a)
    go_a = gather("row", row, total(v["recv_a"]), v["full_a"], v["sem_a2"], offset)
    finish(go_b)
    v["full_b"][span(twin.core, half), :] = total(v["across_b"])
    go_b = halves_back(twin, v["full_b"], v["sem_b3"])
    finish(go_r)
    go_c = frames_across("0")
    finish(go_b)
    second_gram, second_scale = unit(v["full_b"][...] * (1.0 / rows_second))
    finish(go_a)
    go_a = halves_back(twin, v["full_a"], v["sem_a3"])
    finish(go_a)
    first_gram = v["gram_a"]
    first_gram[...], first_scale = unit(v["full_a"][...] * (1.0 / rows_first))
    wide = None
    for p in range(PASSES):
        here = str(p)
        inv[...] = first_gram[...] * second_gram
        begin(*state)
        invert(*state, 0, steps // 8)
        finish(go_c)
        go_d = frames_back(here)
        invert(*state, steps // 8, steps)
        flush(*state)
        finish(go_d)
        full_r = v["full_r" + here]
        frame_sums = jnp.concatenate([full_r[d] for d in range(row)], axis=0)
        if wide is None:
            frame_scale = first_scale * second_scale
        else:
            frame_sums = frame_sums / wide
            frame_scale = first_scale
        solve_frames(frame_sums, frame_scale)
        parts = [here + str(q) for q in range(count)]
        go_s = []
        for q, part in enumerate(parts):
            second_terms(v["terms_s" + part], q)
            go_s.append(scatter(
                "row", row, v["terms_s" + part], v["recv_s" + part], v["sem_s"].at[q]
            ))
        frame_gram = cross(frames_out[...], frames_out[...], HIGH) * (1.0 / frames)
        inv[...] = first_gram[...] * frame_gram
        go_t = []
        at = 0
        begin(*state)
        for q, part in enumerate(parts):
            until = steps if q + 1 == count else min(steps, steps * (7 + q) // 8)
            if at < until:
                invert(*state, at, until)
                at = until
            finish(go_s[q])
            go_t.append(gather(
                "row", row, total(v["recv_s" + part]), v["full_s" + part], v["sem_t"].at[q]
            ))
        flush(*state)
        raw = v["raw_s" + here]
        gram_g, recv_g, across_g, full_g = (
            v[name + here] for name in ("gram_g", "recv_g", "across_g", "full_g")
        )
        for q, part in enumerate(parts):
            finish(go_t[q])
            some = product(v["full_s" + part][...] * first_scale, inv[...], HIGH) * (
                first_scale * (1.0 / math.sqrt(rows_first * frames))
            )
            small = some.shape[0] // row
            for d, place in enumerate(lines(q)):
                raw[place, :] = some[d * small : (d + 1) * small, :]
            terms = cross(some, some, HIGH)
            gram_g[...] = terms if q == 0 else gram_g[...] + terms
        go_g = halves_out(twin, gram_g, recv_g, v["sem_g"])
        last = p + 1 == PASSES
        if last:
            v["terms_f"][...] = jnp.zeros((own_first, rank), jnp.float32)
            first_terms(raw, 0, frames // 4)
        else:
            later = str(p + 1)
            frame_terms(raw, 0, frames)
            go_r = lots_out(sums, v["lots_r" + later], v["recv_r" + later], v["sem_r"])
        finish(go_g)
        go_g = halves_across(twin, gram_g, recv_g, across_g, v["sem_h" + here])
        if last:
            first_terms(raw, frames // 4, frames)
            go_f = scatter("col", col, v["terms_f"], v["recv_f"], v["sem_f"])
        else:
            finish(go_r)
            go_c = frames_across(later)
        finish(go_g)
        full_g[span(twin.core, half), :] = total(across_g)
        go_g = halves_back(twin, full_g, v["sem_i"])
        finish(go_g)
        gram = full_g[...] * (1.0 / rows_second)
        down = lax.broadcasted_iota(jnp.int32, (rank, rank), 0)
        across = lax.broadcasted_iota(jnp.int32, (rank, rank), 1)
        diagonal = jnp.where(down == across, gram, 0.0)
        wide = jnp.sqrt(jnp.sum(diagonal, axis=0, keepdims=True) + epsilon)
        tall = jnp.sqrt(jnp.sum(diagonal, axis=1, keepdims=True) + epsilon)
        second_gram = gram / wide / tall
    inv[...] = second_gram * frame_gram
    begin(*state)
    invert(*state, 0, steps // 8)
    finish(go_f)
    go_f = gather("col", col, total(v["recv_f"]), v["full_f"], v["sem_f2"])
    invert(*state, steps // 8, steps)
    flush(*state)
    finish(go_f)
    second_raw, raw = raw, product(v["full_f"][...] / wide, inv[...], HIGH) * (1.0 / math.sqrt(rows_second * frames))
    squares = jnp.sum(raw * raw, axis=0, keepdims=True)
    go_w = spread("row", row, squares, v["parts_w"], v["sem_w"])
    first_out[...] = raw
    second_out[...] = second_raw[...] / wide
    finish(go_w)
    weights = jnp.sqrt(total(v["parts_w"])[0:1, :] * (1.0 / rows_first) + epsilon)
    weights_out[...] = weights
    first_out[...] = first_out[...] / weights


def deliver(*refs):
    half = len(refs) // 2
    sems = refs[-1]
    copies = [
        pltpu.make_async_copy(source, target, sems.at[k])
        for k, (source, target) in enumerate(zip(refs[:half], refs[half : 2 * half]))
    ]
    for copy in copies:
        copy.start()
    for copy in copies:
        copy.wait()


def body(sizes, tensor, initial_first, initial_second):
    frames, own_first, own_second = tensor.shape
    rank = initial_first.shape[1]
    names, scratch = layout(sizes, frames, own_first, own_second, rank)
    far = pl.BlockSpec(memory_space=pltpu.HBM)
    near = pl.BlockSpec(memory_space=pltpu.VMEM)
    outs = ((own_first, rank), (own_second, rank), (frames, rank), (1, rank))
    shapes = [jax.ShapeDtypeStruct(shape, jnp.float32) for shape in outs]
    results = pl.pallas_call(
        functools.partial(kernel, sizes, names),
        out_shape=shapes,
        in_specs=[far] * 3,
        out_specs=[near] * len(outs),
        scratch_shapes=scratch,
        compiler_params=pltpu.CompilerParams(
            collective_id=0, has_side_effects=True, vmem_limit_bytes=48 * 1024 * 1024
        ),
        name="als",
    )(*[
        pltpu.with_memory_space_constraint(x, pltpu.HBM)
        for x in (tensor, initial_first, initial_second)
    ])
    results = pl.pallas_call(
        deliver,
        out_shape=shapes,
        in_specs=[near] * len(outs),
        out_specs=[far] * len(outs),
        scratch_shapes=[pltpu.SemaphoreType.DMA((len(outs),))],
        compiler_params=pltpu.CompilerParams(vmem_limit_bytes=1024 * 1024),
        name="deliver",
    )(*results)
    factor_first, second, factor_frames, weights = results
    return (factor_first, second, factor_frames, weights.reshape(rank))


def solution(mesh):
    sizes = {"row": mesh.shape["row"], "col": mesh.shape["col"]}
    placed = (P(None, "row", "col"), P("row", None), P("col", None))
    return jax.shard_map(
        functools.partial(body, sizes),
        mesh=mesh,
        in_specs=placed,
        out_specs=(P("row", None), P("col", None), P(), P()),
        check_vma=False,
    )
```

```python
import functools
import math

import jax
import jax.numpy as jnp
from jax import lax
from jax.experimental import pallas as pl
from jax.experimental.pallas import tpu as pltpu
from jax.sharding import PartitionSpec as P

PASSES = 2
LANES = 128
PIVOTS = 16
GROUP = 16
CUTS = 4
MESH = pl.DeviceIdType.MESH
HIGHEST = lax.Precision.HIGHEST
HIGH = lax.Precision.HIGH

epsilon = 1e-06


def product(a, b, precision=HIGHEST):
    return jnp.dot(a, b, precision=precision, preferred_element_type=jnp.float32)


def cross(a, b, precision=HIGHEST):
    return lax.dot_general(
        a, b, (((0,), (0,)), ((), ())), precision=precision, preferred_element_type=jnp.float32
    )


def split(x):
    high = x.astype(jnp.bfloat16)
    rest = x - high.astype(jnp.float32)
    mid = rest.astype(jnp.bfloat16)
    return high, mid, (rest - mid.astype(jnp.float32)).astype(jnp.bfloat16)


def stacked(solved):
    h, m, l = split(solved[...])
    return jnp.concatenate([h, m, h, l, m, h], axis=0)


def update(left, right):
    return jnp.dot(left, right, preferred_element_type=jnp.float32)


def begin(a, panel, solved, left):
    panel[...] = a[0:PIVOTS, :]
    solved[...] = jnp.zeros_like(solved)
    left[...] = jnp.zeros_like(left)


def flush(a, panel, solved, left):
    a[...] = a[...] - update(left[...], stacked(solved))
    a[a.shape[0] - PIVOTS :, :] = solved[...]


def invert(a, panel, solved, left, start, stop):
    size = a.shape[0]
    tiles = size // LANES
    each = LANES // PIVOTS
    row = lax.broadcasted_iota(jnp.int32, (PIVOTS, LANES), 0)
    lane = lax.broadcasted_iota(jnp.int32, (PIVOTS, LANES), 1)
    across = lax.broadcasted_iota(jnp.int32, (size, LANES), 1)
    parts = [slice(q * LANES, (q + 1) * LANES) for q in range(tiles)]

    def line(x, t):
        return jnp.broadcast_to(x[t : t + 1, :], (PIVOTS, LANES))

    def block(g):
        return pl.ds(pl.multiple_of(g * PIVOTS, PIVOTS), PIVOTS)

    def step(own, g, carry):
        at = g * PIVOTS - own * LANES
        place = lane - at
        inside = (place >= 0) & (place < PIVOTS)

        def columns(x):
            picked = [jnp.where(place == t, x, 0.0) for t in range(PIVOTS)]
            return [
                jnp.broadcast_to(jnp.sum(y, axis=1, keepdims=True), (PIVOTS, LANES))
                for y in picked
            ]

        rows = [panel[:, part] for part in parts]
        cols = columns(rows[own])
        right = stacked(solved)
        ahead = block(jnp.minimum(g + 1, size // PIVOTS - 1))
        stale = a[ahead, :] - update(left[ahead, :], right)
        stale = [stale[:, part] for part in parts]
        scales = columns(stale[own])
        stale[own] = jnp.where(inside, 0.0, stale[own])
        whole = update(left[...], right)
        behind = block(jnp.maximum(g - 1, 0))
        for q, part in enumerate(parts):
            kept, done = a[:, part] - whole[:, part], solved[:, part]
            if q == own:
                kept = jnp.where((across >= at) & (across < at + PIVOTS), 0.0, kept)
                done = jnp.where(inside, 0.0, done)
            a[:, part] = kept
            a[behind, part] = done
        beside = jnp.where(inside, 0.0, jnp.where(place < 0, -rows[own], rows[own]))
        h, m, l = split(
            jnp.concatenate([-x for x in rows[:own]] + [beside] + rows[own + 1 :], axis=1)
        )
        left[...] = jnp.concatenate([h, h, m, h, m, l], axis=0).T
        work = list(rows)
        work[own] = jnp.where(inside, jnp.where(place == row, 1.0, 0.0), rows[own])
        for t in range(PIVOTS):
            pivot = 1.0 / line(cols[t], t)
            factor = (cols[t] - jnp.where(row == t, 1.0, 0.0)) * pivot
            cols[t + 1 :] = [x - factor * line(x, t) for x in cols[t + 1 :]]
            work = [x - factor * line(x, t) for x in work]
        for q, part in enumerate(parts):
            fresh = stale[q]
            for t in range(PIVOTS):
                fresh = fresh - scales[t] * line(work[q], t)
            panel[:, part] = fresh
            solved[:, part] = work[q]
        return carry

    for q in range(tiles):
        low, high = max(start, q * each), min(stop, (q + 1) * each)
        if low < high:
            lax.fori_loop(low, high, functools.partial(step, q), 0)


def greet(sizes):
    barrier = pltpu.get_barrier_semaphore()
    for axis, n in sizes.items():
        me = lax.axis_index(axis)
        for d in range(1, n):
            pl.semaphore_signal(
                barrier, inc=1, device_id={axis: lax.rem(me + d, n)}, device_id_type=MESH
            )


def greeted(sizes):
    pl.semaphore_wait(pltpu.get_barrier_semaphore(), sum(n - 1 for n in sizes.values()))


def send(source, target, sems, device):
    pltpu.make_async_remote_copy(
        src_ref=source, dst_ref=target, send_sem=sems.at[0], recv_sem=sems.at[1],
        device_id=device, device_id_type=MESH,
    ).start()


def finish(exchange):
    view, sems = exchange
    if view is not None:
        for k in range(2):
            pltpu.make_async_copy(view, view, sems.at[k]).wait()


def span(index, chunk):
    return pl.ds(pl.multiple_of(index * chunk, 8), chunk)


def others(axis, n):
    me = lax.axis_index(axis)
    if n & (n - 1):
        return [lax.rem(me + d, n) for d in range(1, n)]
    peers = []
    for e in range(n - 1, 0, -1):
        peer = me
        for bit in (1 << k for k in range(n.bit_length() - 1)):
            if e & bit:
                peer = peer + bit - 2 * bit * lax.rem(me // bit, 2)
        peers.append(peer)
    return peers


def cuts_of(own_second, row):
    return max(1, min(CUTS, own_second // row // 8))


def scatter(axis, n, source, recv, sems, offset=0):
    me = lax.axis_index(axis)
    chunk = recv.shape[1]

    def of(peer):
        return pl.ds(pl.multiple_of(offset + peer * chunk, 8), chunk)

    for peer in others(axis, n):
        send(source.at[of(peer), :], recv.at[me], sems, {axis: peer})
    recv[me] = source[of(me), :]
    return recv.at[pl.ds(0, n - 1)], sems


def gather(axis, n, own, full, sems, offset=0):
    me = lax.axis_index(axis)
    chunk = own.shape[0]
    place = pl.ds(pl.multiple_of(offset + me * chunk, 8), chunk)
    full[place, :] = own
    for peer in others(axis, n):
        send(full.at[place, :], full.at[place, :], sems, {axis: peer})
    return full.at[pl.ds(0, (n - 1) * chunk), :], sems


def spread(axis, n, line, parts, sems):
    me = lax.axis_index(axis)
    one = pl.ds(0, 1)
    parts[me, 0:1, :] = line
    for peer in others(axis, n):
        send(parts.at[me, one, :], parts.at[me, one, :], sems, {axis: peer})
    return parts.at[pl.ds(0, n - 1), one, :], sems


def lots_out(sums, lots, recv, sems):
    n, few = lots.shape[:2]
    me = lax.axis_index("row")
    for d in range(n):
        lots[d] = sums[d * few : (d + 1) * few, :]
    recv[me] = lots[me]
    for peer in others("row", n):
        send(lots.at[peer], recv.at[me], sems, {"row": peer})
    return recv.at[pl.ds(0, n - 1)], sems


def lots_share(axis, n, own, full, sems):
    me = lax.axis_index(axis)
    full[me] = own
    for peer in others(axis, n):
        send(full.at[me], full.at[me], sems, {axis: peer})
    return full.at[pl.ds(0, n - 1)], sems


def total(recv):
    result = recv[0]
    for s in range(1, recv.shape[0]):
        result = result + recv[s]
    return result


def total_blocks(full, n):
    chunk = full.shape[0] // n
    result = full[0:chunk, :]
    for s in range(1, n):
        result = result + full[s * chunk : (s + 1) * chunk, :]
    return result


class Twin:
    def __init__(self, col):
        self.count = col // 2
        me = lax.axis_index("col")
        self.core = lax.rem(me, 2)
        self.chip = me // 2
        self.partner = {"col": self.chip * 2 + 1 - self.core}
        self.others = [
            {"col": lax.rem(self.chip + d, self.count) * 2 + self.core}
            for d in range(1, self.count)
        ]


def halves_out(twin, gram, recv, sems):
    half = gram.shape[0] // 2
    send(gram.at[span(1 - twin.core, half), :], recv, sems, twin.partner)
    return recv, sems


def halves_across(twin, gram, recv, across, sems):
    half = gram.shape[0] // 2
    across[twin.chip] = gram[span(twin.core, half), :] + recv[...]
    here = across.at[twin.chip]
    for peer in twin.others:
        send(here, here, sems, peer)
    view = across.at[pl.ds(0, twin.count - 1)] if twin.count > 1 else None
    return view, sems


def halves_back(twin, full, sems):
    half = full.shape[0] // 2
    mine = full.at[span(twin.core, half), :]
    send(mine, mine, sems, twin.partner)
    return mine, sems


def layout(sizes, frames, own_first, own_second, rank):
    row, col = sizes["row"], sizes["col"]
    square = (rank, rank)
    half = rank // 2
    chips = col // 2
    few = frames // row
    count = cuts_of(own_second, row)
    buffers = {
        "tens": (frames, own_first, own_second),
        "held": (frames, own_second, rank),
        "first": (own_first, rank), "second": (own_second, rank),
        "inv": square, "panel": (PIVOTS, rank), "solved": (PIVOTS, rank),
        "sums": (frames, rank),
        "gram_a": square, "recv_a": (row, half // row, rank), "full_a": square,
        "gram_b": square, "recv_b": (half, rank), "across_b": (chips, half, rank),
        "full_b": square,
        "terms_f": (own_first, rank), "recv_f": (col, own_first // col, rank),
        "full_f": (own_first, rank), "parts_w": (row, 8, rank),
    }
    pairs = ["a", "a2", "a3", "b", "b2", "b3", "f", "f2", "w"] + list("rdgi")
    pairs += [name + str(p) for p in range(PASSES) for name in "ch"]
    cuts = ["s", "t"]
    for p in range(PASSES):
        buffers.update({
            "lots_r%d" % p: (row, few, rank), "recv_r%d" % p: (row, few, rank),
            "parts_c%d" % p: (col, few, rank), "full_r%d" % p: (row, few, rank),
            "raw_s%d" % p: (own_second, rank),
            "gram_g%d" % p: square, "recv_g%d" % p: (half, rank),
            "across_g%d" % p: (chips, half, rank), "full_g%d" % p: square,
        })
        for q in range(count):
            buffers.update({
                "terms_s%d%d" % (p, q): (own_second // count, rank),
                "recv_s%d%d" % (p, q): (row, own_second // count // row, rank),
                "full_s%d%d" % (p, q): (own_second // count, rank),
            })
    names = list(buffers) + ["sem_" + name for name in pairs + cuts] + ["sem_load", "sem_move"]
    shapes = [pltpu.VMEM(shape, jnp.float32) for shape in buffers.values()]
    names.insert(len(shapes), "across_left")
    shapes.append(pltpu.VMEM((rank, 6 * PIVOTS), jnp.bfloat16))
    shapes += [pltpu.SemaphoreType.DMA((2,)) for name in pairs]
    shapes += [pltpu.SemaphoreType.DMA((count, 2)) for name in cuts]
    shapes += [pltpu.SemaphoreType.DMA((frames // math.gcd(frames, GROUP),))]
    shapes += [pltpu.SemaphoreType.DMA((2,))]
    return names, shapes


def kernel(sizes, names, tensor, first_in, second_in, first_out, second_out, frames_out, weights_out, *scratch):
    row, col = sizes["row"], sizes["col"]
    v = dict(zip(names, scratch))
    inv, sums, tens, held = v["inv"], v["sums"], v["tens"], v["held"]
    first, second = v["first"], v["second"]
    frames, own_first, own_second = tensor.shape
    rank = first.shape[1]
    half = rank // 2
    count = cuts_of(own_second, row)
    rows_first, rows_second = own_first * row, own_second * col
    steps = rank // PIVOTS
    twin = Twin(col)

    group = math.gcd(frames, GROUP)
    loads = frames // group

    def load(g):
        block = pl.ds(g * group, group)
        return pltpu.make_async_copy(tensor.at[block], tens.at[block], v["sem_load"].at[g])

    def move(source, target, at):
        copy = pltpu.make_async_copy(source, target, v["sem_move"].at[at])
        copy.start()
        return copy

    def contract(start, stop):
        def step(g, carry):
            load(g).wait()
            ks = [g * group + u for u in range(group)]
            parts = [cross(tens[k], first[...], HIGH) for k in ks]
            for k, part in zip(ks, parts):
                held[k] = part
                sums[pl.ds(k, 1), :] = jnp.sum(part * second[...], axis=0, keepdims=True)
            return carry

        lax.fori_loop(start, stop, step, 0)

    def frame_terms(raw, start, stop):
        def step(k, carry):
            sums[pl.ds(k, 1), :] = jnp.sum(held[k] * raw[...], axis=0, keepdims=True)
            return carry

        lax.fori_loop(start, stop, step, 0, unroll=8)

    def lines(q):
        small = own_second // row // count
        starts = [d * small * count + q * small for d in range(row)]
        return [slice(start, start + small) for start in starts]

    def second_terms(out, q):
        small = own_second // row // count
        zero = tuple(jnp.zeros((small, rank), jnp.float32) for _ in range(row))

        def step(k, totals):
            weight = frames_out[pl.ds(k, 1), :]
            return tuple(total + held[k, at, :] * weight for total, at in zip(totals, lines(q)))

        for d, total in enumerate(lax.fori_loop(0, frames, step, zero, unroll=8)):
            out[d * small : (d + 1) * small, :] = total

    def first_terms(raw, start, stop):
        group = math.gcd(stop - start, 4)

        def step(g, carry):
            base = start + g * group
            stacked = tens[pl.ds(base, group)].reshape(group * own_first, own_second)
            part = product(stacked, raw[...], HIGH)
            v["terms_f"][...] += sum(
                part[u * own_first : (u + 1) * own_first, :] * frames_out[pl.ds(base + u, 1), :]
                for u in range(group)
            )
            return carry

        lax.fori_loop(0, (stop - start) // group, step, 0)

    def frames_across(name):
        return lots_share(
            "col", col, total(v["recv_r" + name]), v["parts_c" + name], v["sem_c" + name]
        )

    def frames_back(name):
        return lots_share(
            "row", row, total(v["parts_c" + name]), v["full_r" + name], v["sem_d"]
        )

    def solve_frames(frame_sums, scale):
        raw = product(frame_sums * scale, inv[...], HIGH) * scale
        raw = raw * (1.0 / math.sqrt(rows_first * rows_second))
        normed = raw / jnp.sqrt(jnp.mean(raw * raw, axis=0, keepdims=True) + epsilon)
        frames_out[...] = normed

    state = (inv, v["panel"], v["solved"], v["across_left"])

    def unit(gram):
        down = lax.broadcasted_iota(jnp.int32, (rank, rank), 0)
        across = lax.broadcasted_iota(jnp.int32, (rank, rank), 1)
        diagonal = jnp.where(down == across, gram, 0.0)
        wide = 1.0 / jnp.sqrt(jnp.sum(diagonal, axis=0, keepdims=True))
        tall = 1.0 / jnp.sqrt(jnp.sum(diagonal, axis=1, keepdims=True))
        return gram * wide * tall, wide

    come = [move(first_in, first, 0)]
    greet(sizes)
    come.append(move(second_in, second, 1))
    come[0].wait()
    for g in range(loads):
        load(g).start()
    v["gram_a"][...] = cross(first[...], first[...], HIGH)
    greeted(sizes)
    offset = twin.core * half
    go_a = scatter("row", row, v["gram_a"], v["recv_a"], v["sem_a"], offset)
    come[1].wait()
    v["gram_b"][...] = cross(second[...], second[...], HIGH)
    go_b = halves_out(twin, v["gram_b"], v["recv_b"], v["sem_b"])
    contract(0, loads // 2)
    finish(go_b)
    go_b = halves_across(twin, v["gram_b"], v["recv_b"], v["across_b"], v["sem_b2"])
    contract(loads // 2, loads)
    go_r = lots_out(sums, v["lots_r0"], v["recv_r0"], v["sem_r"])
    finish(go_a)
    go_a = gather("row", row, total(v["recv_a"]), v["full_a"], v["sem_a2"], offset)
    finish(go_b)
    v["full_b"][span(twin.core, half), :] = total(v["across_b"])
    go_b = halves_back(twin, v["full_b"], v["sem_b3"])
    finish(go_r)
    go_c = frames_across("0")
    finish(go_b)
    second_gram, second_scale = unit(v["full_b"][...] * (1.0 / rows_second))
    finish(go_a)
    go_a = halves_back(twin, v["full_a"], v["sem_a3"])
    finish(go_a)
    first_gram = v["gram_a"]
    first_gram[...], first_scale = unit(v["full_a"][...] * (1.0 / rows_first))
    wide = None
    for p in range(PASSES):
        here = str(p)
        inv[...] = first_gram[...] * second_gram
        begin(*state)
        invert(*state, 0, steps // 8)
        finish(go_c)
        go_d = frames_back(here)
        invert(*state, steps // 8, steps)
        flush(*state)
        finish(go_d)
        full_r = v["full_r" + here]
        frame_sums = jnp.concatenate([full_r[d] for d in range(row)], axis=0)
        if wide is None:
            frame_scale = first_scale * second_scale
        else:
            frame_sums = frame_sums / wide
            frame_scale = first_scale
        solve_frames(frame_sums, frame_scale)
        parts = [here + str(q) for q in range(count)]
        go_s = []
        for q, part in enumerate(parts):
            second_terms(v["terms_s" + part], q)
            go_s.append(scatter(
                "row", row, v["terms_s" + part], v["recv_s" + part], v["sem_s"].at[q]
            ))
        frame_gram = cross(frames_out[...], frames_out[...], HIGH) * (1.0 / frames)
        inv[...] = first_gram[...] * frame_gram
        go_t = []
        at = 0
        begin(*state)
        for q, part in enumerate(parts):
            until = steps if q + 1 == count else min(steps, steps * (7 + q) // 8)
            if at < until:
                invert(*state, at, until)
                at = until
            finish(go_s[q])
            go_t.append(gather(
                "row", row, total(v["recv_s" + part]), v["full_s" + part], v["sem_t"].at[q]
            ))
        flush(*state)
        raw = v["raw_s" + here]
        gram_g, recv_g, across_g, full_g = (
            v[name + here] for name in ("gram_g", "recv_g", "across_g", "full_g")
        )
        for q, part in enumerate(parts):
            finish(go_t[q])
            some = product(v["full_s" + part][...] * first_scale, inv[...], HIGH) * (
                first_scale * (1.0 / math.sqrt(rows_first * frames))
            )
            small = some.shape[0] // row
            for d, place in enumerate(lines(q)):
                raw[place, :] = some[d * small : (d + 1) * small, :]
            terms = cross(some, some, HIGH)
            gram_g[...] = terms if q == 0 else gram_g[...] + terms
        go_g = halves_out(twin, gram_g, recv_g, v["sem_g"])
        last = p + 1 == PASSES
        if last:
            v["terms_f"][...] = jnp.zeros((own_first, rank), jnp.float32)
            first_terms(raw, 0, frames // 4)
        else:
            later = str(p + 1)
            frame_terms(raw, 0, frames)
            go_r = lots_out(sums, v["lots_r" + later], v["recv_r" + later], v["sem_r"])
        finish(go_g)
        go_g = halves_across(twin, gram_g, recv_g, across_g, v["sem_h" + here])
        if last:
            first_terms(raw, frames // 4, frames)
            go_f = scatter("col", col, v["terms_f"], v["recv_f"], v["sem_f"])
        else:
            finish(go_r)
            go_c = frames_across(later)
        finish(go_g)
        full_g[span(twin.core, half), :] = total(across_g)
        go_g = halves_back(twin, full_g, v["sem_i"])
        finish(go_g)
        gram = full_g[...] * (1.0 / rows_second)
        down = lax.broadcasted_iota(jnp.int32, (rank, rank), 0)
        across = lax.broadcasted_iota(jnp.int32, (rank, rank), 1)
        diagonal = jnp.where(down == across, gram, 0.0)
        wide = jnp.sqrt(jnp.sum(diagonal, axis=0, keepdims=True) + epsilon)
        tall = jnp.sqrt(jnp.sum(diagonal, axis=1, keepdims=True) + epsilon)
        second_gram = gram / wide / tall
    inv[...] = second_gram * frame_gram
    begin(*state)
    invert(*state, 0, steps // 8)
    finish(go_f)
    go_f = gather("col", col, total(v["recv_f"]), v["full_f"], v["sem_f2"])
    invert(*state, steps // 8, steps)
    flush(*state)
    finish(go_f)
    second_raw, raw = raw, product(v["full_f"][...] / wide, inv[...], HIGH) * (1.0 / math.sqrt(rows_second * frames))
    squares = jnp.sum(raw * raw, axis=0, keepdims=True)
    go_w = spread("row", row, squares, v["parts_w"], v["sem_w"])
    first_out[...] = raw
    second_out[...] = second_raw[...] / wide
    finish(go_w)
    weights = jnp.sqrt(total(v["parts_w"])[0:1, :] * (1.0 / rows_first) + epsilon)
    weights_out[...] = weights
    first_out[...] = first_out[...] / weights


def deliver(*refs):
    half = len(refs) // 2
    sems = refs[-1]
    copies = [
        pltpu.make_async_copy(source, target, sems.at[k])
        for k, (source, target) in enumerate(zip(refs[:half], refs[half : 2 * half]))
    ]
    for copy in copies:
        copy.start()
    for copy in copies:
        copy.wait()


def body(sizes, tensor, initial_first, initial_second):
    frames, own_first, own_second = tensor.shape
    rank = initial_first.shape[1]
    names, scratch = layout(sizes, frames, own_first, own_second, rank)
    far = pl.BlockSpec(memory_space=pltpu.HBM)
    near = pl.BlockSpec(memory_space=pltpu.VMEM)
    outs = ((own_first, rank), (own_second, rank), (frames, rank), (1, rank))
    shapes = [jax.ShapeDtypeStruct(shape, jnp.float32) for shape in outs]
    results = pl.pallas_call(
        functools.partial(kernel, sizes, names),
        out_shape=shapes,
        in_specs=[far] * 3,
        out_specs=[near] * len(outs),
        scratch_shapes=scratch,
        compiler_params=pltpu.CompilerParams(
            collective_id=0, has_side_effects=True, vmem_limit_bytes=48 * 1024 * 1024
        ),
        name="als",
    )(*[
        pltpu.with_memory_space_constraint(x, pltpu.HBM)
        for x in (tensor, initial_first, initial_second)
    ])
    results = pl.pallas_call(
        deliver,
        out_shape=shapes,
        in_specs=[near] * len(outs),
        out_specs=[far] * len(outs),
        scratch_shapes=[pltpu.SemaphoreType.DMA((len(outs),))],
        compiler_params=pltpu.CompilerParams(vmem_limit_bytes=1024 * 1024),
        name="deliver",
    )(*results)
    factor_first, second, factor_frames, weights = results
    return (factor_first, second, factor_frames, weights.reshape(rank))


def solution(mesh):
    sizes = {"row": mesh.shape["row"], "col": mesh.shape["col"]}
    placed = (P(None, "row", "col"), P("row", None), P("col", None))
    return jax.shard_map(
        functools.partial(body, sizes),
        mesh=mesh,
        in_specs=placed,
        out_specs=(P("row", None), P("col", None), P(), P()),
        check_vma=False,
    )
```
